32 devices in a mesh: dp: 2 (over x), pp: 4 (over z), tp: 4 (over y, core).
Axes of the slice: x: 2, y: 2, z: 4, core: 2. Of those that a mesh axis runs over, the one named last changes fastest.
Arguments:
- tokens_a: bfloat16 [1024, 5120], P(('dp', 'pp', 'tp')), parts along dimension 0
- segment_a: int32 [1024], P(('dp', 'pp', 'tp')), parts along dimension 0
- position_a: int32 [1024], P(('dp', 'pp', 'tp')), parts along dimension 0
- tokens_b: bfloat16 [8192, 5120], P(('dp', 'pp', 'tp')), parts along dimension 0
- segment_b: int32 [8192], P(('dp', 'pp', 'tp')), parts along dimension 0
- position_b: int32 [8192], P(('dp', 'pp', 'tp')), parts along dimension 0
- norm_attn: bfloat16 [2, 5120], replicated
- w_query: bfloat16 [2, 5120, 5120], P(None, None, 'tp')
- w_key: bfloat16 [2, 5120, 1024], replicated
- w_value: bfloat16 [2, 5120, 1024], replicated
- w_out: bfloat16 [2, 5120, 5120], P(None, 'tp')
- norm_mlp: bfloat16 [2, 5120], replicated
- w_gate: bfloat16 [2, 5120, 13824], P(None, None, 'tp')
- w_up: bfloat16 [2, 5120, 13824], P(None, None, 'tp')
- w_down: bfloat16 [2, 13824, 5120], P(None, 'tp')
Outputs:
- output 1: bfloat16 [1024, 5120], P(('dp', 'pp', 'tp')), parts along dimension 0
- output 2: bfloat16 [8192, 5120], P(('dp', 'pp', 'tp')), parts along dimension 0
There are 2 independent parts. The reference program is written for one: setup_inputs(seed, part) draws one part's arguments, and reference() takes and returns one part's arrays. A program takes and returns all parts, laid end to end along the dimension named above; an argument that names none is the same for every part.
All inputs are finite; a program needn't handle non-finite values.
Results may differ from the reference program's by a relative error of at most 0.0177145.
Values are sent between devices in bfloat16 or wider.
A program may use at most 1.25 GiB of HBM per device.

```python
import math
import jax
import jax.numpy as jnp
from jax import lax

D = 5120
HQ = 40
HKV = 8
HEAD = 128
FF = 13824
LAYERS = 2
TA = 512
TB = 4096
NSEG = 4
ROPE_BASE = 500000.0
EPS = 1e-5


def draw_layout(layout_key, length):
    key_cut, key_step, key_shift = jax.random.split(layout_key, 3)
    cut_points = jnp.sort(jax.random.permutation(key_cut, length - 1)[:NSEG - 1] + 1)
    row_index = jnp.arange(length, dtype=jnp.int32)
    segment = jnp.sum((row_index[:, None] >= cut_points[None, :]).astype(jnp.int32), axis=1)
    step_sizes = jax.random.randint(key_step, (length,), 1, 4, dtype=jnp.int32)
    shifts = jax.random.randint(key_shift, (NSEG,), 0, 4096, dtype=jnp.int32)
    position = jnp.cumsum(step_sizes) + shifts[segment]
    return segment.astype(jnp.int32), position.astype(jnp.int32)


def setup_inputs(seed: int = 0, part: int = 0) -> dict:
    key_list = jax.random.split(jax.random.key(seed), 9)
    data_keys = jax.random.split(jax.random.fold_in(jax.random.key(seed + 1), part), 4)
    segment_a, position_a = draw_layout(data_keys[0], TA)
    segment_b, position_b = draw_layout(data_keys[1], TB)
    score_var = max(1.0, math.log((TA + TB) / 256.0))
    qk_gain = score_var ** 0.25

    def draw_normal(rand_key, dims_shape, std_scale):
        return (jax.random.normal(rand_key, dims_shape, jnp.float32) * std_scale).astype(jnp.bfloat16)

    def draw_gain(rand_key):
        return (1.0 + 0.3 * jax.random.normal(rand_key, (LAYERS, D), jnp.float32)).astype(jnp.bfloat16)

    return {
        'tokens_a': draw_normal(data_keys[2], (TA, D), 1.0),
        'segment_a': segment_a,
        'position_a': position_a,
        'tokens_b': draw_normal(data_keys[3], (TB, D), 1.0),
        'segment_b': segment_b,
        'position_b': position_b,
        'norm_attn': draw_gain(key_list[0]),
        'w_query': draw_normal(key_list[1], (LAYERS, D, HQ * HEAD), qk_gain * D ** -0.5),
        'w_key': draw_normal(key_list[2], (LAYERS, D, HKV * HEAD), qk_gain * D ** -0.5),
        'w_value': draw_normal(key_list[3], (LAYERS, D, HKV * HEAD), D ** -0.5),
        'w_out': draw_normal(key_list[4], (LAYERS, HQ * HEAD, D), (HQ * HEAD) ** -0.5),
        'norm_mlp': draw_gain(key_list[5]),
        'w_gate': draw_normal(key_list[6], (LAYERS, D, FF), D ** -0.5),
        'w_up': draw_normal(key_list[7], (LAYERS, D, FF), D ** -0.5),
        'w_down': draw_normal(key_list[8], (LAYERS, FF, D), 0.5 * FF ** -0.5),
    }


def rms_norm(hidden, gain_vec):
    wide_vals = hidden.astype(jnp.float32)
    inv_rms = lax.rsqrt(jnp.mean(wide_vals * wide_vals, axis=-1, keepdims=True) + EPS)
    return (wide_vals * inv_rms * gain_vec.astype(jnp.float32)).astype(jnp.bfloat16)


def apply_rope(head_vals, position):
    half_dim = head_vals.shape[-1] // 2
    inv_freq = jnp.power(ROPE_BASE, -2.0 * jnp.arange(half_dim, dtype=jnp.float32) / head_vals.shape[-1])
    angles = position.astype(jnp.float32)[..., None] * inv_freq
    cosine = jnp.cos(angles)[..., None, :]
    sine_v = jnp.sin(angles)[..., None, :]
    first_half = head_vals[..., :half_dim]
    second_half = head_vals[..., half_dim:]
    return jnp.concatenate([first_half * cosine - second_half * sine_v, second_half * cosine + first_half * sine_v], axis=-1)


def attention(q_rot, k_rot, v_heads, segment):
    length = q_rot.shape[0]
    q_block = math.gcd(length, 2 ** int(math.log2(max(8, 2 ** 24 // (HQ * length)))))
    n_blocks = length // q_block
    key_index = jnp.arange(length, dtype=jnp.int32)
    sm_scale = HEAD ** -0.5
    k_wide = k_rot.astype(jnp.float32)
    v_wide = v_heads.astype(jnp.float32)

    def one_block(block_in):
        q_blk, idx_blk, seg_blk = block_in
        scores = jnp.einsum('qhgd,khd->hgqk', q_blk.astype(jnp.float32), k_wide) * sm_scale
        allowed = (seg_blk[:, None] == segment[None, :]) & (key_index[None, :] <= idx_blk[:, None])
        soft_probs = jax.nn.softmax(jnp.where(allowed, scores, -1e30), axis=-1).astype(jnp.bfloat16)
        return jnp.einsum('hgqk,khd->qhgd', soft_probs.astype(jnp.float32), v_wide).astype(jnp.bfloat16)

    blocked = lax.map(one_block, (q_rot.reshape(n_blocks, q_block, HKV, HQ // HKV, HEAD), key_index.reshape(n_blocks, q_block), segment.reshape(n_blocks, q_block)))
    return blocked.reshape(length, HQ * HEAD)


def decoder_layer(hidden, layer_w, segment, position):
    g_attn, wq_l, wk_l, wv_l, wo_l, g_mlp, wg_l, wu_l, wd_l = layer_w
    length = hidden.shape[0]
    normed = rms_norm(hidden, g_attn)
    q_proj = jnp.dot(normed, wq_l, preferred_element_type=jnp.float32).reshape(length, HQ, HEAD)
    k_proj = jnp.dot(normed, wk_l, preferred_element_type=jnp.float32).reshape(length, HKV, HEAD)
    v_heads = jnp.dot(normed, wv_l, preferred_element_type=jnp.float32).astype(jnp.bfloat16).reshape(length, HKV, HEAD)
    q_rot = apply_rope(q_proj, position).astype(jnp.bfloat16).reshape(length, HKV, HQ // HKV, HEAD)
    k_rot = apply_rope(k_proj, position).astype(jnp.bfloat16)
    attn_out = attention(q_rot, k_rot, v_heads, segment)
    mixed_res = (hidden.astype(jnp.float32) + jnp.dot(attn_out, wo_l, preferred_element_type=jnp.float32)).astype(jnp.bfloat16)
    normed_mlp = rms_norm(mixed_res, g_mlp)
    gate_proj = jnp.dot(normed_mlp, wg_l, preferred_element_type=jnp.float32)
    up_proj = jnp.dot(normed_mlp, wu_l, preferred_element_type=jnp.float32)
    gated_act = (jax.nn.silu(gate_proj) * up_proj).astype(jnp.bfloat16)
    return (mixed_res.astype(jnp.float32) + jnp.dot(gated_act, wd_l, preferred_element_type=jnp.float32)).astype(jnp.bfloat16)


def reference(tokens_a, segment_a, position_a, tokens_b, segment_b, position_b, norm_attn, w_query, w_key, w_value, w_out, norm_mlp, w_gate, w_up, w_down):
    stacked = (norm_attn, w_query, w_key, w_value, w_out, norm_mlp, w_gate, w_up, w_down)

    def run_stack(tokens, segment, position):
        def scan_body(hidden, layer_w):
            return decoder_layer(hidden, layer_w, segment, position), None
        scan_out = lax.scan(scan_body, tokens, stacked)
        return scan_out[0]

    return (run_stack(tokens_a, segment_a, position_a), run_stack(tokens_b, segment_b, position_b))
```

```python
import functools
import math
import jax
import jax.numpy as jnp
from jax import lax
from jax.experimental import pallas as pl
from jax.experimental.pallas import tpu as pltpu
from jax.sharding import PartitionSpec as P

HEAD = 128
ROPE_BASE = 500000.0
EPS = 1e-5
NEG = -1e30
BF = jnp.bfloat16
F32 = jnp.float32
VMEM_LIMIT = 60 * 1024 * 1024
OWNER_XOR = (0, 2, 1, 3)


def chunk_table(nb, na):
    if nb == 256:
        return [(64, 32), (96, 0), (96, 0)]
    return [(nb // 2, na), (nb // 2, 0)]


def cparams(semantics=None, limit=VMEM_LIMIT):
    return pltpu.CompilerParams(dimension_semantics=semantics, vmem_limit_bytes=limit)


def any_spec():
    return pl.BlockSpec(memory_space=pl.ANY)


def norm_rows(wide, gain):
    inv = lax.rsqrt(jnp.mean(wide * wide, axis=-1, keepdims=True) + EPS)
    return (wide * inv * gain).astype(BF)


def norm_init_kernel(ns, own_ref, got_ref, gain_ref, h_ref, n_ref):
    gain = gain_ref[...].astype(F32)

    def put(src):
        h_ref[...] = src[...]
        n_ref[...] = norm_rows(src[...].astype(F32), gain)

    @pl.when(pl.program_id(0) < ns)
    def _():
        put(own_ref)

    @pl.when(pl.program_id(0) >= ns)
    def _():
        put(got_ref)


def norm_init(own, got, gain, qb):
    q, d = own.shape
    ns = q // qb
    out = jax.ShapeDtypeStruct((2 * q, d), BF)
    return pl.pallas_call(
        functools.partial(norm_init_kernel, ns),
        grid=(2 * ns,),
        in_specs=[
            pl.BlockSpec((qb, d), lambda i: (jnp.minimum(i, ns - 1), 0)),
            pl.BlockSpec((qb, d), lambda i: (jnp.maximum(i - ns, 0), 0)),
            pl.BlockSpec((1, d), lambda i: (0, 0)),
        ],
        out_specs=[pl.BlockSpec((qb, d), lambda i: (i, 0))] * 2,
        out_shape=[out, out],
        compiler_params=cparams(("arbitrary",)),
        cost_estimate=pl.CostEstimate(flops=2 * q * d * 20, bytes_accessed=12 * q * d, transcendentals=2 * q),
        name="norm_init",
    )(own, got, gain)


def add_kernel(a_ref, b_ref, o_ref):
    o_ref[...] = (a_ref[...].astype(F32) + b_ref[...].astype(F32)).astype(BF)


def add(a, b, qb):
    rows, d = a.shape
    spec = pl.BlockSpec((qb, d), lambda i: (i, 0))
    return pl.pallas_call(
        add_kernel,
        grid=(rows // qb,),
        in_specs=[spec, spec],
        out_specs=spec,
        out_shape=jax.ShapeDtypeStruct((rows, d), BF),
        compiler_params=cparams(("arbitrary",)),
        cost_estimate=pl.CostEstimate(flops=rows * d * 10, bytes_accessed=6 * rows * d, transcendentals=0),
        name="add",
    )(a, b)


def norm_add_kernel(h_ref, s_ref, t_ref, gain_ref, ho_ref, n_ref):
    h = (h_ref[...].astype(F32) + (s_ref[...].astype(F32) + t_ref[...].astype(F32))).astype(BF)
    ho_ref[...] = h
    n_ref[...] = norm_rows(h.astype(F32), gain_ref[...].astype(F32))


def norm_add(h, s, t, gain, qb):
    rows, d = h.shape
    n = rows // qb
    out = jax.ShapeDtypeStruct((rows, d), BF)
    same = pl.BlockSpec((qb, d), lambda i: (i, 0))
    return pl.pallas_call(
        norm_add_kernel,
        grid=(n,),
        in_specs=[same, same, pl.BlockSpec((qb, d), lambda i: (lax.rem(i + n // 2, n), 0)), pl.BlockSpec((1, d), lambda i: (0, 0))],
        out_specs=[same, same],
        out_shape=[out, out],
        compiler_params=cparams(("arbitrary",)),
        cost_estimate=pl.CostEstimate(flops=rows * d * 20, bytes_accessed=10 * rows * d, transcendentals=rows),
        name="norm_add",
    )(h, s, t, gain)


def rope(vals, cos, sin):
    return (vals * cos + pltpu.roll(vals, HEAD // 2, 1) * sin).astype(BF)


def qkv_kernel(nkv, sc_ref, n1_ref, n2_ref, wq_ref, wk_ref, wv_ref, cos_ref, sin_ref, q_ref, kv_ref, x_ref):
    j = pl.program_id(0)
    half = n1_ref.shape[0]
    width = nkv * HEAD

    @pl.when(j == 0)
    def _():
        x_ref[:half, :] = n1_ref[...]
        x_ref[half:, :] = n2_ref[...]
        k = jnp.dot(x_ref[...], wk_ref[...], preferred_element_type=F32)
        for i in range(nkv):
            kv_ref[:, i * HEAD:(i + 1) * HEAD] = rope(k[:, i * HEAD:(i + 1) * HEAD], cos_ref[...], sin_ref[...])
        kv_ref[:, width:] = jnp.dot(x_ref[...], wv_ref[...], preferred_element_type=F32).astype(BF)

    @pl.when(j > 0)
    def _():
        acc = jnp.dot(x_ref[...], wq_ref[...], preferred_element_type=F32)
        for i in range(acc.shape[1] // HEAD):
            q_ref[:, i * HEAD:(i + 1) * HEAD] = rope(acc[:, i * HEAD:(i + 1) * HEAD], cos_ref[...], sin_ref[...])


def qkv(sc, n1, n2, wq, wk, wv, cos, sin, layer, nkv):
    half, d = n1.shape
    rows = 2 * half
    qcols = wq.shape[2]
    bq = 256 if qcols % 256 == 0 else qcols
    nq = qcols // bq
    width = nkv * HEAD
    const = lambda j, s: (0, 0)
    grid_spec = pltpu.PrefetchScalarGridSpec(
        num_scalar_prefetch=1,
        grid=(nq + 1,),
        in_specs=[
            pl.BlockSpec((half, d), const, pipeline_mode=pl.Buffered(1)),
            pl.BlockSpec((half, d), const, pipeline_mode=pl.Buffered(1)),
            pl.BlockSpec((None, d, bq), lambda j, s: (layer, 0, jnp.maximum(j - 1, 0))),
            pl.BlockSpec((None, d, width), lambda j, s: (layer, 0, s[0]), pipeline_mode=pl.Buffered(1)),
            pl.BlockSpec((None, d, width), lambda j, s: (layer, 0, s[0]), pipeline_mode=pl.Buffered(1)),
            pl.BlockSpec((rows, HEAD), const, pipeline_mode=pl.Buffered(1)),
            pl.BlockSpec((rows, HEAD), const, pipeline_mode=pl.Buffered(1)),
        ],
        out_specs=[
            pl.BlockSpec((rows, bq), lambda j, s: (0, jnp.maximum(j - 1, 0))),
            pl.BlockSpec((rows, 2 * width), const),
        ],
        scratch_shapes=[pltpu.VMEM((rows, d), BF)],
    )
    flops = 2 * rows * d * (qcols + 2 * width)
    return pl.pallas_call(
        functools.partial(qkv_kernel, nkv),
        grid_spec=grid_spec,
        out_shape=[jax.ShapeDtypeStruct((rows, qcols), BF), jax.ShapeDtypeStruct((rows, 2 * width), BF)],
        compiler_params=cparams(("arbitrary",)),
        cost_estimate=pl.CostEstimate(flops=flops, bytes_accessed=2 * d * (rows + qcols + 2 * width), transcendentals=0),
        name="qkv",
    )(sc, n1, n2, wq, wk, wv, cos, sin)


def flash(q_ref, r0, rows, kv_ref, bk, nkv, group, lo, hi, qi_ref, ql_ref, o_ref, m_ref, l_ref, acc_ref):
    c = HEAD ** -0.5 * math.log2(math.e)
    gr = group * rows
    qi = qi_ref[r0:r0 + rows, :1]
    ql = ql_ref[r0:r0 + rows, :1]
    ql_max = jnp.max(ql)
    qi_min = jnp.min(qi)
    for kh in range(nkv):
        heads = [kh * group + i for i in range(group)]
        qs = jnp.concatenate([q_ref[r0:r0 + rows, h * HEAD:(h + 1) * HEAD] for h in heads], axis=0)
        m_ref[:gr, :] = jnp.full((gr, HEAD), NEG, F32)
        l_ref[:gr, :] = jnp.zeros((gr, HEAD), F32)
        acc_ref[:gr, :] = jnp.zeros((gr, HEAD), F32)

        def step(j, masked, qs=qs, kh=kh):
            base = pl.multiple_of(j * bk, bk)
            k = kv_ref[pl.ds(base, bk), kh * HEAD:(kh + 1) * HEAD]
            v = kv_ref[pl.ds(base, bk), (nkv + kh) * HEAD:(nkv + kh + 1) * HEAD]
            s = lax.dot_general(qs, k, (((1,), (1,)), ((), ())), preferred_element_type=F32)
            if masked:
                kid = base + lax.broadcasted_iota(jnp.int32, (rows, bk), 1)
                ok = (kid <= qi) & (kid >= ql)
                s = jnp.where(ok[None], s.reshape(group, rows, bk), NEG).reshape(gr, bk)
            m_old = m_ref[:gr, :1]
            m_new = jnp.maximum(m_old, jnp.max(s, axis=1, keepdims=True))
            alpha = jnp.exp2((m_old - m_new) * c)
            p = jnp.exp2((s - m_new) * c)
            l_ref[:gr, :] = jnp.broadcast_to(l_ref[:gr, :1] * alpha + jnp.sum(p, axis=1, keepdims=True), (gr, HEAD))
            m_ref[:gr, :] = jnp.broadcast_to(m_new, (gr, HEAD))
            acc_ref[:gr, :] = acc_ref[:gr, :] * alpha + jnp.dot(p.astype(BF), v, preferred_element_type=F32)

        def body(j, carry):
            base = j * bk
            full = (ql_max <= base) & (qi_min >= base + bk - 1)

            @pl.when(full)
            def _():
                step(j, False)

            @pl.when(jnp.logical_not(full))
            def _():
                step(j, True)

            return carry

        lax.fori_loop(lo, hi, body, 0)
        out = (acc_ref[:gr, :] / l_ref[:gr, :]).astype(BF)
        for i, h in enumerate(heads):
            o_ref[r0:r0 + rows, h * HEAD:(h + 1) * HEAD] = out[i * rows:(i + 1) * rows, :]


def attn_kernel(table, me, nkv, group, nb, na, sc_ref, q_ref, qi_ref, ql_ref, *refs):
    n_kv = 4 * len(table)
    kv_hbm = refs[:n_kv]
    o_ref, kvb_ref, kva_ref, m_ref, l_ref, acc_ref, sem = refs[n_kv:]
    o = pl.program_id(0)
    b, a = table[me]

    def copies():
        off_b, off_a = 0, 0
        out = []
        for k, (bk_, ak_) in enumerate(table):
            for s in range(4):
                for place in range(4):
                    owner = sc_ref[0] ^ OWNER_XOR[place]
                    src = kv_hbm[4 * k + s]
                    row = place * (bk_ + ak_)
                    if bk_:
                        dst = pl.multiple_of((3 - s) * 4 * nb + owner * nb + off_b, 16)
                        out.append(pltpu.make_async_copy(src.at[pl.ds(row, bk_), :], kvb_ref.at[pl.ds(dst, bk_), :], sem))
                    if ak_:
                        dst = pl.multiple_of((3 - s) * 4 * na + owner * na + off_a, 16)
                        out.append(pltpu.make_async_copy(src.at[pl.ds(row + bk_, ak_), :], kva_ref.at[pl.ds(dst, ak_), :], sem))
            off_b += bk_
            off_a += ak_
        return out

    @pl.when(o == 0)
    def _():
        for copy in copies():
            copy.start()
        for copy in copies():
            copy.wait()

    common = (qi_ref, ql_ref, o_ref, m_ref, l_ref, acc_ref)
    if b:
        bk = min(512, 16 * nb)
        flash(q_ref, 0, b, kvb_ref, bk, nkv, group, sc_ref[4 + o], sc_ref[8 + o], *common)
    if a:
        bk = min(256, 16 * na)
        flash(q_ref, b, a, kva_ref, bk, nkv, group, sc_ref[12 + o], sc_ref[16 + o], *common)


def attention(table, me, sc, q, qi, ql, kvs, nkv, group, nb, na):
    rows, qcols = q.shape
    own = rows // 4
    b, a = table[me]
    gr = group * max(a, b)
    kvw = 2 * nkv * HEAD
    row_spec = lambda w: pl.BlockSpec((own, w), lambda i, s: (i, 0))
    flat = [x for per_chunk in kvs for x in per_chunk]
    flops = 4 * (4 * b * 16 * nb + 4 * a * 16 * na) * qcols
    return pl.pallas_call(
        functools.partial(attn_kernel, table, me, nkv, group, nb, na),
        grid_spec=pltpu.PrefetchScalarGridSpec(
            num_scalar_prefetch=1,
            grid=(4,),
            in_specs=[row_spec(qcols), row_spec(HEAD), row_spec(HEAD)] + [any_spec()] * len(flat),
            out_specs=row_spec(qcols),
            scratch_shapes=[
                pltpu.VMEM((16 * nb, kvw), BF),
                pltpu.VMEM((16 * na, kvw), BF),
                pltpu.VMEM((gr, HEAD), F32),
                pltpu.VMEM((gr, HEAD), F32),
                pltpu.VMEM((gr, HEAD), F32),
                pltpu.SemaphoreType.DMA,
            ],
        ),
        out_shape=jax.ShapeDtypeStruct((rows, qcols), BF),
        compiler_params=cparams(("arbitrary",)),
        cost_estimate=pl.CostEstimate(flops=flops, bytes_accessed=4 * rows * qcols + 32 * (nb + na) * kvw, transcendentals=0),
        name="attention",
    )(sc, q, qi, ql, *flat)


def oproj_kernel(o_ref, w_ref, pm_ref, pp_ref):
    half = pm_ref.shape[0]
    acc = jnp.dot(o_ref[...], w_ref[...], preferred_element_type=F32)
    pm_ref[...] = acc[:half].astype(BF)
    pp_ref[...] = acc[half:].astype(BF)


def oproj(o, wo, layer):
    rows, k = o.shape
    d = wo.shape[2]
    bn = min(1024, d)
    half = rows // 2
    out = jax.ShapeDtypeStruct((half, d), BF)
    return pl.pallas_call(
        oproj_kernel,
        grid=(d // bn,),
        in_specs=[pl.BlockSpec((rows, k), lambda j: (0, 0), pipeline_mode=pl.Buffered(1)), pl.BlockSpec((None, k, bn), lambda j: (layer, 0, j))],
        out_specs=[pl.BlockSpec((half, bn), lambda j: (0, j))] * 2,
        out_shape=[out, out],
        compiler_params=cparams(("arbitrary",)),
        cost_estimate=pl.CostEstimate(flops=2 * rows * k * d, bytes_accessed=2 * (rows * k + k * d + rows * d), transcendentals=0),
        name="oproj",
    )(o, wo)


def mlp_kernel(layer, bf, bn, n1_ref, n2_ref, wg_ref, wu_ref, wd_ref, pm_ref, pp_ref, x_ref, w_ref, wd_buf, act_ref, x_sem, w_sem, d_sem):
    j = pl.program_id(0)
    half = n1_ref.shape[0]
    ff = wg_ref.shape[2]
    d = wd_ref.shape[2]
    n_up = ff // bf
    n_down = d // bn

    def up_copies(step, slot):
        cols = pl.ds(pl.multiple_of(step * bf, 128), bf)
        return (
            pltpu.make_async_copy(wg_ref.at[layer, :, cols], w_ref.at[slot, :, pl.ds(0, bf)], w_sem.at[slot, 0]),
            pltpu.make_async_copy(wu_ref.at[layer, :, cols], w_ref.at[slot, :, pl.ds(bf, bf)], w_sem.at[slot, 1]),
        )

    def down_copy(step, slot):
        cols = pl.ds(pl.multiple_of(step * bn, 128), bn)
        return pltpu.make_async_copy(wd_ref.at[layer, :, cols], wd_buf.at[slot], d_sem.at[slot])

    def x_copies():
        return (
            pltpu.make_async_copy(n1_ref, x_ref.at[pl.ds(0, half), :], x_sem.at[0]),
            pltpu.make_async_copy(n2_ref, x_ref.at[pl.ds(half, half), :], x_sem.at[1]),
        )

    @pl.when(j == 0)
    def _():
        for copy in x_copies() + up_copies(0, 0):
            copy.start()
        for copy in x_copies():
            copy.wait()

    @pl.when(j < n_up)
    def _():
        slot = lax.rem(j, 2)
        for copy in up_copies(j, slot):
            copy.wait()

        @pl.when(j + 1 < n_up)
        def _():
            for copy in up_copies(j + 1, 1 - slot):
                copy.start()

        @pl.when(j + 1 == n_up)
        def _():
            down_copy(0, 0).start()

        both = jnp.dot(x_ref[...], w_ref[slot], preferred_element_type=F32)
        gate = both[:, :bf]
        act = gate * jax.nn.sigmoid(gate) * both[:, bf:]
        act_ref[:, pl.ds(pl.multiple_of(j * bf, 128), bf)] = act.astype(BF)

    @pl.when(j >= n_up)
    def _():
        i = j - n_up
        slot = lax.rem(i, 2)
        down_copy(i, slot).wait()

        @pl.when(i + 1 < n_down)
        def _():
            down_copy(i + 1, 1 - slot).start()

        acc = jnp.dot(act_ref[...], wd_buf[slot], preferred_element_type=F32)
        pm_ref[...] = acc[:half].astype(BF)
        pp_ref[...] = acc[half:].astype(BF)


def mlp(n1, n2, wg, wu, wd, layer):
    half, d = n1.shape
    rows = 2 * half
    ff = wg.shape[2]
    bf = 384
    bn = 512
    n_up, n_down = ff // bf, d // bn
    out = jax.ShapeDtypeStruct((half, d), BF)
    return pl.pallas_call(
        functools.partial(mlp_kernel, layer, bf, bn),
        grid=(n_up + n_down,),
        in_specs=[any_spec()] * 5,
        out_specs=[pl.BlockSpec((half, bn), lambda j: (0, jnp.maximum(j - n_up, 0)))] * 2,
        out_shape=[out, out],
        scratch_shapes=[
            pltpu.VMEM((rows, d), BF),
            pltpu.VMEM((2, d, 2 * bf), BF),
            pltpu.VMEM((2, ff, bn), BF),
            pltpu.VMEM((rows, ff), BF),
            pltpu.SemaphoreType.DMA((2,)),
            pltpu.SemaphoreType.DMA((2, 2)),
            pltpu.SemaphoreType.DMA((2,)),
        ],
        compiler_params=cparams(("arbitrary",)),
        cost_estimate=pl.CostEstimate(flops=6 * rows * d * ff, bytes_accessed=2 * (2 * rows * d + 3 * d * ff), transcendentals=rows * ff),
        name="mlp",
    )(n1, n2, wg, wu, wd)


def solution(mesh):
    row_spec = P(('dp', 'pp', 'tp'), None)
    id_spec = P(('dp', 'pp', 'tp'))
    col_spec = P(None, None, 'tp')
    in_row_spec = P(None, 'tp', None)
    full_spec = P()
    n_pp = mesh.shape['pp']
    across_core = [(i, i ^ 1) for i in range(4)]
    across_y = [(i, i ^ 2) for i in range(4)]

    def per_device(tok_a, seg_a, pos_a, tok_b, seg_b, pos_b, g_attn, wq, wk, wv, wo, g_mlp, wg, wu, wd):
        t = lax.axis_index('tp')
        p = lax.axis_index('pp')
        n_layers, _ = g_attn.shape
        nb, na = tok_b.shape[0], tok_a.shape[0]
        n_kv_all = wk.shape[2] // HEAD
        nkv = n_kv_all // 4
        group = wq.shape[2] // HEAD // nkv
        table = chunk_table(nb, na)
        n_chunks = len(table)
        owners = [t ^ x for x in OWNER_XOR]
        qb = 32 if nb == 256 else 16

        off_b, off_a, b0, a0 = [], [], 0, 0
        for b, a in table:
            off_b.append(b0)
            off_a.append(a0)
            b0, a0 = b0 + b, a0 + a
        gain_attn = [g_attn[l:l + 1] for l in range(n_layers)]
        gain_mlp = [g_mlp[l:l + 1] for l in range(n_layers)]

        own_rows = []
        for (b, a), ob, oa in zip(table, off_b, off_a):
            parts = [tok_b[ob:ob + b]] if b else []
            parts += [tok_a[oa:oa + a]] if a else []
            own_rows.append(parts[0] if len(parts) == 1 else jnp.concatenate(parts, axis=0))

        h, n_mine, n_part = [None] * n_chunks, [None] * n_chunks, [None] * n_chunks
        for k in range(n_chunks):
            got = lax.ppermute(own_rows[k], 'tp', across_y)
            h[k], n_mine[k] = norm_init(own_rows[k], got, gain_attn[0], qb)
            n_part[k] = lax.ppermute(n_mine[k], 'tp', across_core)

        ints = jnp.concatenate([seg_b, pos_b, seg_a, pos_a])
        all_ints = lax.all_gather(ints, ('pp', 'tp')).reshape(n_pp, 4, 2 * (nb + na))

        def starts_of(seg_all):
            return [jnp.sum((seg_all < v).astype(jnp.int32)) for v in range(4)]

        here = lax.dynamic_index_in_dim(all_ints, p, 0, keepdims=False)
        here = jnp.concatenate([lax.dynamic_index_in_dim(here, o, 0, keepdims=True) for o in owners], axis=0)

        def request(base, n_own):
            seg_all = all_ints[:, :, base:base + n_own]
            starts = starts_of(seg_all)
            seg = here[:, base:base + n_own]
            pos = here[:, base + n_own:base + 2 * n_own]
            shift = (n_pp - 1 - p) * 4 * n_own
            lo = jnp.zeros_like(seg) + starts[0]
            for v in range(1, 4):
                lo = lo + jnp.where(seg >= v, starts[v] - starts[v - 1], 0)
            own_ids = jnp.stack(owners).astype(jnp.int32)[:, None] * n_own + jnp.arange(n_own, dtype=jnp.int32)[None, :]
            idx = own_ids + (n_pp - 1) * 4 * n_own
            return idx, lo + shift, pos

        idx_b, lo_b, pos_b_rows = request(0, nb)
        idx_a, lo_a, pos_a_rows = request(2 * nb, na)

        inv_freq = jnp.power(ROPE_BASE, -2.0 * jnp.arange(HEAD // 2, dtype=F32) / HEAD)

        def trig(pos):
            angles = pos.astype(F32)[..., None] * inv_freq
            cos, sin = jnp.cos(angles), jnp.sin(angles)
            return jnp.concatenate([cos, cos], axis=-1), jnp.concatenate([-sin, sin], axis=-1)

        cos_b, sin_b = trig(pos_b_rows)
        cos_a, sin_a = trig(pos_a_rows)
        t_arr = jnp.stack([t]).astype(jnp.int32)

        cos, sin, q_idx, q_low, scal = [], [], [], [], []
        bk_b, bk_a = min(512, 16 * nb), min(256, 16 * na)
        for (b, a), ob, oa in zip(table, off_b, off_a):
            def pick(xb, xa):
                parts = ([xb[:, ob:ob + b]] if b else []) + ([xa[:, oa:oa + a]] if a else [])
                both = parts[0] if len(parts) == 1 else jnp.concatenate(parts, axis=1)
                return both.reshape((4 * (a + b),) + both.shape[2:])

            cos.append(pick(cos_b, cos_a))
            sin.append(pick(sin_b, sin_a))
            wide = lambda x: jnp.broadcast_to(x[:, None], (x.shape[0], HEAD))
            q_idx.append(wide(pick(idx_b, idx_a)))
            q_low.append(wide(pick(lo_b, lo_a)))
            zero = jnp.zeros((4,), jnp.int32)
            lo_blk_b = lo_b[:, ob] // bk_b if b else zero
            hi_blk_b = idx_b[:, ob + b - 1] // bk_b + 1 if b else zero
            lo_blk_a = lo_a[:, oa] // bk_a if a else zero
            hi_blk_a = idx_a[:, oa + a - 1] // bk_a + 1 if a else zero
            scal.append(jnp.concatenate([jnp.broadcast_to(t_arr, (4,)), lo_blk_b, hi_blk_b, lo_blk_a, hi_blk_a]).astype(jnp.int32))

        def reduce_across(p_mine, p_part):
            got = lax.ppermute(p_part, 'tp', across_core)
            return add(p_mine, got, qb)

        out_b, out_a = [], []
        for l in range(n_layers):
            q, kvs = [None] * n_chunks, [None] * n_chunks
            for k in range(n_chunks):
                q[k], kv = qkv(t_arr, n_mine[k], n_part[k], wq, wk, wv, cos[k], sin[k], l, nkv)
                kvs[k] = [kv] + [lax.ppermute(kv, 'pp', [(i, i + s) for i in range(n_pp - s)]) for s in range(1, n_pp)]
            for k in range(n_chunks):
                o = attention(table, k, scal[k], q[k], q_idx[k], q_low[k], kvs, nkv, group, nb, na)
                p_mine, p_part = oproj(o, wo, l)
                s = reduce_across(p_mine, p_part)
                got = lax.ppermute(s, 'tp', across_y)
                h[k], n_mine[k] = norm_add(h[k], s, got, gain_mlp[l], qb)
                n_part[k] = lax.ppermute(n_mine[k], 'tp', across_core)
            for k in range(n_chunks):
                p_mine, p_part = mlp(n_mine[k], n_part[k], wg, wu, wd, l)
                s = reduce_across(p_mine, p_part)
                if l + 1 < n_layers:
                    got = lax.ppermute(s, 'tp', across_y)
                    h[k], n_mine[k] = norm_add(h[k], s, got, gain_attn[l + 1], qb)
                    n_part[k] = lax.ppermute(n_mine[k], 'tp', across_core)
                else:
                    b, a = table[k]
                    rows = a + b
                    got = lax.ppermute(s[rows:], 'tp', across_y)
                    res = (h[k][:rows].astype(F32) + (s[:rows].astype(F32) + got.astype(F32))).astype(BF)
                    if b:
                        out_b.append(res[:b])
                    if a:
                        out_a.append(res[b:])
        join = lambda parts: parts[0] if len(parts) == 1 else jnp.concatenate(parts, axis=0)
        return join(out_a), join(out_b)

    def prefill(tokens_a, segment_a, position_a, tokens_b, segment_b, position_b, norm_attn, w_query, w_key, w_value, w_out, norm_mlp, w_gate, w_up, w_down):
        mapped = jax.shard_map(per_device, mesh=mesh, in_specs=(row_spec, id_spec, id_spec, row_spec, id_spec, id_spec, full_spec, col_spec, full_spec, full_spec, in_row_spec, full_spec, col_spec, col_spec, in_row_spec), out_specs=(row_spec, row_spec), check_vma=False)
        return mapped(tokens_a, segment_a, position_a, tokens_b, segment_b, position_b, norm_attn, w_query, w_key, w_value, w_out, norm_mlp, w_gate, w_up, w_down)

    return prefill
```

```python
import functools
import math
import jax
import jax.numpy as jnp
from jax import lax
from jax.experimental import pallas as pl
from jax.experimental.pallas import tpu as pltpu
from jax.sharding import PartitionSpec as P

HEAD = 128
ROPE_BASE = 500000.0
EPS = 1e-5
NEG = -1e30
BF = jnp.bfloat16
F32 = jnp.float32
VMEM_LIMIT = 60 * 1024 * 1024
OWNER_XOR = (0, 2, 1, 3)


def chunk_table(nb, na):
    if nb == 256:
        return [(64, 32), (96, 0), (96, 0)]
    return [(nb // 2, na), (nb // 2, 0)]


def cparams(semantics=None, limit=VMEM_LIMIT):
    return pltpu.CompilerParams(dimension_semantics=semantics, vmem_limit_bytes=limit)


def any_spec():
    return pl.BlockSpec(memory_space=pl.ANY)


MESH = pl.DeviceIdType.MESH


def other_core():
    t = lax.axis_index('tp')
    return {'tp': t + 1 - 2 * (t % 2)}


def meet():
    barrier = pltpu.get_barrier_semaphore()
    pl.semaphore_signal(barrier, inc=1, device_id=other_core(), device_id_type=MESH)
    pl.semaphore_wait(barrier, 1)


def norm_rows(wide, gain):
    inv = lax.rsqrt(jnp.mean(wide * wide, axis=-1, keepdims=True) + EPS)
    return (wide * inv * gain).astype(BF)


def norm_scratch(half, d, rb, init):
    n = half // rb
    bufs = [pltpu.VMEM((half, d), BF)] * (1 if init else 3)
    return bufs + [pltpu.SemaphoreType.DMA((2, 3)), pltpu.SemaphoreType.DMA((n,)), pltpu.SemaphoreType.DMA((n,)), pltpu.SemaphoreType.DMA]


class NormExchange:
    def __init__(self, init, rb, srcs, gain_ref, ho_ref, x_ref, scratch):
        self.init, self.rb, self.srcs, self.gain_ref, self.ho_ref, self.x_ref = init, rb, srcs, gain_ref, ho_ref, x_ref
        self.bufs = scratch[:1 if init else 3]
        self.in_sem, self.send_sem, self.recv_sem, self.out_sem = scratch[1 if init else 3:]
        self.half = x_ref.shape[0] // 2
        self.own = self.half // 2
        self.n = self.half // rb

    def loads(self, piece):
        q = self.own
        dst = pl.ds(piece * q, q)
        if self.init:
            return [pltpu.make_async_copy(self.srcs[piece], self.bufs[0].at[dst, :], self.in_sem.at[piece, 0])]
        src = (dst, dst, pl.ds((1 - piece) * q, q))
        return [pltpu.make_async_copy(ref.at[rows, :], buf.at[dst, :], self.in_sem.at[piece, i]) for i, (ref, rows, buf) in enumerate(zip(self.srcs, src, self.bufs))]

    def send(self, i):
        rows = pl.ds(pl.multiple_of(i * self.rb, self.rb), self.rb)
        there = pl.ds(pl.multiple_of(self.half + i * self.rb, self.rb), self.rb)
        return pltpu.make_async_remote_copy(src_ref=self.x_ref.at[rows, :], dst_ref=self.x_ref.at[there, :], send_sem=self.send_sem.at[i], recv_sem=self.recv_sem.at[i], device_id=other_core(), device_id_type=MESH)

    def store(self):
        return pltpu.make_async_copy(self.bufs[0], self.ho_ref, self.out_sem)

    def start(self, piece):
        for copy in self.loads(piece):
            copy.start()

    def run(self):
        gain = self.gain_ref[...].astype(F32)
        per = self.n // 2

        def block(i, carry):
            rows = pl.ds(pl.multiple_of(i * self.rb, self.rb), self.rb)
            if self.init:
                h = self.bufs[0][rows, :]
            else:
                hb, sb, tb = self.bufs
                h = (hb[rows, :].astype(F32) + (sb[rows, :].astype(F32) + tb[rows, :].astype(F32))).astype(BF)
                hb[rows, :] = h
            self.x_ref[rows, :] = norm_rows(h.astype(F32), gain)

            @pl.when(i >= 1)
            def _():
                self.send(i - 1).start()

            return carry

        for piece in range(2):
            for copy in self.loads(piece):
                copy.wait()
            lax.fori_loop(piece * per, (piece + 1) * per, block, 0)
        self.store().start()
        self.send(self.n - 1).start()

    def arrive(self):
        for i in range(self.n):
            self.send(i).wait_recv()

    def finish(self):
        for i in range(self.n):
            self.send(i).wait_send()
        self.store().wait()


def sum_scratch(half, d, bn):
    n = d // bn
    return [
        pltpu.VMEM((2, half, bn), F32),
        pltpu.VMEM((n, half, bn), BF),
        pltpu.VMEM((n, half, bn), BF),
        pltpu.VMEM((half, d), BF),
        pltpu.SemaphoreType.DMA((n,)),
        pltpu.SemaphoreType.DMA((n,)),
        pltpu.SemaphoreType.DMA((n,)),
    ]


class ChipSum:
    def __init__(self, outs, scratch):
        self.outs = outs
        self.mine, self.give, self.got, self.total, self.send_sem, self.recv_sem, self.out_sem = scratch
        self.n, self.half, self.bn = self.give.shape

    def send(self, i):
        return pltpu.make_async_remote_copy(src_ref=self.give.at[i], dst_ref=self.got.at[i], send_sem=self.send_sem.at[i], recv_sem=self.recv_sem.at[i], device_id=other_core(), device_id_type=MESH)

    def cols(self, i):
        return pl.ds(pl.multiple_of(i * self.bn, 128), self.bn)

    def stores(self, i):
        rows = self.half // len(self.outs)
        return [pltpu.make_async_copy(self.total.at[pl.ds(r * rows, rows), self.cols(i)], out.at[:, self.cols(i)], self.out_sem.at[i]) for r, out in enumerate(self.outs)]

    def keep(self, i, acc):
        self.mine[i % 2] = acc[:self.half]
        self.give[i] = acc[self.half:].astype(BF)

    def combine(self, i):
        self.send(i).wait_recv()
        self.total[:, self.cols(i)] = (self.mine[i % 2] + self.got[i].astype(F32)).astype(BF)

    def store(self, i):
        for copy in self.stores(i):
            copy.start()

    def tail(self):
        last = self.n - 1
        self.send(last).start()
        self.store(last - 1)
        self.combine(last)
        self.store(last)
        for i in range(self.n):
            self.send(i).wait_send()
            for copy in self.stores(i):
                copy.wait()


def rope(vals, cos, sin):
    return (vals * cos + pltpu.roll(vals, HEAD // 2, 1) * sin).astype(BF)


def qkv_blocks(qcols):
    blocks, c = [], 0
    while c < qcols:
        width = min(512, qcols - c)
        blocks.append((c, width))
        c += width
    return blocks


def qkv_kernel(init, layer, nkv, rb, *refs):
    n_src = 2 if init else 3
    srcs = refs[:n_src]
    gain_ref, wq_ref, wk_ref, wv_ref, cos_ref, sin_ref, ho_ref, q_ref, kv_ref, x_ref, w_ref, q_buf, kv_buf, w_sem, o_sem = refs[n_src:n_src + 15]
    norm = NormExchange(init, rb, srcs, gain_ref, ho_ref, x_ref, refs[n_src + 15:])
    width = nkv * HEAD
    blocks = qkv_blocks(q_buf.shape[1])
    t = lax.axis_index('tp')

    def loads():
        cols = pl.ds(pl.multiple_of(t * width, 128), width)
        copies = [
            pltpu.make_async_copy(wk_ref.at[layer, :, cols], w_ref.at[:, pl.ds(0, width)], w_sem.at[0]),
            pltpu.make_async_copy(wv_ref.at[layer, :, cols], w_ref.at[:, pl.ds(width, width)], w_sem.at[1]),
        ]
        for i, (c, bw) in enumerate(blocks):
            copies.append(pltpu.make_async_copy(wq_ref.at[layer, :, pl.ds(c, bw)], w_ref.at[:, pl.ds(2 * width + c, bw)], w_sem.at[2 + i]))
        return copies

    norm.start(0)
    norm.start(1)
    for copy in loads():
        copy.start()
    meet()
    norm.run()
    norm.arrive()
    weights = loads()
    weights[0].wait()
    weights[1].wait()
    both = jnp.dot(x_ref[...], w_ref[:, :2 * width], preferred_element_type=F32)
    for i in range(nkv):
        kv_buf[:, i * HEAD:(i + 1) * HEAD] = rope(both[:, i * HEAD:(i + 1) * HEAD], cos_ref[...], sin_ref[...])
    kv_buf[:, width:] = both[:, width:].astype(BF)
    outs = [pltpu.make_async_copy(kv_buf, kv_ref, o_sem.at[0])]
    outs[0].start()
    for j, (c, bw) in enumerate(blocks):
        weights[2 + j].wait()
        acc = jnp.dot(x_ref[...], w_ref[:, 2 * width + c:2 * width + c + bw], preferred_element_type=F32)
        for i in range(bw // HEAD):
            q_buf[:, c + i * HEAD:c + (i + 1) * HEAD] = rope(acc[:, i * HEAD:(i + 1) * HEAD], cos_ref[...], sin_ref[...])
        outs.append(pltpu.make_async_copy(q_buf.at[:, pl.ds(c, bw)], q_ref.at[:, pl.ds(c, bw)], o_sem.at[1 + j]))
        outs[-1].start()
    norm.finish()
    for copy in outs:
        copy.wait()


def qkv(srcs, gain, wq, wk, wv, cos, sin, layer, nkv, rb):
    init = len(srcs) == 2
    d = wq.shape[1]
    half = 2 * srcs[0].shape[0] if init else srcs[0].shape[0]
    rows = 2 * half
    qcols = wq.shape[2]
    width = nkv * HEAD
    vmem = pl.BlockSpec(memory_space=pltpu.VMEM)
    n_w = 2 + len(qkv_blocks(qcols))
    return pl.pallas_call(
        functools.partial(qkv_kernel, init, layer, nkv, rb),
        in_specs=[any_spec()] * len(srcs) + [vmem, any_spec(), any_spec(), any_spec(), vmem, vmem],
        out_specs=[any_spec()] * 3,
        out_shape=[jax.ShapeDtypeStruct((half, d), BF), jax.ShapeDtypeStruct((rows, qcols), BF), jax.ShapeDtypeStruct((rows, 2 * width), BF)],
        scratch_shapes=[
            pltpu.VMEM((rows, d), BF),
            pltpu.VMEM((d, 2 * width + qcols), BF),
            pltpu.VMEM((rows, qcols), BF),
            pltpu.VMEM((rows, 2 * width), BF),
            pltpu.SemaphoreType.DMA((n_w,)),
            pltpu.SemaphoreType.DMA((n_w,)),
        ] + norm_scratch(half, d, rb, init),
        compiler_params=pltpu.CompilerParams(vmem_limit_bytes=48 * 1024 * 1024, collective_id=3 if init else 0, has_side_effects=True),
        cost_estimate=pl.CostEstimate(flops=2 * rows * d * (qcols + 2 * width), bytes_accessed=2 * d * (rows + qcols + 2 * width), transcendentals=0),
        name="qkv_init" if init else "qkv",
    )(*srcs, gain, wq, wk, wv, cos, sin)


SM_C = HEAD ** -0.5 * math.log2(math.e)


def lanes(x, width):
    return jnp.concatenate([x] * (width // HEAD), axis=1) if width > HEAD else x


def flash_step(qs, k, v, ok, m, l, acc):
    s = lax.dot_general(qs, k, (((1,), (1,)), ((), ())), preferred_element_type=F32) * SM_C
    if ok is not None:
        s = jnp.where(ok, s, NEG)
    _, width = s.shape
    m_new = jnp.maximum(m, jnp.max(s, axis=1, keepdims=True))
    alpha = jnp.exp2(m - m_new)
    p = jnp.exp2(s - lanes(m_new, width))
    part = p[:, :HEAD]
    for i in range(1, width // HEAD):
        part = part + p[:, i * HEAD:(i + 1) * HEAD]
    return m_new, l * alpha + part, acc * alpha + jnp.dot(p.astype(BF), v, preferred_element_type=F32)


def flash(q_rows, qi, ql, kv_ref, bk, nkv, group, lo, hi, m_ref, l_ref, acc_ref):
    rows = qi.shape[0]
    gr = group * rows
    ql_max = jnp.max(ql)
    qi_min = jnp.min(qi)
    qs = [jnp.concatenate([q_rows(kh * group + i) for i in range(group)], axis=0) for kh in range(nkv)]
    m_ref[:, :gr, :] = jnp.full((nkv, gr, HEAD), NEG, F32)
    l_ref[:, :gr, :] = jnp.zeros((nkv, gr, HEAD), F32)
    acc_ref[:, :gr, :] = jnp.zeros((nkv, gr, HEAD), F32)

    def step(j, masked):
        base = pl.multiple_of(j * bk, bk)
        ok = None
        if masked:
            kid = base + lax.broadcasted_iota(jnp.int32, (rows, bk), 1)
            ok = (kid <= qi) & (kid >= ql)
            ok = jnp.concatenate([ok] * group, axis=0)
        new = []
        for kh in range(nkv):
            k = kv_ref[pl.ds(base, bk), kh * HEAD:(kh + 1) * HEAD]
            v = kv_ref[pl.ds(base, bk), (nkv + kh) * HEAD:(nkv + kh + 1) * HEAD]
            new.append(flash_step(qs[kh], k, v, ok, m_ref[kh, :gr, :], l_ref[kh, :gr, :], acc_ref[kh, :gr, :]))
        for kh in range(nkv):
            m_ref[kh, :gr, :], l_ref[kh, :gr, :], acc_ref[kh, :gr, :] = new[kh]

    def body(j, carry):
        base = j * bk
        full = (ql_max <= base) & (qi_min >= base + bk - 1)

        @pl.when(full)
        def _():
            step(j, False)

        @pl.when(jnp.logical_not(full))
        def _():
            step(j, True)

        return carry

    lax.fori_loop(lo, hi, body, 0)
    outs = []
    for kh in range(nkv):
        total = jnp.sum(l_ref[kh, :gr, :], axis=1, keepdims=True)
        out = (acc_ref[kh, :gr, :] / total).astype(BF)
        outs += [out[i * rows:(i + 1) * rows, :] for i in range(group)]
    return outs


def attn_kernel(table, me, nkv, group, nb, na, bks, sc_ref, q_ref, qi_ref, ql_ref, *refs):
    n_kv = 4 * len(table)
    kv_hbm = refs[:n_kv]
    o_ref, kvb_ref, kva_ref, m_ref, l_ref, acc_ref, sem = refs[n_kv:]
    b, a = table[me]
    own = a + b
    t = lax.axis_index('tp')

    def copies():
        off_b, off_a = 0, 0
        out = []
        for k, (bk_, ak_) in enumerate(table):
            for s in range(4):
                for place in range(4):
                    owner = t ^ OWNER_XOR[place]
                    src = kv_hbm[4 * k + s]
                    row = place * (bk_ + ak_)
                    if b and bk_:
                        dst = pl.multiple_of((3 - s) * 4 * nb + owner * nb + off_b, 16)
                        out.append(pltpu.make_async_copy(src.at[pl.ds(row, bk_), :], kvb_ref.at[pl.ds(dst, bk_), :], sem))
                    if a and ak_:
                        dst = pl.multiple_of((3 - s) * 4 * na + owner * na + off_a, 16)
                        out.append(pltpu.make_async_copy(src.at[pl.ds(row + bk_, ak_), :], kva_ref.at[pl.ds(dst, ak_), :], sem))
            off_b += bk_
            off_a += ak_
        return out

    for copy in copies():
        copy.start()
    for copy in copies():
        copy.wait()
    if b:
        def one_owner(o, carry):
            r0 = pl.multiple_of(o * own, 16)
            q_rows = lambda h: q_ref[pl.ds(r0, b), h * HEAD:(h + 1) * HEAD]
            outs = flash(q_rows, qi_ref[pl.ds(r0, b), :1], ql_ref[pl.ds(r0, b), :1], kvb_ref, bks[0], nkv, group, sc_ref[o], sc_ref[4 + o], m_ref, l_ref, acc_ref)
            for h, out in enumerate(outs):
                o_ref[pl.ds(r0, b), h * HEAD:(h + 1) * HEAD] = out
            return carry

        lax.fori_loop(0, 4, one_owner, 0)
    if a:
        spans = [(o * own + b, o * own + b + a) for o in range(4)]
        gather = lambda ref, c0, c1: jnp.concatenate([ref[r0:r1, c0:c1] for r0, r1 in spans], axis=0)
        outs = flash(lambda h: gather(q_ref, h * HEAD, (h + 1) * HEAD), gather(qi_ref, 0, 1), gather(ql_ref, 0, 1), kva_ref, bks[1], nkv, group, sc_ref[8], sc_ref[9], m_ref, l_ref, acc_ref)
        for h, out in enumerate(outs):
            for o, (r0, r1) in enumerate(spans):
                o_ref[r0:r1, h * HEAD:(h + 1) * HEAD] = out[o * a:(o + 1) * a, :]


def attention(table, me, sc, q, qi, ql, kvs, nkv, group, nb, na, bks):
    rows, qcols = q.shape
    b, a = table[me]
    gr = group * max(4 * a, b)
    kvw = 2 * nkv * HEAD
    vmem = lambda: pl.BlockSpec(memory_space=pltpu.VMEM)
    flat = [x for per_chunk in kvs for x in per_chunk]
    flops = 4 * (4 * b * 16 * nb + 4 * a * 16 * na) * qcols
    return pl.pallas_call(
        functools.partial(attn_kernel, table, me, nkv, group, nb, na, bks),
        in_specs=[pl.BlockSpec(memory_space=pltpu.SMEM), vmem(), vmem(), vmem()] + [any_spec()] * len(flat),
        out_specs=vmem(),
        scratch_shapes=[
            pltpu.VMEM((16 * nb, kvw), BF),
            pltpu.VMEM((16 * na, kvw), BF),
            pltpu.VMEM((nkv, gr, HEAD), F32),
            pltpu.VMEM((nkv, gr, HEAD), F32),
            pltpu.VMEM((nkv, gr, HEAD), F32),
            pltpu.SemaphoreType.DMA,
        ],
        out_shape=jax.ShapeDtypeStruct((rows, qcols), BF),
        compiler_params=cparams(limit=40 * 1024 * 1024),
        cost_estimate=pl.CostEstimate(flops=flops, bytes_accessed=4 * rows * qcols + 32 * (nb + na) * kvw, transcendentals=0),
        name="attention",
    )(sc, q, qi, ql, *flat)


def oproj_kernel(layer, bn, o_ref, w_ref, so_ref, w_buf, w_sem, *scratch):
    chip = ChipSum([so_ref], scratch)

    def load(i):
        cols = pl.ds(i * bn, bn)
        return pltpu.make_async_copy(w_ref.at[layer, :, cols], w_buf.at[:, cols], w_sem.at[i])

    for i in range(chip.n):
        load(i).start()
    meet()
    for i in range(chip.n):
        load(i).wait()
        if i >= 1:
            chip.send(i - 1).start()
        if i >= 2:
            chip.store(i - 2)
        acc = jnp.dot(o_ref[...], w_buf[:, i * bn:(i + 1) * bn], preferred_element_type=F32)
        if i >= 1:
            chip.combine(i - 1)
        chip.keep(i, acc)
    chip.tail()


def oproj(o, wo, layer):
    rows, k = o.shape
    d = wo.shape[2]
    bn = min(1024, d // 2)
    half = rows // 2
    return pl.pallas_call(
        functools.partial(oproj_kernel, layer, bn),
        in_specs=[pl.BlockSpec(memory_space=pltpu.VMEM), any_spec()],
        out_specs=any_spec(),
        out_shape=jax.ShapeDtypeStruct((half, d), BF),
        scratch_shapes=[pltpu.VMEM((k, d), BF), pltpu.SemaphoreType.DMA((d // bn,))] + sum_scratch(half, d, bn),
        compiler_params=pltpu.CompilerParams(vmem_limit_bytes=40 * 1024 * 1024, collective_id=1, has_side_effects=True),
        cost_estimate=pl.CostEstimate(flops=2 * rows * k * d, bytes_accessed=2 * (rows * k + k * d + rows * d), transcendentals=0),
        name="oproj",
    )(o, wo)


def mlp_kernel(layer, bf, rb, n_out, *refs):
    srcs = refs[:3]
    gain_ref, wg_ref, wu_ref, wd_ref, ho_ref = refs[3:8]
    outs = refs[8:8 + n_out]
    x_ref, w_ref, wd_buf, both_ref, act_ref, w_sem, d_sem = refs[8 + n_out:15 + n_out]
    scratch = refs[15 + n_out:]
    norm = NormExchange(False, rb, srcs, gain_ref, ho_ref, x_ref, scratch[:7])
    chip = ChipSum(outs, scratch[7:])
    n_up = wg_ref.shape[2] // bf
    n_down = chip.n

    def up_copies(step, slot):
        cols = pl.ds(pl.multiple_of(step * bf, 128), bf)
        return (
            pltpu.make_async_copy(wg_ref.at[layer, :, cols], w_ref.at[slot, :, pl.ds(0, bf)], w_sem.at[slot, 0]),
            pltpu.make_async_copy(wu_ref.at[layer, :, cols], w_ref.at[slot, :, pl.ds(bf, bf)], w_sem.at[slot, 1]),
        )

    def down_copy(step, slot):
        return pltpu.make_async_copy(wd_ref.at[layer, :, chip.cols(step)], wd_buf.at[slot], d_sem.at[slot])

    def gated(slot, step):
        gate = both_ref[slot, :, :bf]
        act = gate * jax.nn.sigmoid(gate) * both_ref[slot, :, bf:]
        act_ref[:, pl.ds(pl.multiple_of(step * bf, 128), bf)] = act.astype(BF)

    norm.start(0)
    norm.start(1)
    for step in range(2):
        for copy in up_copies(step, step):
            copy.start()
    meet()
    norm.run()
    norm.arrive()

    def up(j, carry):
        slot = j % 2
        for copy in up_copies(j, slot):
            copy.wait()

        @pl.when(jnp.logical_and(j >= 1, j + 1 < n_up))
        def _():
            for copy in up_copies(j + 1, 1 - slot):
                copy.start()

        both = jnp.dot(x_ref[...], w_ref[slot], preferred_element_type=F32)

        @pl.when(j >= 1)
        def _():
            gated(1 - slot, j - 1)

        both_ref[slot] = both
        return carry

    lax.fori_loop(0, n_up, up, 0)
    for step in range(2):
        down_copy(step, step).start()
    gated((n_up - 1) % 2, n_up - 1)

    def down(i, carry):
        slot = i % 2
        down_copy(i, slot).wait()

        @pl.when(jnp.logical_and(i >= 1, i + 1 < n_down))
        def _():
            down_copy(i + 1, 1 - slot).start()

        @pl.when(i >= 1)
        def _():
            chip.send(i - 1).start()

        @pl.when(i >= 2)
        def _():
            chip.store(i - 2)

        acc = jnp.dot(act_ref[...], wd_buf[slot], preferred_element_type=F32)

        @pl.when(i >= 1)
        def _():
            chip.combine(i - 1)

        chip.keep(i, acc)
        return carry

    lax.fori_loop(0, n_down, down, 0)
    chip.tail()
    norm.finish()


def mlp(h, s, t, gain, wg, wu, wd, layer, rb, n_out):
    half, d = h.shape
    rows = 2 * half
    ff = wg.shape[2]
    bf = 384
    bn = min(512, d // 2)
    out = jax.ShapeDtypeStruct((half, d), BF)
    part = jax.ShapeDtypeStruct((half // n_out, d), BF)
    return pl.pallas_call(
        functools.partial(mlp_kernel, layer, bf, rb, n_out),
        in_specs=[any_spec()] * 3 + [pl.BlockSpec(memory_space=pltpu.VMEM)] + [any_spec()] * 3,
        out_specs=[any_spec()] * (1 + n_out),
        out_shape=[out] + [part] * n_out,
        scratch_shapes=[
            pltpu.VMEM((rows, d), BF),
            pltpu.VMEM((2, d, 2 * bf), BF),
            pltpu.VMEM((2, ff, bn), BF),
            pltpu.VMEM((2, rows, 2 * bf), F32),
            pltpu.VMEM((rows, ff), BF),
            pltpu.SemaphoreType.DMA((2, 2)),
            pltpu.SemaphoreType.DMA((2,)),
        ] + norm_scratch(half, d, rb, False) + sum_scratch(half, d, bn),
        compiler_params=pltpu.CompilerParams(vmem_limit_bytes=VMEM_LIMIT, collective_id=2, has_side_effects=True),
        cost_estimate=pl.CostEstimate(flops=6 * rows * d * ff, bytes_accessed=2 * (2 * rows * d + 3 * d * ff), transcendentals=rows * ff),
        name="mlp",
    )(h, s, t, gain, wg, wu, wd)


def solution(mesh):
    row_spec = P(('dp', 'pp', 'tp'), None)
    id_spec = P(('dp', 'pp', 'tp'))
    col_spec = P(None, None, 'tp')
    in_row_spec = P(None, 'tp', None)
    full_spec = P()
    n_pp = mesh.shape['pp']
    across_y = [(i, i ^ 2) for i in range(4)]

    def per_device(tok_a, seg_a, pos_a, tok_b, seg_b, pos_b, g_attn, wq, wk, wv, wo, g_mlp, wg, wu, wd):
        t = lax.axis_index('tp')
        p = lax.axis_index('pp')
        n_layers, _ = g_attn.shape
        nb, na = tok_b.shape[0], tok_a.shape[0]
        n_kv_all = wk.shape[2] // HEAD
        nkv = n_kv_all // 4
        group = wq.shape[2] // HEAD // nkv
        table = chunk_table(nb, na)
        n_chunks = len(table)
        owners = [t ^ x for x in OWNER_XOR]
        rb = 32 if nb == 256 else 16

        off_b, off_a, b0, a0 = [], [], 0, 0
        for b, a in table:
            off_b.append(b0)
            off_a.append(a0)
            b0, a0 = b0 + b, a0 + a
        gain_attn = [g_attn[l:l + 1] for l in range(n_layers)]
        gain_mlp = [g_mlp[l:l + 1] for l in range(n_layers)]

        own_rows = []
        for (b, a), ob, oa in zip(table, off_b, off_a):
            parts = [tok_b[ob:ob + b]] if b else []
            parts += [tok_a[oa:oa + a]] if a else []
            own_rows.append(parts[0] if len(parts) == 1 else jnp.concatenate(parts, axis=0))

        got_rows = [lax.ppermute(own_rows[k], 'tp', across_y) for k in range(n_chunks)]

        ints = jnp.concatenate([seg_b, pos_b, seg_a, pos_a])
        tp_ints = lax.all_gather(ints, 'tp').reshape(4, 2 * (nb + na))
        here = jnp.concatenate([lax.dynamic_index_in_dim(tp_ints, o, 0, keepdims=True) for o in owners], axis=0)
        below = jnp.stack([jnp.sum((seg < v).astype(jnp.int32)) for seg in (seg_b, seg_a) for v in range(4)])
        below = lax.psum(jnp.concatenate([below, jnp.zeros((120,), jnp.int32)]), ('pp', 'tp'))

        def request(base, n_own, which):
            seg = here[:, base:base + n_own]
            pos = here[:, base + n_own:base + 2 * n_own]
            starts = [below[4 * which + v] for v in range(4)]
            shift = (n_pp - 1 - p) * 4 * n_own
            lo = jnp.zeros_like(seg) + starts[0]
            for v in range(1, 4):
                lo = lo + jnp.where(seg >= v, starts[v] - starts[v - 1], 0)
            own_ids = jnp.stack(owners).astype(jnp.int32)[:, None] * n_own + jnp.arange(n_own, dtype=jnp.int32)[None, :]
            idx = own_ids + (n_pp - 1) * 4 * n_own
            return idx, lo + shift, pos

        idx_b, lo_b, pos_b_rows = request(0, nb, 0)
        idx_a, lo_a, pos_a_rows = request(2 * nb, na, 1)

        inv_freq = jnp.power(ROPE_BASE, -2.0 * jnp.arange(HEAD // 2, dtype=F32) / HEAD)

        def trig(pos):
            angles = pos.astype(F32)[..., None] * inv_freq
            cos, sin = jnp.cos(angles), jnp.sin(angles)
            return jnp.concatenate([cos, cos], axis=-1), jnp.concatenate([-sin, sin], axis=-1)

        cos_b, sin_b = trig(pos_b_rows)
        cos_a, sin_a = trig(pos_a_rows)

        cos, sin, q_idx, q_low, scal = [], [], [], [], []
        bk_b, bk_a = min(512, 16 * nb), min(512, 16 * na)
        for (b, a), ob, oa in zip(table, off_b, off_a):
            def pick(xb, xa):
                parts = ([xb[:, ob:ob + b]] if b else []) + ([xa[:, oa:oa + a]] if a else [])
                both = parts[0] if len(parts) == 1 else jnp.concatenate(parts, axis=1)
                return both.reshape((4 * (a + b),) + both.shape[2:])

            cos.append(pick(cos_b, cos_a))
            sin.append(pick(sin_b, sin_a))
            wide = lambda x: jnp.broadcast_to(x[:, None], (x.shape[0], HEAD))
            q_idx.append(wide(pick(idx_b, idx_a)))
            q_low.append(wide(pick(lo_b, lo_a)))
            zero = jnp.zeros((4,), jnp.int32)
            lo_blk_b = lo_b[:, ob] // bk_b if b else zero
            hi_blk_b = idx_b[:, ob + b - 1] // bk_b + 1 if b else zero
            lo_blk_a = jnp.min(lo_a[:, oa:oa + 1], axis=0) // bk_a if a else zero[:1]
            hi_blk_a = jnp.max(idx_a[:, oa + a - 1:oa + a], axis=0) // bk_a + 1 if a else zero[:1]
            scal.append(jnp.concatenate([lo_blk_b, hi_blk_b, lo_blk_a, hi_blk_a]).astype(jnp.int32))

        out_b, out_a = [], []
        srcs = list(zip(own_rows, got_rows))
        h = [None] * n_chunks
        for l in range(n_layers):
            q, kvs = [None] * n_chunks, [None] * n_chunks
            last = l + 1 == n_layers
            for k in range(n_chunks):
                h[k], q[k], kv = qkv(srcs[k], gain_attn[l], wq, wk, wv, cos[k], sin[k], l, nkv, rb)
                kvs[k] = [kv] + [lax.ppermute(kv, 'pp', [(i, i + s) for i in range(n_pp - s)]) for s in range(1, n_pp)]
            sums = []
            for k in range(n_chunks):
                o = attention(table, k, scal[k], q[k], q_idx[k], q_low[k], kvs, nkv, group, nb, na, (bk_b, bk_a))
                s = oproj(o, wo, l)
                sums.append((s, lax.ppermute(s, 'tp', across_y)))
            for k in range(n_chunks):
                h[k], *parts = mlp(h[k], *sums[k], gain_mlp[l], wg, wu, wd, l, rb, 2 if last else 1)
                got = lax.ppermute(parts[-1], 'tp', across_y)
                srcs[k] = (h[k], parts[0], got)
        for (b, a), (res, mine, got) in zip(table, srcs):
            res = (res[:a + b].astype(F32) + (mine.astype(F32) + got.astype(F32))).astype(BF)
            if b:
                out_b.append(res[:b])
            if a:
                out_a.append(res[b:])
        join = lambda parts: parts[0] if len(parts) == 1 else jnp.concatenate(parts, axis=0)
        return join(out_a), join(out_b)

    def prefill(tokens_a, segment_a, position_a, tokens_b, segment_b, position_b, norm_attn, w_query, w_key, w_value, w_out, norm_mlp, w_gate, w_up, w_down):
        mapped = jax.shard_map(per_device, mesh=mesh, in_specs=(row_spec, id_spec, id_spec, row_spec, id_spec, id_spec, full_spec, col_spec, full_spec, full_spec, in_row_spec, full_spec, col_spec, col_spec, in_row_spec), out_specs=(row_spec, row_spec), check_vma=False)
        return mapped(tokens_a, segment_a, position_a, tokens_b, segment_b, position_b, norm_attn, w_query, w_key, w_value, w_out, norm_mlp, w_gate, w_up, w_down)

    return prefill
```

```python
import functools
import math
import jax
import jax.numpy as jnp
from jax import lax
from jax.experimental import pallas as pl
from jax.experimental.pallas import tpu as pltpu
from jax.sharding import PartitionSpec as P

HEAD = 128
ROPE_BASE = 500000.0
EPS = 1e-5
NEG = -1e30
BF = jnp.bfloat16
F32 = jnp.float32
VMEM_LIMIT = 60 * 1024 * 1024
OWNER_XOR = (0, 2, 1, 3)


def chunk_table(nb, na):
    if nb == 256:
        return [(64, 32), (112, 0), (80, 0)]
    return [(nb // 2, na), (nb // 2, 0)]


def cparams(semantics=None, limit=VMEM_LIMIT):
    return pltpu.CompilerParams(dimension_semantics=semantics, vmem_limit_bytes=limit)


def hbm():
    return pl.BlockSpec(memory_space=pltpu.HBM)


MESH = pl.DeviceIdType.MESH


def other_core():
    t = lax.axis_index('tp')
    return {'tp': t + 1 - 2 * (t % 2)}


def meet():
    barrier = pltpu.get_barrier_semaphore()
    pl.semaphore_signal(barrier, inc=1, device_id=other_core(), device_id_type=MESH)
    pl.semaphore_wait(barrier, 1)


def norm_rows(wide, gain):
    inv = lax.rsqrt(jnp.mean(wide * wide, axis=-1, keepdims=True) + EPS)
    return (wide * inv * gain).astype(BF)


def norm_scratch(half, d, rb, init):
    n = half // rb
    bufs = [pltpu.VMEM((half, d), BF)] * (1 if init else 3)
    return bufs + [pltpu.VMEM((1, d), BF), pltpu.SemaphoreType.DMA((2, 4)), pltpu.SemaphoreType.DMA((n,)), pltpu.SemaphoreType.DMA((n,)), pltpu.SemaphoreType.DMA]


class NormExchange:
    def __init__(self, init, rb, srcs, gain_ref, ho_ref, x_ref, scratch):
        self.init, self.rb, self.srcs, self.gain_ref, self.ho_ref, self.x_ref = init, rb, srcs, gain_ref, ho_ref, x_ref
        self.bufs = scratch[:1 if init else 3]
        self.gain_buf, self.in_sem, self.send_sem, self.recv_sem, self.out_sem = scratch[1 if init else 3:]
        self.half = x_ref.shape[0] // 2
        self.own = self.half // 2
        self.n = self.half // rb

    def gain(self, piece):
        return [] if piece else [pltpu.make_async_copy(self.gain_ref, self.gain_buf, self.in_sem.at[0, 3])]

    def loads(self, piece):
        q = self.own
        dst = pl.ds(piece * q, q)
        if self.init:
            return self.gain(piece) + [pltpu.make_async_copy(self.srcs[piece], self.bufs[0].at[dst, :], self.in_sem.at[piece, 0])]
        src = (dst, dst, pl.ds((1 - piece) * q, q))
        return self.gain(piece) + [pltpu.make_async_copy(ref.at[rows, :], buf.at[dst, :], self.in_sem.at[piece, i]) for i, (ref, rows, buf) in enumerate(zip(self.srcs, src, self.bufs))]

    def send(self, i):
        rows = pl.ds(pl.multiple_of(i * self.rb, self.rb), self.rb)
        there = pl.ds(pl.multiple_of(self.half + i * self.rb, self.rb), self.rb)
        return pltpu.make_async_remote_copy(src_ref=self.x_ref.at[rows, :], dst_ref=self.x_ref.at[there, :], send_sem=self.send_sem.at[i], recv_sem=self.recv_sem.at[i], device_id=other_core(), device_id_type=MESH)

    def store(self):
        return pltpu.make_async_copy(self.bufs[0], self.ho_ref, self.out_sem)

    def start(self, piece):
        for copy in self.loads(piece):
            copy.start()

    def run(self, after_first):
        per = self.n // 2

        def block(i, carry):
            rows = pl.ds(pl.multiple_of(i * self.rb, self.rb), self.rb)
            if self.init:
                h = self.bufs[0][rows, :]
            else:
                hb, sb, tb = self.bufs
                h = (hb[rows, :].astype(F32) + (sb[rows, :].astype(F32) + tb[rows, :].astype(F32))).astype(BF)
                hb[rows, :] = h
            self.x_ref[rows, :] = norm_rows(h.astype(F32), self.gain_buf[...].astype(F32))

            @pl.when(i >= 1)
            def _():
                self.send(i - 1).start()

            return carry

        for piece in range(2):
            for copy in self.loads(piece):
                copy.wait()
            if piece == 0:
                after_first()
            lax.fori_loop(piece * per, (piece + 1) * per, block, 0)
        self.store().start()
        self.send(self.n - 1).start()

    def arrive(self):
        for i in range(self.n):
            self.send(i).wait_recv()

    def finish(self):
        for i in range(self.n):
            self.send(i).wait_send()
        self.store().wait()


def sum_scratch(half, d, bn):
    n = d // bn
    return [
        pltpu.VMEM((3, half, bn), F32),
        pltpu.VMEM((n, half, bn), BF),
        pltpu.VMEM((n, half, bn), BF),
        pltpu.VMEM((half, d), BF),
        pltpu.SemaphoreType.DMA((n,)),
        pltpu.SemaphoreType.DMA((n,)),
        pltpu.SemaphoreType.DMA((n,)),
    ]


class ChipSum:
    def __init__(self, outs, scratch):
        self.outs = outs
        self.mine, self.give, self.got, self.total, self.send_sem, self.recv_sem, self.out_sem = scratch
        self.n, self.half, self.bn = self.give.shape

    def send(self, i):
        return pltpu.make_async_remote_copy(src_ref=self.give.at[i], dst_ref=self.got.at[i], send_sem=self.send_sem.at[i], recv_sem=self.recv_sem.at[i], device_id=other_core(), device_id_type=MESH)

    def cols(self, i):
        return pl.ds(pl.multiple_of(i * self.bn, 128), self.bn)

    def stores(self, i):
        rows = self.half // len(self.outs)
        return [pltpu.make_async_copy(self.total.at[pl.ds(r * rows, rows), self.cols(i)], out.at[:, self.cols(i)], self.out_sem.at[i]) for r, out in enumerate(self.outs)]

    def keep(self, i, acc):
        self.mine[i % 3] = acc[:self.half]
        self.give[i] = acc[self.half:].astype(BF)

    def combine(self, i):
        self.send(i).wait_recv()
        self.total[:, self.cols(i)] = (self.mine[i % 3] + self.got[i].astype(F32)).astype(BF)

    def store(self, i):
        for copy in self.stores(i):
            copy.start()

    def tail(self):
        last = self.n - 1
        self.send(last).start()
        if self.n >= 3:
            self.store(last - 2)
        self.combine(last - 1)
        self.store(last - 1)
        self.combine(last)
        self.store(last)
        for i in range(self.n):
            self.send(i).wait_send()
            for copy in self.stores(i):
                copy.wait()


def rope(vals, cos, sin):
    return (vals * cos + pltpu.roll(vals, HEAD // 2, 1) * sin).astype(BF)


def qkv_blocks(qcols):
    blocks, c = [], 0
    while c < qcols:
        width = min(512, qcols - c)
        blocks.append((c, width))
        c += width
    return blocks


def qkv_kernel(init, layer, nkv, rb, *refs):
    n_src = 2 if init else 3
    srcs = refs[:n_src]
    gain_ref, wq_ref, wk_ref, wv_ref, cos_hbm, sin_hbm, ho_ref, q_ref, kv_ref, x_ref, w_ref, q_buf, kv_buf, cos_ref, sin_ref, w_sem, o_sem = refs[n_src:n_src + 17]
    norm = NormExchange(init, rb, srcs, gain_ref, ho_ref, x_ref, refs[n_src + 17:])
    half = x_ref.shape[0] // 2
    width = nkv * HEAD
    blocks = qkv_blocks(q_buf.shape[1])
    t = lax.axis_index('tp')

    def loads():
        cols = pl.ds(pl.multiple_of(t * width, 128), width)
        copies = [
            pltpu.make_async_copy(wk_ref.at[layer, :, cols], w_ref.at[:, pl.ds(0, width)], w_sem.at[0]),
            pltpu.make_async_copy(wv_ref.at[layer, :, cols], w_ref.at[:, pl.ds(width, width)], w_sem.at[1]),
        ]
        for i, (c, bw) in enumerate(blocks):
            copies.append(pltpu.make_async_copy(wq_ref.at[layer, :, pl.ds(c, bw)], w_ref.at[:, pl.ds(2 * width + c, bw)], w_sem.at[2 + i]))
        copies.append(pltpu.make_async_copy(cos_hbm, cos_ref, w_sem.at[2 + len(blocks)]))
        copies.append(pltpu.make_async_copy(sin_hbm, sin_ref, w_sem.at[3 + len(blocks)]))
        return copies

    weights = loads()

    def start_weights():
        for copy in weights:
            copy.start()

    norm.start(0)
    norm.start(1)
    meet()
    norm.run(start_weights)
    for copy in weights[-2:] + weights[:2]:
        copy.wait()

    def kv_rows(r0, r1):
        both = jnp.dot(x_ref[r0:r1, :], w_ref[:, :2 * width], preferred_element_type=F32)
        for i in range(nkv):
            kv_buf[r0:r1, i * HEAD:(i + 1) * HEAD] = rope(both[:, i * HEAD:(i + 1) * HEAD], cos_ref[r0:r1, :], sin_ref[r0:r1, :])
        kv_buf[r0:r1, width:] = both[:, width:].astype(BF)

    kv_rows(0, half)
    norm.arrive()
    kv_rows(half, 2 * half)
    outs = [pltpu.make_async_copy(kv_buf, kv_ref, o_sem.at[0])]
    outs[0].start()
    for j, (c, bw) in enumerate(blocks):
        weights[2 + j].wait()
        acc = jnp.dot(x_ref[...], w_ref[:, 2 * width + c:2 * width + c + bw], preferred_element_type=F32)
        for i in range(bw // HEAD):
            q_buf[:, c + i * HEAD:c + (i + 1) * HEAD] = rope(acc[:, i * HEAD:(i + 1) * HEAD], cos_ref[...], sin_ref[...])
        outs.append(pltpu.make_async_copy(q_buf.at[:, pl.ds(c, bw)], q_ref.at[:, pl.ds(c, bw)], o_sem.at[1 + j]))
        outs[-1].start()
    norm.finish()
    for copy in outs:
        copy.wait()


def qkv(srcs, gain, wq, wk, wv, cos, sin, layer, nkv, rb):
    init = len(srcs) == 2
    d = wq.shape[1]
    half = 2 * srcs[0].shape[0] if init else srcs[0].shape[0]
    rows = 2 * half
    qcols = wq.shape[2]
    width = nkv * HEAD
    n_w = 4 + len(qkv_blocks(qcols))
    return pl.pallas_call(
        functools.partial(qkv_kernel, init, layer, nkv, rb),
        in_specs=[hbm()] * len(srcs) + [hbm()] * 6,
        out_specs=[hbm()] * 3,
        out_shape=[jax.ShapeDtypeStruct((half, d), BF), jax.ShapeDtypeStruct((rows, qcols), BF), jax.ShapeDtypeStruct((rows, 2 * width), BF)],
        scratch_shapes=[
            pltpu.VMEM((rows, d), BF),
            pltpu.VMEM((d, 2 * width + qcols), BF),
            pltpu.VMEM((rows, qcols), BF),
            pltpu.VMEM((rows, 2 * width), BF),
            pltpu.VMEM((rows, HEAD), F32),
            pltpu.VMEM((rows, HEAD), F32),
            pltpu.SemaphoreType.DMA((n_w,)),
            pltpu.SemaphoreType.DMA((n_w,)),
        ] + norm_scratch(half, d, rb, init),
        compiler_params=pltpu.CompilerParams(vmem_limit_bytes=48 * 1024 * 1024, collective_id=3 if init else 0, has_side_effects=True),
        cost_estimate=pl.CostEstimate(flops=2 * rows * d * (qcols + 2 * width), bytes_accessed=2 * d * (rows + qcols + 2 * width), transcendentals=0),
        name="qkv_init" if init else "qkv",
    )(*srcs, gain, wq, wk, wv, cos, sin)


SM_C = HEAD ** -0.5 * math.log2(math.e)


def lanes(x, width):
    return jnp.concatenate([x] * (width // HEAD), axis=1) if width > HEAD else x


def flash_step(qs, k, v, ok, m, l, acc):
    s = lax.dot_general(qs, k, (((1,), (1,)), ((), ())), preferred_element_type=F32) * SM_C
    if ok is not None:
        s = jnp.where(ok, s, NEG)
    _, width = s.shape
    m_new = jnp.maximum(m, jnp.max(s, axis=1, keepdims=True))
    alpha = jnp.exp2(m - m_new)
    p = jnp.exp2(s - lanes(m_new, width))
    part = p[:, :HEAD]
    for i in range(1, width // HEAD):
        part = part + p[:, i * HEAD:(i + 1) * HEAD]
    return m_new, l * alpha + part, acc * alpha + jnp.dot(p.astype(BF), v, preferred_element_type=F32)


def flash(q_rows, qi, ql, qi_min, ql_max, kv_ref, bk, nkv, group, lo, hi, m_ref, l_ref, acc_ref):
    rows = qi.shape[0]
    gr = group * rows
    qs = [jnp.concatenate([q_rows(kh * group + i) for i in range(group)], axis=0) for kh in range(nkv)]
    m_ref[:, :gr, :] = jnp.full((nkv, gr, HEAD), NEG, F32)
    l_ref[:, :gr, :] = jnp.zeros((nkv, gr, HEAD), F32)
    acc_ref[:, :gr, :] = jnp.zeros((nkv, gr, HEAD), F32)

    def step(j, masked):
        base = pl.multiple_of(j * bk, bk)
        ok = None
        if masked:
            kid = base + lax.broadcasted_iota(jnp.int32, (rows, bk), 1)
            ok = (kid <= qi) & (kid >= ql)
            ok = jnp.concatenate([ok] * group, axis=0)
        new = []
        for kh in range(nkv):
            k = kv_ref[pl.ds(base, bk), kh * HEAD:(kh + 1) * HEAD]
            v = kv_ref[pl.ds(base, bk), (nkv + kh) * HEAD:(nkv + kh + 1) * HEAD]
            new.append(flash_step(qs[kh], k, v, ok, m_ref[kh, :gr, :], l_ref[kh, :gr, :], acc_ref[kh, :gr, :]))
        for kh in range(nkv):
            m_ref[kh, :gr, :], l_ref[kh, :gr, :], acc_ref[kh, :gr, :] = new[kh]

    def body(j, carry):
        base = j * bk
        full = (ql_max <= base) & (qi_min >= base + bk - 1)

        @pl.when(full)
        def _():
            step(j, False)

        @pl.when(jnp.logical_not(full))
        def _():
            step(j, True)

        return carry

    lax.fori_loop(lo, hi, body, 0)
    outs = []
    for kh in range(nkv):
        total = jnp.sum(l_ref[kh, :gr, :], axis=1, keepdims=True)
        out = (acc_ref[kh, :gr, :] / total).astype(BF)
        outs += [out[i * rows:(i + 1) * rows, :] for i in range(group)]
    return outs


def attn_kernel(table, me, nkv, group, nb, na, bks, sc_ref, q_hbm, *refs):
    n_kv = 4 * len(table)
    kv_hbm = refs[:n_kv]
    o_ref, q_ref, kvb_ref, kva_ref, m_ref, l_ref, acc_ref, sem, q_sem = refs[n_kv:]
    b, a = table[me]
    own = a + b
    t = lax.axis_index('tp')
    p = lax.axis_index('pp')
    load_q = pltpu.make_async_copy(q_hbm, q_ref, q_sem)
    load_q.start()

    def copies(s):
        off_b, off_a = 0, 0
        out = []
        for k, (bk_, ak_) in enumerate(table):
            for place in range(4):
                owner = t ^ OWNER_XOR[place]
                src = kv_hbm[4 * k + s]
                row = place * (bk_ + ak_)
                if b and bk_:
                    dst = pl.multiple_of((3 - s) * 4 * nb + owner * nb + off_b, 16)
                    out.append(pltpu.make_async_copy(src.at[pl.ds(row, bk_), :], kvb_ref.at[pl.ds(dst, bk_), :], sem))
                if a and ak_:
                    dst = pl.multiple_of((3 - s) * 4 * na + owner * na + off_a, 16)
                    out.append(pltpu.make_async_copy(src.at[pl.ds(row + bk_, ak_), :], kva_ref.at[pl.ds(dst, ak_), :], sem))
            off_b += bk_
            off_a += ak_
        return out

    for s in range(4):
        for copy in copies(s):
            copy.start()
    load_q.wait()
    for s in range(4):
        for copy in copies(s):
            copy.wait()

    def first_key(which, n_own):
        return [sc_ref[4 * which + v] + (3 - p) * 4 * n_own for v in range(4)]

    def lowest(starts, idx):
        low = jnp.zeros_like(idx) + starts[0]
        for v in range(1, 4):
            low = jnp.where(idx >= starts[v], starts[v], low)
        return low

    offs = [(sum(x[0] for x in table[:me])), (sum(x[1] for x in table[:me]))]
    if b:
        starts_b = first_key(0, nb)

        def one_owner(o, carry):
            r0 = pl.multiple_of(o * own, 16)
            owner = t ^ (2 * (o % 2) + o // 2)
            i0 = 12 * nb + owner * nb + offs[0]
            low0 = starts_b[0]
            for v in range(1, 4):
                low0 = jnp.where(i0 >= starts_b[v], starts_b[v], low0)
            idx = i0 + lax.broadcasted_iota(jnp.int32, (b, 1), 0)
            low = lowest(starts_b, idx)
            last_low = jnp.where(i0 + b - 1 >= starts_b[1], starts_b[1], starts_b[0])
            for v in range(2, 4):
                last_low = jnp.where(i0 + b - 1 >= starts_b[v], starts_b[v], last_low)
            q_rows = lambda h: q_ref[pl.ds(r0, b), h * HEAD:(h + 1) * HEAD]
            outs = flash(q_rows, idx, low, i0, last_low, kvb_ref, bks[0], nkv, group, low0 // bks[0], (i0 + b - 1) // bks[0] + 1, m_ref, l_ref, acc_ref)
            for h, out in enumerate(outs):
                o_ref[pl.ds(r0, b), h * HEAD:(h + 1) * HEAD] = out
            return carry

        lax.fori_loop(0, 4, one_owner, 0)
    if a:
        starts_a = first_key(1, na)
        idx = jnp.concatenate([12 * na + (t ^ OWNER_XOR[o]) * na + offs[1] + lax.broadcasted_iota(jnp.int32, (a, 1), 0) for o in range(4)], axis=0)
        low = lowest(starts_a, idx)
        spans = [(o * own + b, o * own + b + a) for o in range(4)]
        gather = lambda c0, c1: jnp.concatenate([q_ref[r0:r1, c0:c1] for r0, r1 in spans], axis=0)
        n_blocks = 16 * na // bks[1]
        outs = flash(lambda h: gather(h * HEAD, (h + 1) * HEAD), idx, low, 0, 16 * na, kva_ref, bks[1], nkv, group, starts_a[0] // bks[1], n_blocks, m_ref, l_ref, acc_ref)
        for h, out in enumerate(outs):
            for o, (r0, r1) in enumerate(spans):
                o_ref[r0:r1, h * HEAD:(h + 1) * HEAD] = out[o * a:(o + 1) * a, :]


def attention(table, me, sc, q, kvs, nkv, group, nb, na, bks):
    rows, qcols = q.shape
    b, a = table[me]
    gr = group * max(4 * a, b)
    kvw = 2 * nkv * HEAD
    flat = [x for per_chunk in kvs for x in per_chunk]
    flops = 4 * (4 * b * 16 * nb + 4 * a * 16 * na) * qcols
    return pl.pallas_call(
        functools.partial(attn_kernel, table, me, nkv, group, nb, na, bks),
        in_specs=[pl.BlockSpec(memory_space=pltpu.SMEM), hbm()] + [hbm()] * len(flat),
        out_specs=pl.BlockSpec(memory_space=pltpu.VMEM),
        scratch_shapes=[
            pltpu.VMEM((rows, qcols), BF),
            pltpu.VMEM((16 * nb, kvw), BF),
            pltpu.VMEM((16 * na, kvw), BF),
            pltpu.VMEM((nkv, gr, HEAD), F32),
            pltpu.VMEM((nkv, gr, HEAD), F32),
            pltpu.VMEM((nkv, gr, HEAD), F32),
            pltpu.SemaphoreType.DMA,
            pltpu.SemaphoreType.DMA,
        ],
        out_shape=jax.ShapeDtypeStruct((rows, qcols), BF),
        compiler_params=cparams(limit=40 * 1024 * 1024),
        cost_estimate=pl.CostEstimate(flops=flops, bytes_accessed=4 * rows * qcols + 32 * (nb + na) * kvw, transcendentals=0),
        name="attention",
    )(sc, q, *flat)


def oproj_kernel(layer, bn, o_hbm, w_ref, so_ref, o_ref, w_buf, w_sem, *scratch):
    chip = ChipSum([so_ref], scratch)
    loads = [pltpu.make_async_copy(w_ref.at[layer, :, pl.ds(i * bn, bn)], w_buf.at[:, pl.ds(i * bn, bn)], w_sem.at[i]) for i in range(chip.n)]
    load_o = pltpu.make_async_copy(o_hbm, o_ref, w_sem.at[chip.n])
    load_o.start()
    for copy in loads:
        copy.start()
    meet()
    load_o.wait()
    for i in range(chip.n):
        loads[i].wait()
        if i >= 1:
            chip.send(i - 1).start()
        if i >= 3:
            chip.store(i - 3)
        acc = jnp.dot(o_ref[...], w_buf[:, i * bn:(i + 1) * bn], preferred_element_type=F32)
        if i >= 2:
            chip.combine(i - 2)
        chip.keep(i, acc)
    chip.tail()


def oproj(o, wo, layer):
    rows, k = o.shape
    d = wo.shape[2]
    bn = min(1024, d // 2)
    half = rows // 2
    return pl.pallas_call(
        functools.partial(oproj_kernel, layer, bn),
        in_specs=[hbm(), hbm()],
        out_specs=hbm(),
        out_shape=jax.ShapeDtypeStruct((half, d), BF),
        scratch_shapes=[pltpu.VMEM((rows, k), BF), pltpu.VMEM((k, d), BF), pltpu.SemaphoreType.DMA((d // bn + 1,))] + sum_scratch(half, d, bn),
        compiler_params=pltpu.CompilerParams(vmem_limit_bytes=40 * 1024 * 1024, collective_id=1, has_side_effects=True),
        cost_estimate=pl.CostEstimate(flops=2 * rows * k * d, bytes_accessed=2 * (rows * k + k * d + rows * d), transcendentals=0),
        name="oproj",
    )(o, wo)


def mlp_kernel(layer, bf, bn, rb, n_out, *refs):
    srcs = refs[:3]
    gain_ref, wg_ref, wu_ref, wd_ref, ho_ref = refs[3:8]
    outs = refs[8:8 + n_out]
    x_ref, w_ref, both_ref, act_ref, w_sem = refs[8 + n_out:13 + n_out]
    scratch = refs[13 + n_out:]
    norm = NormExchange(False, rb, srcs, gain_ref, ho_ref, x_ref, scratch[:8])
    chip = ChipSum(outs, scratch[8:])
    ff = wg_ref.shape[2]
    n_up = ff // bf
    n_down = chip.n
    half = x_ref.shape[0] // 2

    def up_copies(step):
        slot = step % 3
        cols = pl.ds(pl.multiple_of(step * bf, 128), bf)
        return (
            pltpu.make_async_copy(wg_ref.at[layer, :, cols], w_ref.at[slot, pl.ds(0, wg_ref.shape[1]), pl.ds(0, bf)], w_sem.at[slot, 0]),
            pltpu.make_async_copy(wu_ref.at[layer, :, cols], w_ref.at[slot, pl.ds(0, wg_ref.shape[1]), pl.ds(bf, bf)], w_sem.at[slot, 1]),
        )

    def down_copy(step):
        slot = (step + n_up) % 3
        return pltpu.make_async_copy(wd_ref.at[layer, :, chip.cols(step)], w_ref.at[slot, pl.ds(0, ff), pl.ds(0, bn)], w_sem.at[slot, 0])

    def gated(step):
        slot = step % 2
        gate = both_ref[slot, :, :bf]
        act = gate * jax.nn.sigmoid(gate) * both_ref[slot, :, bf:]
        act_ref[:, pl.ds(pl.multiple_of(step * bf, 128), bf)] = act.astype(BF)

    def start_up(step):
        for copy in up_copies(step):
            copy.start()

    def wait_up(step):
        for copy in up_copies(step):
            copy.wait()

    norm.start(0)
    norm.start(1)
    meet()
    norm.run(lambda: start_up(0))
    start_up(1)
    wait_up(0)
    start_up(2) if n_up > 2 else down_copy(0).start()
    both_ref[0, :half, :] = jnp.dot(x_ref[:half, :], w_ref[0, :x_ref.shape[1], :], preferred_element_type=F32)
    norm.arrive()
    both_ref[0, half:, :] = jnp.dot(x_ref[half:, :], w_ref[0, :x_ref.shape[1], :], preferred_element_type=F32)

    def up(j, carry):
        wait_up(j)

        @pl.when(j + 2 < n_up)
        def _():
            start_up(j + 2)

        @pl.when(j + 2 >= n_up)
        def _():
            down_copy(j + 2 - n_up).start()

        gated(j - 1)
        both_ref[j % 2] = jnp.dot(x_ref[...], w_ref[j % 3, :x_ref.shape[1], :], preferred_element_type=F32)
        return carry

    lax.fori_loop(1, n_up, up, 0)
    gated(n_up - 1)

    def down(i, carry):
        down_copy(i).wait()

        @pl.when(i + 2 < n_down)
        def _():
            down_copy(i + 2).start()

        @pl.when(i >= 1)
        def _():
            chip.send(i - 1).start()

        @pl.when(i >= 3)
        def _():
            chip.store(i - 3)

        acc = jnp.dot(act_ref[...], w_ref[(i + n_up) % 3, :ff, :bn], preferred_element_type=F32)

        @pl.when(i >= 2)
        def _():
            chip.combine(i - 2)

        chip.keep(i, acc)
        return carry

    lax.fori_loop(0, n_down, down, 0)
    chip.tail()
    norm.finish()


def mlp(h, s, t, gain, wg, wu, wd, layer, rb, n_out):
    half, d = h.shape
    rows = 2 * half
    ff = wg.shape[2]
    bf = 384
    bn = min(512, d // 2)
    out = jax.ShapeDtypeStruct((half, d), BF)
    part = jax.ShapeDtypeStruct((half // n_out, d), BF)
    return pl.pallas_call(
        functools.partial(mlp_kernel, layer, bf, bn, rb, n_out),
        in_specs=[hbm()] * 7,
        out_specs=[hbm()] * (1 + n_out),
        out_shape=[out] + [part] * n_out,
        scratch_shapes=[
            pltpu.VMEM((rows, d), BF),
            pltpu.VMEM((3, max(d, ff), 2 * bf), BF),
            pltpu.VMEM((2, rows, 2 * bf), F32),
            pltpu.VMEM((rows, ff), BF),
            pltpu.SemaphoreType.DMA((3, 2)),
        ] + norm_scratch(half, d, rb, False) + sum_scratch(half, d, bn),
        compiler_params=pltpu.CompilerParams(vmem_limit_bytes=VMEM_LIMIT, collective_id=2, has_side_effects=True),
        cost_estimate=pl.CostEstimate(flops=6 * rows * d * ff, bytes_accessed=2 * (2 * rows * d + 3 * d * ff), transcendentals=rows * ff),
        name="mlp",
    )(h, s, t, gain, wg, wu, wd)


def solution(mesh):
    row_spec = P(('dp', 'pp', 'tp'), None)
    id_spec = P(('dp', 'pp', 'tp'))
    col_spec = P(None, None, 'tp')
    in_row_spec = P(None, 'tp', None)
    full_spec = P()
    n_pp = mesh.shape['pp']
    across_core = [(i, i ^ 1) for i in range(4)]
    across_y = [(i, i ^ 2) for i in range(4)]

    def per_device(tok_a, seg_a, pos_a, tok_b, seg_b, pos_b, g_attn, wq, wk, wv, wo, g_mlp, wg, wu, wd):
        n_layers, _ = g_attn.shape
        nb, na = tok_b.shape[0], tok_a.shape[0]
        n_kv_all = wk.shape[2] // HEAD
        nkv = n_kv_all // 4
        group = wq.shape[2] // HEAD // nkv
        table = chunk_table(nb, na)
        n_chunks = len(table)
        rb = 16

        off_b, off_a, b0, a0 = [], [], 0, 0
        for b, a in table:
            off_b.append(b0)
            off_a.append(a0)
            b0, a0 = b0 + b, a0 + a
        gain_attn = [g_attn[l:l + 1] for l in range(n_layers)]
        gain_mlp = [g_mlp[l:l + 1] for l in range(n_layers)]

        own_rows = []
        for (b, a), ob, oa in zip(table, off_b, off_a):
            parts = [tok_b[ob:ob + b]] if b else []
            parts += [tok_a[oa:oa + a]] if a else []
            own_rows.append(parts[0] if len(parts) == 1 else jnp.concatenate(parts, axis=0))

        below = jnp.stack([jnp.sum((seg < v).astype(jnp.int32)) for seg in (seg_b, seg_a) for v in range(4)])
        ints = jnp.concatenate([pos_b, pos_a, below, jnp.zeros((512 - nb - na - 8,), jnp.int32)])
        ints_y = lax.ppermute(ints, 'tp', across_y)
        got_rows = [lax.ppermute(own_rows[k], 'tp', across_y) for k in range(n_chunks)]
        pair = jnp.stack([ints, ints_y])
        pair_c = lax.ppermute(pair, 'tp', across_core)
        ids = jnp.concatenate([pair, pair_c], axis=0)
        below = jnp.sum(ids[:, nb + na:nb + na + 8], axis=0)
        pos_b_rows, pos_a_rows = ids[:, :nb], ids[:, nb:nb + na]
        others = [lax.ppermute(below, 'pp', [(i, (i + s) % n_pp) for i in range(n_pp)]) for s in range(1, n_pp)]
        starts = below + others[0] + others[1] + others[2]

        inv_freq = jnp.power(ROPE_BASE, -2.0 * jnp.arange(HEAD // 2, dtype=F32) / HEAD)

        def trig(pos):
            angles = pos.astype(F32)[..., None] * inv_freq
            cos, sin = jnp.cos(angles), jnp.sin(angles)
            return jnp.concatenate([cos, cos], axis=-1), jnp.concatenate([-sin, sin], axis=-1)

        cos_b, sin_b = trig(pos_b_rows)
        cos_a, sin_a = trig(pos_a_rows)

        cos, sin = [], []
        bk_b, bk_a = min(512, 16 * nb), min(512, 16 * na)
        for (b, a), ob, oa in zip(table, off_b, off_a):
            def pick(xb, xa):
                parts = ([xb[:, ob:ob + b]] if b else []) + ([xa[:, oa:oa + a]] if a else [])
                both = parts[0] if len(parts) == 1 else jnp.concatenate(parts, axis=1)
                return both.reshape((4 * (a + b),) + both.shape[2:])

            cos.append(pick(cos_b, cos_a))
            sin.append(pick(sin_b, sin_a))

        out_b, out_a = [], []
        srcs = list(zip(own_rows, got_rows))
        h = [None] * n_chunks
        for l in range(n_layers):
            q, kvs = [None] * n_chunks, [None] * n_chunks
            last = l + 1 == n_layers
            for k in range(n_chunks):
                h[k], q[k], kv = qkv(srcs[k], gain_attn[l], wq, wk, wv, cos[k], sin[k], l, nkv, rb)
                kvs[k] = [kv]
                for s in range(1, n_pp):
                    if k + 1 < n_chunks:
                        kvs[k].append(lax.ppermute(kvs[k][-1], 'pp', [(i, i + 1) for i in range(s - 1, n_pp - 1)]))
                    else:
                        kvs[k].append(lax.ppermute(kv, 'pp', [(i, i + s) for i in range(n_pp - s)]))
            sums = []
            for k in range(n_chunks):
                o = attention(table, k, starts, q[k], kvs, nkv, group, nb, na, (bk_b, bk_a))
                s = oproj(o, wo, l)
                sums.append((s, lax.ppermute(s, 'tp', across_y)))
            for k in range(n_chunks):
                h[k], *parts = mlp(h[k], *sums[k], gain_mlp[l], wg, wu, wd, l, rb, 2 if last else 1)
                got = lax.ppermute(parts[-1], 'tp', across_y)
                srcs[k] = (h[k], parts[0], got)
        for (b, a), (res, mine, got) in zip(table, srcs):
            res = (res[:a + b].astype(F32) + (mine.astype(F32) + got.astype(F32))).astype(BF)
            if b:
                out_b.append(res[:b])
            if a:
                out_a.append(res[b:])
        join = lambda parts: parts[0] if len(parts) == 1 else jnp.concatenate(parts, axis=0)
        return join(out_a), join(out_b)

    def prefill(tokens_a, segment_a, position_a, tokens_b, segment_b, position_b, norm_attn, w_query, w_key, w_value, w_out, norm_mlp, w_gate, w_up, w_down):
        mapped = jax.shard_map(per_device, mesh=mesh, in_specs=(row_spec, id_spec, id_spec, row_spec, id_spec, id_spec, full_spec, col_spec, full_spec, full_spec, in_row_spec, full_spec, col_spec, col_spec, in_row_spec), out_specs=(row_spec, row_spec), check_vma=False)
        return mapped(tokens_a, segment_a, position_a, tokens_b, segment_b, position_b, norm_attn, w_query, w_key, w_value, w_out, norm_mlp, w_gate, w_up, w_down)

    return prefill
```

```python
import functools
import math
import jax
import jax.numpy as jnp
from jax import lax
from jax.experimental import pallas as pl
from jax.experimental.pallas import tpu as pltpu
from jax.sharding import PartitionSpec as P

HEAD = 128
ROPE_BASE = 500000.0
EPS = 1e-5
NEG = -1e30
BF = jnp.bfloat16
F32 = jnp.float32
VMEM_LIMIT = 63 * 1024 * 1024
OWNER_XOR = (0, 2, 1, 3)


def chunk_table(nb, na):
    if nb == 256:
        return [(112, 0), (80, 32), (64, 0)]
    return [(nb // 2, na), (nb // 2, 0)]


def cparams(semantics=None, limit=VMEM_LIMIT):
    return pltpu.CompilerParams(dimension_semantics=semantics, vmem_limit_bytes=limit)


def hbm():
    return pl.BlockSpec(memory_space=pltpu.HBM)


MESH = pl.DeviceIdType.MESH


def other_core():
    t = lax.axis_index('tp')
    return {'tp': t + 1 - 2 * (t % 2)}


def meet():
    barrier = pltpu.get_barrier_semaphore()
    pl.semaphore_signal(barrier, inc=1, device_id=other_core(), device_id_type=MESH)
    pl.semaphore_wait(barrier, 1)


def norm_rows(wide, gain):
    inv = lax.rsqrt(jnp.mean(wide * wide, axis=-1, keepdims=True) + EPS)
    return (wide * inv * gain).astype(BF)


def norm_scratch(half, d, rb, init):
    n = half // rb
    bufs = [pltpu.VMEM((half, d), BF)] * (1 if init else 3)
    return bufs + [pltpu.VMEM((1, d), BF), pltpu.SemaphoreType.DMA((2, 4)), pltpu.SemaphoreType.DMA((n,)), pltpu.SemaphoreType.DMA((n,)), pltpu.SemaphoreType.DMA]


class NormExchange:
    def __init__(self, init, rb, srcs, gain_ref, ho_ref, x_ref, scratch):
        self.init, self.rb, self.srcs, self.gain_ref, self.ho_ref, self.x_ref = init, rb, srcs, gain_ref, ho_ref, x_ref
        self.bufs = scratch[:1 if init else 3]
        self.gain_buf, self.in_sem, self.send_sem, self.recv_sem, self.out_sem = scratch[1 if init else 3:]
        self.half = x_ref.shape[0] // 2
        self.own = self.half // 2
        self.n = self.half // rb

    def gain(self, piece):
        return [] if piece else [pltpu.make_async_copy(self.gain_ref, self.gain_buf, self.in_sem.at[0, 3])]

    def loads(self, piece):
        q = self.own
        dst = pl.ds(piece * q, q)
        if self.init:
            return self.gain(piece) + [pltpu.make_async_copy(self.srcs[piece], self.bufs[0].at[dst, :], self.in_sem.at[piece, 0])]
        src = (dst, dst, pl.ds((1 - piece) * q, q))
        return self.gain(piece) + [pltpu.make_async_copy(ref.at[rows, :], buf.at[dst, :], self.in_sem.at[piece, i]) for i, (ref, rows, buf) in enumerate(zip(self.srcs, src, self.bufs))]

    def send(self, i):
        rows = pl.ds(pl.multiple_of(i * self.rb, self.rb), self.rb)
        there = pl.ds(pl.multiple_of(self.half + i * self.rb, self.rb), self.rb)
        return pltpu.make_async_remote_copy(src_ref=self.x_ref.at[rows, :], dst_ref=self.x_ref.at[there, :], send_sem=self.send_sem.at[i], recv_sem=self.recv_sem.at[i], device_id=other_core(), device_id_type=MESH)

    def store(self):
        return pltpu.make_async_copy(self.bufs[0], self.ho_ref, self.out_sem)

    def start(self, piece):
        for copy in self.loads(piece):
            copy.start()

    def run(self, after_first):
        per = self.n // 2

        def block(i, carry):
            rows = pl.ds(pl.multiple_of(i * self.rb, self.rb), self.rb)
            if self.init:
                h = self.bufs[0][rows, :]
            else:
                hb, sb, tb = self.bufs
                h = (hb[rows, :].astype(F32) + (sb[rows, :].astype(F32) + tb[rows, :].astype(F32))).astype(BF)
                hb[rows, :] = h
            self.x_ref[rows, :] = norm_rows(h.astype(F32), self.gain_buf[...].astype(F32))

            @pl.when(i >= 1)
            def _():
                self.send(i - 1).start()

            return carry

        for piece in range(2):
            for copy in self.loads(piece):
                copy.wait()
            if piece == 0:
                after_first()
            lax.fori_loop(piece * per, (piece + 1) * per, block, 0)
        self.store().start()
        self.send(self.n - 1).start()

    def arrive(self):
        for i in range(self.n):
            self.send(i).wait_recv()

    def finish(self):
        for i in range(self.n):
            self.send(i).wait_send()
        self.store().wait()


def sum_scratch(half, d, bn):
    n = d // bn
    return [
        pltpu.VMEM((3, half, bn), F32),
        pltpu.VMEM((n, half, bn), BF),
        pltpu.VMEM((n, half, bn), BF),
        pltpu.VMEM((half, d), BF),
        pltpu.SemaphoreType.DMA((n,)),
        pltpu.SemaphoreType.DMA((n,)),
        pltpu.SemaphoreType.DMA((n,)),
    ]


class ChipSum:
    def __init__(self, outs, scratch):
        self.outs = outs
        self.mine, self.give, self.got, self.total, self.send_sem, self.recv_sem, self.out_sem = scratch
        self.n, self.half, self.bn = self.give.shape

    def send(self, i):
        return pltpu.make_async_remote_copy(src_ref=self.give.at[i], dst_ref=self.got.at[i], send_sem=self.send_sem.at[i], recv_sem=self.recv_sem.at[i], device_id=other_core(), device_id_type=MESH)

    def cols(self, i):
        return pl.ds(pl.multiple_of(i * self.bn, 128), self.bn)

    def stores(self, i):
        rows = self.half // len(self.outs)
        return [pltpu.make_async_copy(self.total.at[pl.ds(r * rows, rows), self.cols(i)], out.at[:, self.cols(i)], self.out_sem.at[i]) for r, out in enumerate(self.outs)]

    def keep(self, i, acc):
        self.mine[i % 3] = acc[:self.half]
        self.give[i] = acc[self.half:].astype(BF)

    def combine(self, i):
        self.send(i).wait_recv()
        self.total[:, self.cols(i)] = (self.mine[i % 3] + self.got[i].astype(F32)).astype(BF)

    def store(self, i):
        for copy in self.stores(i):
            copy.start()

    def tail(self):
        last = self.n - 1
        self.send(last).start()
        if self.n >= 3:
            self.store(last - 2)
        self.combine(last - 1)
        self.store(last - 1)
        self.combine(last)
        self.store(last)
        for i in range(self.n):
            self.send(i).wait_send()
            for copy in self.stores(i):
                copy.wait()


def rope(vals, cos, sin):
    return (vals * cos + pltpu.roll(vals, HEAD // 2, 1) * sin).astype(BF)


def kv_kernel(init, layer, nkv, rb, *refs):
    n_src = 2 if init else 3
    srcs = refs[:n_src]
    gain_ref, wk_ref, wv_ref, cos_hbm, sin_hbm, ho_ref, n_ref, kv_ref, x_ref, w_ref, kv_buf, cos_ref, sin_ref, w_sem, o_sem = refs[n_src:n_src + 15]
    norm = NormExchange(init, rb, srcs, gain_ref, ho_ref, x_ref, refs[n_src + 15:])
    half = x_ref.shape[0] // 2
    own = half // 2
    width = nkv * HEAD
    t = lax.axis_index('tp')
    cols = pl.ds(pl.multiple_of(t * width, 128), width)
    weights = [
        pltpu.make_async_copy(wk_ref.at[layer, :, cols], w_ref.at[:, pl.ds(0, width)], w_sem.at[0]),
        pltpu.make_async_copy(wv_ref.at[layer, :, cols], w_ref.at[:, pl.ds(width, width)], w_sem.at[1]),
        pltpu.make_async_copy(cos_hbm, cos_ref, w_sem.at[2]),
        pltpu.make_async_copy(sin_hbm, sin_ref, w_sem.at[3]),
    ]
    owners = (t, (t + 2) % 4, t + 1 - 2 * (t % 2), 3 - t)

    def start_weights():
        for copy in weights:
            copy.start()

    def rows_out(r0):
        rows = pl.ds(r0, half)
        return pltpu.make_async_copy(x_ref.at[rows, :], n_ref.at[rows, :], o_sem.at[4 + r0 // half])

    def kv_out(place):
        return pltpu.make_async_copy(kv_buf.at[pl.ds(place * own, own), :], kv_ref.at[owners[place]], o_sem.at[place])

    def kv_rows(r0, r1):
        both = jnp.dot(x_ref[r0:r1, :], w_ref[...], preferred_element_type=F32)
        for i in range(nkv):
            kv_buf[r0:r1, i * HEAD:(i + 1) * HEAD] = rope(both[:, i * HEAD:(i + 1) * HEAD], cos_ref[r0:r1, :], sin_ref[r0:r1, :])
        kv_buf[r0:r1, width:] = both[:, width:].astype(BF)

    norm.start(0)
    norm.start(1)
    meet()
    norm.run(start_weights)
    rows_out(0).start()
    for copy in weights:
        copy.wait()
    kv_rows(0, half)
    norm.arrive()
    rows_out(half).start()
    kv_out(0).start()
    kv_out(1).start()
    kv_rows(half, 2 * half)
    kv_out(2).start()
    kv_out(3).start()
    norm.finish()
    rows_out(0).wait()
    rows_out(half).wait()
    for place in range(4):
        kv_out(place).wait()


def kv_proj(srcs, gain, wk, wv, cos, sin, layer, nkv, rb):
    init = len(srcs) == 2
    d = wk.shape[1]
    half = 2 * srcs[0].shape[0] if init else srcs[0].shape[0]
    rows = 2 * half
    width = nkv * HEAD
    return pl.pallas_call(
        functools.partial(kv_kernel, init, layer, nkv, rb),
        in_specs=[hbm()] * (len(srcs) + 5),
        out_specs=[hbm()] * 3,
        out_shape=[jax.ShapeDtypeStruct((half, d), BF), jax.ShapeDtypeStruct((rows, d), BF), jax.ShapeDtypeStruct((4, rows // 4, 2 * width), BF)],
        scratch_shapes=[
            pltpu.VMEM((rows, d), BF),
            pltpu.VMEM((d, 2 * width), BF),
            pltpu.VMEM((rows, 2 * width), BF),
            pltpu.VMEM((rows, HEAD), F32),
            pltpu.VMEM((rows, HEAD), F32),
            pltpu.SemaphoreType.DMA((4,)),
            pltpu.SemaphoreType.DMA((6,)),
        ] + norm_scratch(half, d, rb, init),
        compiler_params=pltpu.CompilerParams(vmem_limit_bytes=VMEM_LIMIT, collective_id=3 if init else 0, has_side_effects=True),
        cost_estimate=pl.CostEstimate(flops=2 * rows * d * 2 * width, bytes_accessed=2 * d * (3 * rows + 2 * width), transcendentals=0),
        name="kv_init" if init else "kv_proj",
    )(*srcs, gain, wk, wv, cos, sin)


def q_blocks(qcols):
    blocks, c = [], 0
    while c < qcols:
        width = min(512 if c else 256, qcols - c)
        blocks.append((c, width))
        c += width
    return blocks


def q_kernel(layer, n_hbm, wq_ref, cos_hbm, sin_hbm, q_ref, x_ref, w_ref, q_buf, cos_ref, sin_ref, w_sem, o_sem):
    blocks = q_blocks(q_buf.shape[1])
    loads = [pltpu.make_async_copy(n_hbm, x_ref, w_sem.at[0])]
    loads += [pltpu.make_async_copy(wq_ref.at[layer, :, pl.ds(c, bw)], w_ref.at[:, pl.ds(c, bw)], w_sem.at[3 + i]) for i, (c, bw) in enumerate(blocks)]
    trig = [pltpu.make_async_copy(cos_hbm, cos_ref, w_sem.at[1]), pltpu.make_async_copy(sin_hbm, sin_ref, w_sem.at[2])]
    for copy in loads[:2] + trig + loads[2:]:
        copy.start()
    for copy in loads[:1] + trig:
        copy.wait()
    outs = []
    for j, (c, bw) in enumerate(blocks):
        loads[1 + j].wait()
        acc = jnp.dot(x_ref[...], w_ref[:, c:c + bw], preferred_element_type=F32)
        for i in range(bw // HEAD):
            q_buf[:, c + i * HEAD:c + (i + 1) * HEAD] = rope(acc[:, i * HEAD:(i + 1) * HEAD], cos_ref[...], sin_ref[...])
        outs.append(pltpu.make_async_copy(q_buf.at[:, pl.ds(c, bw)], q_ref.at[:, pl.ds(c, bw)], o_sem.at[j]))
        outs[-1].start()
    for copy in outs:
        copy.wait()


def q_proj(n, wq, cos, sin, layer):
    rows, d = n.shape
    qcols = wq.shape[2]
    nb = len(q_blocks(qcols))
    return pl.pallas_call(
        functools.partial(q_kernel, layer),
        in_specs=[hbm()] * 4,
        out_specs=hbm(),
        out_shape=jax.ShapeDtypeStruct((rows, qcols), BF),
        scratch_shapes=[
            pltpu.VMEM((rows, d), BF),
            pltpu.VMEM((d, qcols), BF),
            pltpu.VMEM((rows, qcols), BF),
            pltpu.VMEM((rows, HEAD), F32),
            pltpu.VMEM((rows, HEAD), F32),
            pltpu.SemaphoreType.DMA((3 + nb,)),
            pltpu.SemaphoreType.DMA((nb,)),
        ],
        compiler_params=cparams(),
        cost_estimate=pl.CostEstimate(flops=2 * rows * d * qcols, bytes_accessed=2 * d * (rows + qcols), transcendentals=0),
        name="q_proj",
    )(n, wq, cos, sin)


SM_C = HEAD ** -0.5 * math.log2(math.e)


def lanes(x, width):
    return jnp.concatenate([x] * (width // HEAD), axis=1) if width > HEAD else x


def flash_step(qs, k, v, ok, m, l, acc):
    s = lax.dot_general(qs, k, (((1,), (1,)), ((), ())), preferred_element_type=F32) * SM_C
    if ok is not None:
        s = jnp.where(ok, s, NEG)
    _, width = s.shape
    m_new = jnp.maximum(m, jnp.max(s, axis=1, keepdims=True))
    alpha = jnp.exp2(m - m_new)
    p = jnp.exp2(s - lanes(m_new, width))
    part = p[:, :HEAD]
    for i in range(1, width // HEAD):
        part = part + p[:, i * HEAD:(i + 1) * HEAD]
    return m_new, l * alpha + part, acc * alpha + jnp.dot(p.astype(BF), v, preferred_element_type=F32)


def flash(q_rows, qi, ql, qi_min, ql_max, kv_ref, bk, nkv, group, lo, hi, m_ref, l_ref, acc_ref):
    rows = qi.shape[0]
    gr = group * rows
    qs = [jnp.concatenate([q_rows(kh * group + i) for i in range(group)], axis=0) for kh in range(nkv)]
    m_ref[:, :gr, :] = jnp.full((nkv, gr, HEAD), NEG, F32)
    l_ref[:, :gr, :] = jnp.zeros((nkv, gr, HEAD), F32)
    acc_ref[:, :gr, :] = jnp.zeros((nkv, gr, HEAD), F32)

    per = kv_ref.shape[1]

    def keys(j, col):
        block = kv_ref[pl.ds(j * (bk // per), bk // per), :, col * HEAD:(col + 1) * HEAD]
        return block.reshape(bk, HEAD)

    def step(j, masked):
        base = j * bk
        ok = None
        if masked:
            kid = base + lax.broadcasted_iota(jnp.int32, (rows, bk), 1)
            ok = (kid <= qi) & (kid >= ql)
            ok = jnp.concatenate([ok] * group, axis=0)
        new = []
        for kh in range(nkv):
            k = keys(j, kh)
            v = keys(j, nkv + kh)
            new.append(flash_step(qs[kh], k, v, ok, m_ref[kh, :gr, :], l_ref[kh, :gr, :], acc_ref[kh, :gr, :]))
        for kh in range(nkv):
            m_ref[kh, :gr, :], l_ref[kh, :gr, :], acc_ref[kh, :gr, :] = new[kh]

    def body(j, carry):
        base = j * bk
        full = (ql_max <= base) & (qi_min >= base + bk - 1)

        @pl.when(full)
        def _():
            step(j, False)

        @pl.when(jnp.logical_not(full))
        def _():
            step(j, True)

        return carry

    lax.fori_loop(lo, hi, body, 0)
    outs = []
    for kh in range(nkv):
        total = jnp.sum(l_ref[kh, :gr, :], axis=1, keepdims=True)
        out = (acc_ref[kh, :gr, :] / total).astype(BF)
        outs += [out[i * rows:(i + 1) * rows, :] for i in range(group)]
    return outs


def attn_kernel(table, me, nkv, group, nb, na, bks, sc_ref, q_hbm, *refs):
    n_kv = 4 * len(table)
    kv_hbm = refs[:n_kv]
    o_hbm, q_ref, o_ref, kvb_ref, kva_ref, m_ref, l_ref, acc_ref, sem, q_sem, o_sem = refs[n_kv:]
    b, a = table[me]
    own = a + b
    t = lax.axis_index('tp')
    p = lax.axis_index('pp')
    load_q = pltpu.make_async_copy(q_hbm, q_ref, q_sem)
    load_q.start()

    def copies(s):
        off_b, off_a = 0, 0
        out = []
        for k, (bk_, ak_) in enumerate(table):
            src = kv_hbm[4 * k + s]
            slot = pl.ds((3 - s) * 4, 4)
            if b and bk_:
                out.append(pltpu.make_async_copy(src.at[:, pl.ds(0, bk_), :], kvb_ref.at[slot, pl.ds(off_b, bk_), :], sem))
            if a and ak_:
                out.append(pltpu.make_async_copy(src.at[:, pl.ds(bk_, ak_), :], kva_ref.at[slot, pl.ds(off_a, ak_), :], sem))
            off_b += bk_
            off_a += ak_
        return out

    for s in range(4):
        for copy in copies(s):
            copy.start()
    load_q.wait()
    for s in range(4):
        for copy in copies(s):
            copy.wait()

    def first_key(which, n_own):
        return [sc_ref[4 * which + v] + (3 - p) * 4 * n_own for v in range(4)]

    def lowest(starts, idx):
        low = jnp.zeros_like(idx) + starts[0]
        for v in range(1, 4):
            low = jnp.where(idx >= starts[v], starts[v], low)
        return low

    offs = [(sum(x[0] for x in table[:me])), (sum(x[1] for x in table[:me]))]

    def store(o):
        rows = pl.ds(pl.multiple_of(o * own, 16), own)
        return pltpu.make_async_copy(o_ref.at[rows, :], o_hbm.at[rows, :], o_sem)

    if b:
        starts_b = first_key(0, nb)

        def one_owner(o, carry):
            r0 = pl.multiple_of(o * own, 16)
            owner = t ^ (2 * (o % 2) + o // 2)
            i0 = 12 * nb + owner * nb + offs[0]
            low0 = starts_b[0]
            for v in range(1, 4):
                low0 = jnp.where(i0 >= starts_b[v], starts_b[v], low0)
            idx = i0 + lax.broadcasted_iota(jnp.int32, (b, 1), 0)
            low = lowest(starts_b, idx)
            last_low = jnp.where(i0 + b - 1 >= starts_b[1], starts_b[1], starts_b[0])
            for v in range(2, 4):
                last_low = jnp.where(i0 + b - 1 >= starts_b[v], starts_b[v], last_low)
            q_rows = lambda h: q_ref[pl.ds(r0, b), h * HEAD:(h + 1) * HEAD]
            outs = flash(q_rows, idx, low, i0, last_low, kvb_ref, bks[0], nkv, group, low0 // bks[0], (i0 + b - 1) // bks[0] + 1, m_ref, l_ref, acc_ref)
            for h, out in enumerate(outs):
                o_ref[pl.ds(r0, b), h * HEAD:(h + 1) * HEAD] = out
            if not a:
                store(o).start()
            return carry

        lax.fori_loop(0, 4, one_owner, 0)
    if a:
        starts_a = first_key(1, na)
        idx = jnp.concatenate([12 * na + (t ^ OWNER_XOR[o]) * na + offs[1] + lax.broadcasted_iota(jnp.int32, (a, 1), 0) for o in range(4)], axis=0)
        low = lowest(starts_a, idx)
        spans = [(o * own + b, o * own + b + a) for o in range(4)]
        gather = lambda c0, c1: jnp.concatenate([q_ref[r0:r1, c0:c1] for r0, r1 in spans], axis=0)
        n_blocks = 16 * na // bks[1]
        outs = flash(lambda h: gather(h * HEAD, (h + 1) * HEAD), idx, low, 0, 16 * na, kva_ref, bks[1], nkv, group, starts_a[0] // bks[1], n_blocks, m_ref, l_ref, acc_ref)
        for h, out in enumerate(outs):
            for o, (r0, r1) in enumerate(spans):
                o_ref[r0:r1, h * HEAD:(h + 1) * HEAD] = out[o * a:(o + 1) * a, :]
        for o in range(4):
            store(o).start()
    for o in range(4):
        store(o).wait()


def attention(table, me, sc, q, kvs, nkv, group, nb, na, bks):
    rows, qcols = q.shape
    b, a = table[me]
    gr = group * max(4 * a, b)
    kvw = 2 * nkv * HEAD
    flat = [x for per_chunk in kvs for x in per_chunk]
    flops = 4 * (4 * b * 16 * nb + 4 * a * 16 * na) * qcols
    return pl.pallas_call(
        functools.partial(attn_kernel, table, me, nkv, group, nb, na, bks),
        in_specs=[pl.BlockSpec(memory_space=pltpu.SMEM), hbm()] + [hbm()] * len(flat),
        out_specs=hbm(),
        scratch_shapes=[
            pltpu.VMEM((rows, qcols), BF),
            pltpu.VMEM((rows, qcols), BF),
            pltpu.VMEM((16, nb, kvw), BF),
            pltpu.VMEM((16, na, kvw), BF),
            pltpu.VMEM((nkv, gr, HEAD), F32),
            pltpu.VMEM((nkv, gr, HEAD), F32),
            pltpu.VMEM((nkv, gr, HEAD), F32),
            pltpu.SemaphoreType.DMA,
            pltpu.SemaphoreType.DMA,
            pltpu.SemaphoreType.DMA,
        ],
        out_shape=jax.ShapeDtypeStruct((rows, qcols), BF),
        compiler_params=cparams(),
        cost_estimate=pl.CostEstimate(flops=flops, bytes_accessed=4 * rows * qcols + 32 * (nb + na) * kvw, transcendentals=0),
        name="attention",
    )(sc, q, *flat)


def oproj_kernel(layer, bn, o_hbm, w_ref, so_ref, o_ref, w_buf, w_sem, *scratch):
    chip = ChipSum([so_ref], scratch)
    loads = [pltpu.make_async_copy(w_ref.at[layer, :, pl.ds(i * bn, bn)], w_buf.at[:, pl.ds(i * bn, bn)], w_sem.at[i]) for i in range(chip.n)]
    load_o = pltpu.make_async_copy(o_hbm, o_ref, w_sem.at[chip.n])
    load_o.start()
    for copy in loads:
        copy.start()
    meet()
    load_o.wait()
    for i in range(chip.n):
        loads[i].wait()
        if i >= 1:
            chip.send(i - 1).start()
        if i >= 3:
            chip.store(i - 3)
        acc = jnp.dot(o_ref[...], w_buf[:, i * bn:(i + 1) * bn], preferred_element_type=F32)
        if i >= 2:
            chip.combine(i - 2)
        chip.keep(i, acc)
    chip.tail()


def oproj(o, wo, layer):
    rows, k = o.shape
    d = wo.shape[2]
    bn = min(1024, d // 2)
    half = rows // 2
    return pl.pallas_call(
        functools.partial(oproj_kernel, layer, bn),
        in_specs=[hbm(), hbm()],
        out_specs=hbm(),
        out_shape=jax.ShapeDtypeStruct((half, d), BF),
        scratch_shapes=[pltpu.VMEM((rows, k), BF), pltpu.VMEM((k, d), BF), pltpu.SemaphoreType.DMA((d // bn + 1,))] + sum_scratch(half, d, bn),
        compiler_params=pltpu.CompilerParams(vmem_limit_bytes=VMEM_LIMIT, collective_id=1, has_side_effects=True),
        cost_estimate=pl.CostEstimate(flops=2 * rows * k * d, bytes_accessed=2 * (rows * k + k * d + rows * d), transcendentals=0),
        name="oproj",
    )(o, wo)


def mlp_kernel(layer, bf, bn, rb, n_out, *refs):
    srcs = refs[:3]
    gain_ref, wg_ref, wu_ref, wd_ref, ho_ref = refs[3:8]
    outs = refs[8:8 + n_out]
    x_ref, w_ref, both_ref, act_ref, w_sem, f_sem = refs[8 + n_out:14 + n_out]
    scratch = refs[14 + n_out:]
    d = x_ref.shape[1]
    norm = NormExchange(False, rb, srcs, gain_ref, ho_ref, x_ref, scratch[:8])
    chip = ChipSum(outs, scratch[8:])
    ff = wg_ref.shape[2]
    n_up = ff // bf
    n_down = chip.n
    half = x_ref.shape[0] // 2

    def up_copies(step):
        slot = step % 3
        cols = pl.ds(pl.multiple_of(step * bf, 128), bf)
        return (
            pltpu.make_async_copy(wg_ref.at[layer, :, cols], w_ref.at[slot, pl.ds(0, wg_ref.shape[1]), pl.ds(0, bf)], w_sem.at[slot, 0]),
            pltpu.make_async_copy(wu_ref.at[layer, :, cols], w_ref.at[slot, pl.ds(0, wg_ref.shape[1]), pl.ds(bf, bf)], w_sem.at[slot, 1]),
        )

    def down_copy(step):
        slot = (step + n_up) % 3
        return pltpu.make_async_copy(wd_ref.at[layer, :, chip.cols(step)], w_ref.at[slot, pl.ds(0, ff), pl.ds(0, bn)], w_sem.at[slot, 0])

    def gated(step):
        slot = step % 2
        gate = both_ref[slot, :, :bf]
        act = gate * jax.nn.sigmoid(gate) * both_ref[slot, :, bf:]
        act_ref[:, pl.ds(pl.multiple_of(step * bf, 128), bf)] = act.astype(BF)

    def first_copies(i):
        cols, dest = pl.ds(i * HEAD, HEAD), 2 * i * HEAD
        return (
            pltpu.make_async_copy(wg_ref.at[layer, :, cols], w_ref.at[0, pl.ds(0, d), pl.ds(dest, HEAD)], f_sem.at[i, 0]),
            pltpu.make_async_copy(wu_ref.at[layer, :, cols], w_ref.at[0, pl.ds(0, d), pl.ds(dest + HEAD, HEAD)], f_sem.at[i, 1]),
        )

    def first(i, r0, r1):
        both = jnp.dot(x_ref[r0:r1, :], w_ref[0, :d, 2 * i * HEAD:2 * (i + 1) * HEAD], preferred_element_type=F32)
        both_ref[0, r0:r1, i * HEAD:(i + 1) * HEAD] = both[:, :HEAD]
        both_ref[0, r0:r1, bf + i * HEAD:bf + (i + 1) * HEAD] = both[:, HEAD:]

    def start_first(parts):
        for i in parts:
            for copy in first_copies(i):
                copy.start()

    def start_up(step):
        for copy in up_copies(step):
            copy.start()

    def wait_up(step):
        for copy in up_copies(step):
            copy.wait()

    n_first = bf // HEAD
    norm.start(0)
    start_first([0])
    norm.start(1)
    meet()
    norm.run(lambda: start_first(range(1, n_first)))
    start_up(1)
    start_up(2) if n_up > 2 else down_copy(0).start()
    for i in range(n_first):
        for copy in first_copies(i):
            copy.wait()
        first(i, 0, half)
    norm.arrive()
    for i in range(n_first):
        first(i, half, 2 * half)

    def up(j, carry):
        wait_up(j)

        @pl.when(j + 2 < n_up)
        def _():
            start_up(j + 2)

        @pl.when(j + 2 >= n_up)
        def _():
            down_copy(j + 2 - n_up).start()

        gated(j - 1)
        both_ref[j % 2] = jnp.dot(x_ref[...], w_ref[j % 3, :x_ref.shape[1], :], preferred_element_type=F32)
        return carry

    lax.fori_loop(1, n_up, up, 0)
    gated(n_up - 1)

    def down(i, carry):
        down_copy(i).wait()

        @pl.when(i + 2 < n_down)
        def _():
            down_copy(i + 2).start()

        @pl.when(i >= 1)
        def _():
            chip.send(i - 1).start()

        @pl.when(i >= 3)
        def _():
            chip.store(i - 3)

        acc = jnp.dot(act_ref[...], w_ref[(i + n_up) % 3, :ff, :bn], preferred_element_type=F32)

        @pl.when(i >= 2)
        def _():
            chip.combine(i - 2)

        chip.keep(i, acc)
        return carry

    lax.fori_loop(0, n_down, down, 0)
    chip.tail()
    norm.finish()


def mlp(h, s, t, gain, wg, wu, wd, layer, rb, n_out):
    half, d = h.shape
    rows = 2 * half
    ff = wg.shape[2]
    bf = 384
    bn = min(512, d // 2)
    out = jax.ShapeDtypeStruct((half, d), BF)
    part = jax.ShapeDtypeStruct((half // n_out, d), BF)
    return pl.pallas_call(
        functools.partial(mlp_kernel, layer, bf, bn, rb, n_out),
        in_specs=[hbm()] * 7,
        out_specs=[hbm()] * (1 + n_out),
        out_shape=[out] + [part] * n_out,
        scratch_shapes=[
            pltpu.VMEM((rows, d), BF),
            pltpu.VMEM((3, max(d, ff), 2 * bf), BF),
            pltpu.VMEM((2, rows, 2 * bf), F32),
            pltpu.VMEM((rows, ff), BF),
            pltpu.SemaphoreType.DMA((3, 2)),
            pltpu.SemaphoreType.DMA((bf // HEAD, 2)),
        ] + norm_scratch(half, d, rb, False) + sum_scratch(half, d, bn),
        compiler_params=pltpu.CompilerParams(vmem_limit_bytes=VMEM_LIMIT, collective_id=2, has_side_effects=True),
        cost_estimate=pl.CostEstimate(flops=6 * rows * d * ff, bytes_accessed=2 * (2 * rows * d + 3 * d * ff), transcendentals=rows * ff),
        name="mlp",
    )(h, s, t, gain, wg, wu, wd)


def final_kernel(b, a, off, n_in, *refs):
    srcs, outs = refs[:3], refs[n_in:n_in + 1 + bool(a)]
    bufs, in_sem, out_sem = refs[n_in + 1 + bool(a):n_in + 4 + bool(a)], refs[-2], refs[-1]
    loads = [pltpu.make_async_copy(src.at[pl.ds(0, a + b), :], buf, in_sem.at[i]) for i, (src, buf) in enumerate(zip(srcs, bufs))]
    for copy in loads:
        copy.start()
    for copy in loads:
        copy.wait()

    def block(i, carry):
        rows = pl.ds(pl.multiple_of(i * 16, 16), 16)
        h, s, t = (buf[rows, :].astype(F32) for buf in bufs)
        bufs[0][rows, :] = (h + (s + t)).astype(BF)
        return carry

    lax.fori_loop(0, (a + b) // 16, block, 0)
    stores = [pltpu.make_async_copy(bufs[0].at[pl.ds(0, b), :], outs[0].at[pl.ds(off, b), :], out_sem.at[0])]
    if a:
        stores.append(pltpu.make_async_copy(bufs[0].at[pl.ds(b, a), :], outs[1], out_sem.at[1]))
    for copy in stores:
        copy.start()
    for copy in stores:
        copy.wait()


def final(h, s, t, b, a, off, n_b, out_b):
    d = h.shape[1]
    args = (h, s, t) if out_b is None else (h, s, t, out_b)
    shapes = [jax.ShapeDtypeStruct((n_b, d), BF)] + ([jax.ShapeDtypeStruct((a, d), BF)] if a else [])
    return pl.pallas_call(
        functools.partial(final_kernel, b, a, off, len(args)),
        in_specs=[hbm()] * len(args),
        out_specs=[hbm()] * len(shapes),
        out_shape=shapes,
        input_output_aliases={} if out_b is None else {3: 0},
        scratch_shapes=[pltpu.VMEM((a + b, d), BF)] * 3 + [pltpu.SemaphoreType.DMA((3,)), pltpu.SemaphoreType.DMA((2,))],
        compiler_params=cparams(),
        cost_estimate=pl.CostEstimate(flops=20 * (a + b) * d, bytes_accessed=8 * (a + b) * d, transcendentals=0),
        name="final",
    )(*args)


def solution(mesh):
    row_spec = P(('dp', 'pp', 'tp'), None)
    id_spec = P(('dp', 'pp', 'tp'))
    col_spec = P(None, None, 'tp')
    in_row_spec = P(None, 'tp', None)
    full_spec = P()
    n_pp = mesh.shape['pp']
    across_core = [(i, i ^ 1) for i in range(4)]
    across_y = [(i, i ^ 2) for i in range(4)]

    def per_device(tok_a, seg_a, pos_a, tok_b, seg_b, pos_b, g_attn, wq, wk, wv, wo, g_mlp, wg, wu, wd):
        n_layers, _ = g_attn.shape
        nb, na = tok_b.shape[0], tok_a.shape[0]
        n_kv_all = wk.shape[2] // HEAD
        nkv = n_kv_all // 4
        group = wq.shape[2] // HEAD // nkv
        table = chunk_table(nb, na)
        n_chunks = len(table)
        rb = 16

        off_b, off_a, b0, a0 = [], [], 0, 0
        for b, a in table:
            off_b.append(b0)
            off_a.append(a0)
            b0, a0 = b0 + b, a0 + a
        gain_attn = [g_attn[l:l + 1] for l in range(n_layers)]
        gain_mlp = [g_mlp[l:l + 1] for l in range(n_layers)]

        own_rows = []
        for (b, a), ob, oa in zip(table, off_b, off_a):
            parts = [tok_b[ob:ob + b]] if b else []
            parts += [tok_a[oa:oa + a]] if a else []
            own_rows.append(parts[0] if len(parts) == 1 else jnp.concatenate(parts, axis=0))

        def permute(x, axis, pairs):
            return lax.ppermute(x, axis, pairs)

        def over_core(mine, got):
            pair = jnp.stack([mine, got])
            return jnp.concatenate([pair, permute(pair, 'tp', across_core)], axis=0)

        below = jnp.stack([jnp.sum((seg < v).astype(jnp.int32)) for seg in (seg_b, seg_a) for v in range(4)])
        pos_b_rows = over_core(pos_b, permute(pos_b, 'tp', across_y))
        got_rows = [permute(own_rows[k], 'tp', across_y) for k in range(n_chunks)]
        got_pos_a, got_below = permute(pos_a, 'tp', across_y), permute(below, 'tp', across_y)

        inv_freq = jnp.power(ROPE_BASE, -2.0 * jnp.arange(HEAD // 2, dtype=F32) / HEAD)

        def trig(pos):
            angles = pos.astype(F32)[..., None] * inv_freq
            cos, sin = jnp.cos(angles), jnp.sin(angles)
            return jnp.concatenate([cos, cos], axis=-1), jnp.concatenate([-sin, sin], axis=-1)

        def chunk_trig(k, after):
            (b, a), ob, oa = table[k], off_b[k], off_a[k]
            parts = ([pos_b_rows[:, ob:ob + b]] if b else []) + ([pos_a_rows[:, oa:oa + a]] if a else [])
            pos = (parts[0] if len(parts) == 1 else jnp.concatenate(parts, axis=1)).reshape(4 * (a + b))
            if after is not None:
                pos, _ = lax.optimization_barrier((pos, after))
            return trig(pos)

        cos, sin = [None] * n_chunks, [None] * n_chunks
        bk_b, bk_a = min(512, 16 * nb), min(512, 16 * na)
        out_b, out_a = None, None
        srcs = list(zip(own_rows, got_rows))
        h = [None] * n_chunks
        for l in range(n_layers):
            q, kvs, n = [None] * n_chunks, [None] * n_chunks, [None] * n_chunks
            last = l + 1 == n_layers
            for k in range(n_chunks):
                if l == 0:
                    cos[k], sin[k] = chunk_trig(k, kvs[k - 1][0] if k else None)
                h[k], n[k], kv = kv_proj(srcs[k], gain_attn[l], wk, wv, cos[k], sin[k], l, nkv, rb)
                q[k] = q_proj(n[k], wq, cos[k], sin[k], l)
                if l == 0 and k == 0:
                    got_pos_a, got_below, _ = lax.optimization_barrier((got_pos_a, got_below, kv))
                    pos_a_rows = over_core(pos_a, got_pos_a)
                    below = jnp.sum(over_core(below, got_below), axis=0)
                    others = [permute(below, 'pp', [(i, (i + s) % n_pp) for i in range(n_pp)]) for s in range(1, n_pp)]
                    starts = below + others[0] + others[1] + others[2]
                kvs[k] = [kv]
                for s in range(1, n_pp):
                    if k == 2 or (k == 0 and l):
                        kvs[k].append(permute(kv, 'pp', [(i, i + s) for i in range(n_pp - s)]))
                    else:
                        kvs[k].append(permute(kvs[k][-1], 'pp', [(i, i + 1) for i in range(s - 1, n_pp - 1)]))
            sums = []
            for k in range(n_chunks):
                o = attention(table, k, starts, q[k], kvs, nkv, group, nb, na, (bk_b, bk_a))
                s = oproj(o, wo, l)
                sums.append((s, permute(s, 'tp', across_y)))
            for k in range(n_chunks):
                h[k], *parts = mlp(h[k], *sums[k], gain_mlp[l], wg, wu, wd, l, rb, 2 if last else 1)
                got = permute(parts[-1], 'tp', across_y)
                srcs[k] = (h[k], parts[0], got)
        for k, ((b, a), parts) in enumerate(zip(table, srcs)):
            out_b, *rest = final(*parts, b, a, off_b[k], nb, out_b)
            out_a = rest[0] if rest else out_a
        return out_a, out_b

    def prefill(tokens_a, segment_a, position_a, tokens_b, segment_b, position_b, norm_attn, w_query, w_key, w_value, w_out, norm_mlp, w_gate, w_up, w_down):
        mapped = jax.shard_map(per_device, mesh=mesh, in_specs=(row_spec, id_spec, id_spec, row_spec, id_spec, id_spec, full_spec, col_spec, full_spec, full_spec, in_row_spec, full_spec, col_spec, col_spec, in_row_spec), out_specs=(row_spec, row_spec), check_vma=False)
        return mapped(tokens_a, segment_a, position_a, tokens_b, segment_b, position_b, norm_attn, w_query, w_key, w_value, w_out, norm_mlp, w_gate, w_up, w_down)

    return prefill
```

```python
import functools
import math
import jax
import jax.numpy as jnp
from jax import lax
from jax.experimental import pallas as pl
from jax.experimental.pallas import tpu as pltpu
from jax.sharding import PartitionSpec as P

HEAD = 128
ROPE_BASE = 500000.0
EPS = 1e-5
NEG = -1e30
BF = jnp.bfloat16
F32 = jnp.float32
VMEM_LIMIT = 63 * 1024 * 1024
OWNER_XOR = (0, 2, 1, 3)


def chunk_table(nb, na):
    if nb == 256:
        return [(112, 0), (80, 32), (64, 0)]
    return [(nb // 2, na), (nb // 2, 0)]


def cparams(semantics=None, limit=VMEM_LIMIT):
    return pltpu.CompilerParams(dimension_semantics=semantics, vmem_limit_bytes=limit)


def hbm():
    return pl.BlockSpec(memory_space=pltpu.HBM)


MESH = pl.DeviceIdType.MESH


def other_core():
    t = lax.axis_index('tp')
    return {'tp': t + 1 - 2 * (t % 2)}


def other_side():
    return {'tp': (lax.axis_index('tp') + 2) % 4}


def meet(across=False):
    barrier = pltpu.get_barrier_semaphore()
    peers = [other_core()] + ([other_side()] if across else [])
    for peer in peers:
        pl.semaphore_signal(barrier, inc=1, device_id=peer, device_id_type=MESH)
    pl.semaphore_wait(barrier, len(peers))


def norm_rows(wide, gain):
    inv = lax.rsqrt(jnp.mean(wide * wide, axis=-1, keepdims=True) + EPS)
    return (wide * inv * gain).astype(BF)


def norm_scratch(half, d, rb, init):
    n = half // rb
    bufs = [pltpu.VMEM((half, d), BF)] * (1 if init else 3)
    return bufs + [pltpu.VMEM((1, d), BF), pltpu.SemaphoreType.DMA((2, 4)), pltpu.SemaphoreType.DMA((n,)), pltpu.SemaphoreType.DMA((n,)), pltpu.SemaphoreType.DMA]


class NormExchange:
    def __init__(self, init, rb, srcs, gain_ref, ho_ref, x_ref, scratch):
        self.init, self.rb, self.srcs, self.gain_ref, self.ho_ref, self.x_ref = init, rb, srcs, gain_ref, ho_ref, x_ref
        self.bufs = scratch[:1 if init else 3]
        self.gain_buf, self.in_sem, self.send_sem, self.recv_sem, self.out_sem = scratch[1 if init else 3:]
        self.half = x_ref.shape[0] // 2
        self.own = self.half // 2
        self.n = self.half // rb

    def gain(self, piece):
        return [] if piece else [pltpu.make_async_copy(self.gain_ref, self.gain_buf, self.in_sem.at[0, 3])]

    def loads(self, piece):
        q = self.own
        dst = pl.ds(piece * q, q)
        if self.init:
            return self.gain(piece) + [pltpu.make_async_copy(self.srcs[piece], self.bufs[0].at[dst, :], self.in_sem.at[piece, 0])]
        src = (dst, dst, pl.ds((1 - piece) * q, q))
        return self.gain(piece) + [pltpu.make_async_copy(ref.at[rows, :], buf.at[dst, :], self.in_sem.at[piece, i]) for i, (ref, rows, buf) in enumerate(zip(self.srcs, src, self.bufs))]

    def send(self, i):
        rows = pl.ds(pl.multiple_of(i * self.rb, self.rb), self.rb)
        there = pl.ds(pl.multiple_of(self.half + i * self.rb, self.rb), self.rb)
        return pltpu.make_async_remote_copy(src_ref=self.x_ref.at[rows, :], dst_ref=self.x_ref.at[there, :], send_sem=self.send_sem.at[i], recv_sem=self.recv_sem.at[i], device_id=other_core(), device_id_type=MESH)

    def store(self):
        return pltpu.make_async_copy(self.bufs[0], self.ho_ref, self.out_sem)

    def start(self, piece):
        for copy in self.loads(piece):
            copy.start()

    def run(self, after_first):
        per = self.n // 2

        def block(i, carry):
            rows = pl.ds(pl.multiple_of(i * self.rb, self.rb), self.rb)
            if self.init:
                h = self.bufs[0][rows, :]
            else:
                hb, sb, tb = self.bufs
                h = (hb[rows, :].astype(F32) + (sb[rows, :].astype(F32) + tb[rows, :].astype(F32))).astype(BF)
                hb[rows, :] = h
            self.x_ref[rows, :] = norm_rows(h.astype(F32), self.gain_buf[...].astype(F32))

            @pl.when(i >= 1)
            def _():
                self.send(i - 1).start()

            return carry

        for piece in range(2):
            for copy in self.loads(piece):
                copy.wait()
            if piece == 0:
                after_first()
            lax.fori_loop(piece * per, (piece + 1) * per, block, 0)
        self.store().start()
        self.send(self.n - 1).start()

    def arrive(self):
        for i in range(self.n):
            self.send(i).wait_recv()

    def finish(self):
        for i in range(self.n):
            self.send(i).wait_send()
        self.store().wait()


def sum_scratch(half, d, bn, across=False):
    n = d // bn
    extra = [pltpu.VMEM((half // 2, d), BF), pltpu.SemaphoreType.DMA((n,)), pltpu.SemaphoreType.DMA((n,)), pltpu.SemaphoreType.DMA]
    return [
        pltpu.VMEM((3, half, bn), F32),
        pltpu.VMEM((n, half, bn), BF),
        pltpu.VMEM((n, half, bn), BF),
        pltpu.VMEM((half, d), BF),
        pltpu.SemaphoreType.DMA((n,)),
        pltpu.SemaphoreType.DMA((n,)),
        pltpu.SemaphoreType.DMA((n,)),
    ] + (extra if across else [])


class ChipSum:
    def __init__(self, outs, scratch, across=False):
        self.across = across
        self.outs = outs
        self.mine, self.give, self.got, self.total, self.send_sem, self.recv_sem, self.out_sem, *extra = scratch
        if across:
            self.far, self.y_send, self.y_recv, self.far_sem = extra
        self.n, self.half, self.bn = self.give.shape

    def send(self, i):
        return pltpu.make_async_remote_copy(src_ref=self.give.at[i], dst_ref=self.got.at[i], send_sem=self.send_sem.at[i], recv_sem=self.recv_sem.at[i], device_id=other_core(), device_id_type=MESH)

    def send_far(self, i):
        q = self.half // 2
        return pltpu.make_async_remote_copy(src_ref=self.total.at[pl.ds(q, q), self.cols(i)], dst_ref=self.far.at[:, self.cols(i)], send_sem=self.y_send.at[i], recv_sem=self.y_recv.at[i], device_id=other_side(), device_id_type=MESH)

    def cols(self, i):
        return pl.ds(pl.multiple_of(i * self.bn, 128), self.bn)

    def stores(self, i):
        copies, row = [], 0
        for out in self.outs[:1] if self.across else self.outs:
            copies.append(pltpu.make_async_copy(self.total.at[pl.ds(row, out.shape[0]), self.cols(i)], out.at[:, self.cols(i)], self.out_sem.at[i]))
            row += out.shape[0]
        return copies

    def keep(self, i, acc):
        self.mine[i % 3] = acc[:self.half]
        self.give[i] = acc[self.half:].astype(BF)

    def combine(self, i):
        self.send(i).wait_recv()
        self.total[:, self.cols(i)] = (self.mine[i % 3] + self.got[i].astype(F32)).astype(BF)

    def store(self, i):
        if self.across:
            self.send_far(i).start()
        for copy in self.stores(i):
            copy.start()

    def tail(self):
        last = self.n - 1
        self.send(last).start()
        if self.n >= 3:
            self.store(last - 2)
        self.combine(last - 1)
        self.store(last - 1)
        self.combine(last)
        self.store(last)
        for i in range(self.n):
            self.send(i).wait_send()
            for copy in self.stores(i):
                copy.wait()
        if self.across:
            for i in range(self.n):
                self.send_far(i).wait()
            copy = pltpu.make_async_copy(self.far, self.outs[1], self.far_sem)
            copy.start()
            copy.wait()


def rope(vals, cos, sin):
    return (vals * cos + pltpu.roll(vals, HEAD // 2, 1) * sin).astype(BF)


def kv_kernel(init, layer, nkv, rb, *refs):
    n_src = 2 if init else 3
    srcs = refs[:n_src]
    gain_ref, wk_ref, wv_ref, cos_hbm, sin_hbm, ho_ref, n_ref, kv_ref, x_ref, w_ref, kv_buf, cos_ref, sin_ref, w_sem, o_sem = refs[n_src:n_src + 15]
    norm = NormExchange(init, rb, srcs, gain_ref, ho_ref, x_ref, refs[n_src + 15:])
    half = x_ref.shape[0] // 2
    own = half // 2
    width = nkv * HEAD
    t = lax.axis_index('tp')
    cols = pl.ds(pl.multiple_of(t * width, 128), width)
    weights = [
        pltpu.make_async_copy(wk_ref.at[layer, :, cols], w_ref.at[:, pl.ds(0, width)], w_sem.at[0]),
        pltpu.make_async_copy(wv_ref.at[layer, :, cols], w_ref.at[:, pl.ds(width, width)], w_sem.at[1]),
        pltpu.make_async_copy(cos_hbm, cos_ref, w_sem.at[2]),
        pltpu.make_async_copy(sin_hbm, sin_ref, w_sem.at[3]),
    ]
    owners = (t, (t + 2) % 4, t + 1 - 2 * (t % 2), 3 - t)

    def start_weights():
        for copy in weights:
            copy.start()

    def rows_out(r0):
        rows = pl.ds(r0, half)
        return pltpu.make_async_copy(x_ref.at[rows, :], n_ref.at[rows, :], o_sem.at[4 + r0 // half])

    def kv_out(place):
        return pltpu.make_async_copy(kv_buf.at[pl.ds(place * own, own), :], kv_ref.at[owners[place]], o_sem.at[place])

    def kv_rows(r0, r1):
        both = jnp.dot(x_ref[r0:r1, :], w_ref[...], preferred_element_type=F32)
        for i in range(nkv):
            kv_buf[r0:r1, i * HEAD:(i + 1) * HEAD] = rope(both[:, i * HEAD:(i + 1) * HEAD], cos_ref[r0:r1, :], sin_ref[r0:r1, :])
        kv_buf[r0:r1, width:] = both[:, width:].astype(BF)

    norm.start(0)
    norm.start(1)
    meet()
    norm.run(start_weights)
    rows_out(0).start()
    for copy in weights:
        copy.wait()
    kv_rows(0, half)
    norm.arrive()
    rows_out(half).start()
    kv_out(0).start()
    kv_out(1).start()
    kv_rows(half, 2 * half)
    kv_out(2).start()
    kv_out(3).start()
    norm.finish()
    rows_out(0).wait()
    rows_out(half).wait()
    for place in range(4):
        kv_out(place).wait()


def kv_proj(srcs, gain, wk, wv, cos, sin, layer, nkv, rb):
    init = len(srcs) == 2
    d = wk.shape[1]
    half = 2 * srcs[0].shape[0] if init else srcs[0].shape[0]
    rows = 2 * half
    width = nkv * HEAD
    return pl.pallas_call(
        functools.partial(kv_kernel, init, layer, nkv, rb),
        in_specs=[hbm()] * (len(srcs) + 5),
        out_specs=[hbm()] * 3,
        out_shape=[jax.ShapeDtypeStruct((half, d), BF), jax.ShapeDtypeStruct((rows, d), BF), jax.ShapeDtypeStruct((4, rows // 4, 2 * width), BF)],
        scratch_shapes=[
            pltpu.VMEM((rows, d), BF),
            pltpu.VMEM((d, 2 * width), BF),
            pltpu.VMEM((rows, 2 * width), BF),
            pltpu.VMEM((rows, HEAD), F32),
            pltpu.VMEM((rows, HEAD), F32),
            pltpu.SemaphoreType.DMA((4,)),
            pltpu.SemaphoreType.DMA((6,)),
        ] + norm_scratch(half, d, rb, init),
        compiler_params=pltpu.CompilerParams(vmem_limit_bytes=VMEM_LIMIT, collective_id=3 if init else 0, has_side_effects=True),
        cost_estimate=pl.CostEstimate(flops=2 * rows * d * 2 * width, bytes_accessed=2 * d * (3 * rows + 2 * width), transcendentals=0),
        name="kv_init" if init else "kv_proj",
    )(*srcs, gain, wk, wv, cos, sin)


def q_blocks(qcols):
    blocks, c = [], 0
    while c < qcols:
        width = min(512 if c else 256, qcols - c)
        blocks.append((c, width))
        c += width
    return blocks


def q_kernel(layer, n_in, *refs):
    ns, trigs, outs = refs[:n_in], refs[n_in:3 * n_in], refs[3 * n_in + 1:4 * n_in + 1]
    wq_ref = refs[3 * n_in]
    x_ref, w_ref, q_buf, cos_ref, sin_ref, w_sem, o_sem, x_sem = refs[4 * n_in + 1:]
    blocks = q_blocks(q_buf.shape[1])
    loads, trig, offs, row = [], [], [], 0
    for i, n_hbm in enumerate(ns):
        rows = pl.ds(row, n_hbm.shape[0])
        loads.append(pltpu.make_async_copy(n_hbm, x_ref.at[rows, :], x_sem.at[i, 0]))
        trig.append(pltpu.make_async_copy(trigs[2 * i], cos_ref.at[rows, :], x_sem.at[i, 1]))
        trig.append(pltpu.make_async_copy(trigs[2 * i + 1], sin_ref.at[rows, :], x_sem.at[i, 2]))
        offs.append(rows)
        row += n_hbm.shape[0]
    weights = [pltpu.make_async_copy(wq_ref.at[layer, :, pl.ds(c, bw)], w_ref.at[:, pl.ds(c, bw)], w_sem.at[i]) for i, (c, bw) in enumerate(blocks)]
    for copy in loads + weights[:1] + trig + weights[1:]:
        copy.start()
    for copy in loads + trig:
        copy.wait()
    stores = []
    for j, (c, bw) in enumerate(blocks):
        weights[j].wait()
        acc = jnp.dot(x_ref[...], w_ref[:, c:c + bw], preferred_element_type=F32)
        for i in range(bw // HEAD):
            q_buf[:, c + i * HEAD:c + (i + 1) * HEAD] = rope(acc[:, i * HEAD:(i + 1) * HEAD], cos_ref[...], sin_ref[...])
        for i, q_ref in enumerate(outs):
            stores.append(pltpu.make_async_copy(q_buf.at[offs[i], pl.ds(c, bw)], q_ref.at[:, pl.ds(c, bw)], o_sem.at[i, j]))
            stores[-1].start()
    for copy in stores:
        copy.wait()


def q_proj(ns, wq, trigs, layer):
    d = ns[0].shape[1]
    rows = sum(n.shape[0] for n in ns)
    qcols = wq.shape[2]
    nb = len(q_blocks(qcols))
    return pl.pallas_call(
        functools.partial(q_kernel, layer, len(ns)),
        in_specs=[hbm()] * (3 * len(ns) + 1),
        out_specs=[hbm()] * len(ns),
        out_shape=[jax.ShapeDtypeStruct((n.shape[0], qcols), BF) for n in ns],
        scratch_shapes=[
            pltpu.VMEM((rows, d), BF),
            pltpu.VMEM((d, qcols), BF),
            pltpu.VMEM((rows, qcols), BF),
            pltpu.VMEM((rows, HEAD), F32),
            pltpu.VMEM((rows, HEAD), F32),
            pltpu.SemaphoreType.DMA((nb,)),
            pltpu.SemaphoreType.DMA((len(ns), nb)),
            pltpu.SemaphoreType.DMA((len(ns), 3)),
        ],
        compiler_params=cparams(),
        cost_estimate=pl.CostEstimate(flops=2 * rows * d * qcols, bytes_accessed=2 * d * (rows + qcols), transcendentals=0),
        name="q_proj",
    )(*ns, *trigs, wq)


SM_C = HEAD ** -0.5 * math.log2(math.e)


def lanes(x, width):
    return jnp.concatenate([x] * (width // HEAD), axis=1) if width > HEAD else x


def flash_step(qs, k, v, ok, m, l, acc):
    s = lax.dot_general(qs, k, (((1,), (1,)), ((), ())), preferred_element_type=F32) * SM_C
    if ok is not None:
        s = jnp.where(ok, s, NEG)
    _, width = s.shape
    m_new = jnp.maximum(m, jnp.max(s, axis=1, keepdims=True))
    alpha = jnp.exp2(m - m_new)
    p = jnp.exp2(s - lanes(m_new, width))
    part = p[:, :HEAD]
    for i in range(1, width // HEAD):
        part = part + p[:, i * HEAD:(i + 1) * HEAD]
    return m_new, l * alpha + part, acc * alpha + jnp.dot(p.astype(BF), v, preferred_element_type=F32)


def flash(q_rows, qi, ql, qi_min, ql_max, kv_ref, bk, nkv, group, lo, hi, m_ref, l_ref, acc_ref):
    rows = qi.shape[0]
    gr = group * rows
    qs = [jnp.concatenate([q_rows(kh * group + i) for i in range(group)], axis=0) for kh in range(nkv)]
    m_ref[:, :gr, :] = jnp.full((nkv, gr, HEAD), NEG, F32)
    l_ref[:, :gr, :] = jnp.zeros((nkv, gr, HEAD), F32)
    acc_ref[:, :gr, :] = jnp.zeros((nkv, gr, HEAD), F32)

    per = kv_ref.shape[1]

    def keys(j, col):
        block = kv_ref[pl.ds(j * (bk // per), bk // per), :, col * HEAD:(col + 1) * HEAD]
        return block.reshape(bk, HEAD)

    def step(j, masked):
        base = j * bk
        ok = None
        if masked:
            kid = base + lax.broadcasted_iota(jnp.int32, (rows, bk), 1)
            ok = (kid <= qi) & (kid >= ql)
            ok = jnp.concatenate([ok] * group, axis=0)
        new = []
        for kh in range(nkv):
            k = keys(j, kh)
            v = keys(j, nkv + kh)
            new.append(flash_step(qs[kh], k, v, ok, m_ref[kh, :gr, :], l_ref[kh, :gr, :], acc_ref[kh, :gr, :]))
        for kh in range(nkv):
            m_ref[kh, :gr, :], l_ref[kh, :gr, :], acc_ref[kh, :gr, :] = new[kh]

    def body(j, carry):
        base = j * bk
        full = (ql_max <= base) & (qi_min >= base + bk - 1)

        @pl.when(full)
        def _():
            step(j, False)

        @pl.when(jnp.logical_not(full))
        def _():
            step(j, True)

        return carry

    lax.fori_loop(lo, hi, body, 0)
    outs = []
    for kh in range(nkv):
        total = jnp.sum(l_ref[kh, :gr, :], axis=1, keepdims=True)
        out = (acc_ref[kh, :gr, :] / total).astype(BF)
        outs += [out[i * rows:(i + 1) * rows, :] for i in range(group)]
    return outs


def attn_kernel(table, mes, nkv, group, nb, na, bks, sc_ref, *refs):
    n_me, n_kv = len(mes), 4 * len(table)
    q_hbm, kv_hbm, o_hbm = refs[:n_me], refs[n_me:n_me + n_kv], refs[n_me + n_kv:2 * n_me + n_kv]
    refs = refs[2 * n_me + n_kv:]
    q_refs, o_refs = refs[:n_me], refs[n_me:2 * n_me]
    kvb_ref, kva_ref, m_ref, l_ref, acc_ref, sem, q_sem, o_sem = refs[2 * n_me:]
    with_a = any(table[me][1] for me in mes)
    t = lax.axis_index('tp')
    p = lax.axis_index('pp')
    load_q = [pltpu.make_async_copy(src, dst, q_sem) for src, dst in zip(q_hbm, q_refs)]
    copies, off_b, off_a = [], 0, 0
    for k, (bk_, ak_) in enumerate(table):
        for s in range(4):
            src = kv_hbm[4 * k + s]
            slot = pl.ds((3 - s) * 4, 4)
            if bk_:
                copies.append(pltpu.make_async_copy(src.at[:, pl.ds(0, bk_), :], kvb_ref.at[slot, pl.ds(off_b, bk_), :], sem))
            if with_a and ak_:
                copies.append(pltpu.make_async_copy(src.at[:, pl.ds(bk_, ak_), :], kva_ref.at[slot, pl.ds(off_a, ak_), :], sem))
        off_b += bk_
        off_a += ak_
    for copy in copies + load_q:
        copy.start()
    for copy in copies + load_q:
        copy.wait()

    def first_key(which, n_own):
        return [sc_ref[4 * which + v] + (3 - p) * 4 * n_own for v in range(4)]

    def lowest(starts, idx):
        low = jnp.zeros_like(idx) + starts[0]
        for v in range(1, 4):
            low = jnp.where(idx >= starts[v], starts[v], low)
        return low

    def one_chunk(me, q_ref, o_ref, out_hbm):
        b, a = table[me]
        own = a + b
        off_b, off_a = sum(x[0] for x in table[:me]), sum(x[1] for x in table[:me])

        def store(o):
            rows = pl.ds(pl.multiple_of(o * own, 16), own)
            return pltpu.make_async_copy(o_ref.at[rows, :], out_hbm.at[rows, :], o_sem)

        if b:
            starts_b = first_key(0, nb)

            def one_owner(o, carry):
                r0 = pl.multiple_of(o * own, 16)
                owner = t ^ (2 * (o % 2) + o // 2)
                i0 = 12 * nb + owner * nb + off_b
                low0 = lowest(starts_b, i0)
                last_low = lowest(starts_b, i0 + b - 1)
                idx = i0 + lax.broadcasted_iota(jnp.int32, (b, 1), 0)
                q_rows = lambda h: q_ref[pl.ds(r0, b), h * HEAD:(h + 1) * HEAD]
                outs = flash(q_rows, idx, lowest(starts_b, idx), i0, last_low, kvb_ref, bks[0], nkv, group, low0 // bks[0], (i0 + b - 1) // bks[0] + 1, m_ref, l_ref, acc_ref)
                for h, out in enumerate(outs):
                    o_ref[pl.ds(r0, b), h * HEAD:(h + 1) * HEAD] = out
                if not a:
                    store(o).start()
                return carry

            lax.fori_loop(0, 4, one_owner, 0)
        if a:
            starts_a = first_key(1, na)
            idx = jnp.concatenate([12 * na + (t ^ OWNER_XOR[o]) * na + off_a + lax.broadcasted_iota(jnp.int32, (a, 1), 0) for o in range(4)], axis=0)
            spans = [(o * own + b, o * own + b + a) for o in range(4)]
            gather = lambda c0, c1: jnp.concatenate([q_ref[r0:r1, c0:c1] for r0, r1 in spans], axis=0)
            n_blocks = 16 * na // bks[1]
            outs = flash(lambda h: gather(h * HEAD, (h + 1) * HEAD), idx, lowest(starts_a, idx), 0, 16 * na, kva_ref, bks[1], nkv, group, starts_a[0] // bks[1], n_blocks, m_ref, l_ref, acc_ref)
            for h, out in enumerate(outs):
                for o, (r0, r1) in enumerate(spans):
                    o_ref[r0:r1, h * HEAD:(h + 1) * HEAD] = out[o * a:(o + 1) * a, :]
            for o in range(4):
                store(o).start()
        return [store(o) for o in range(4)]

    stores = []
    for i, me in enumerate(mes):
        stores += one_chunk(me, q_refs[i], o_refs[i], o_hbm[i])
    for copy in stores:
        copy.wait()


def attention(table, mes, sc, qs, kvs, nkv, group, nb, na, bks):
    qcols = qs[0].shape[1]
    gr = group * max(max(4 * table[me][1], table[me][0]) for me in mes)
    kvw = 2 * nkv * HEAD
    flat = [x for per_chunk in kvs for x in per_chunk]
    flops = sum(4 * (4 * table[me][0] * 16 * nb + 4 * table[me][1] * 16 * na) * qcols for me in mes)
    shapes = [jax.ShapeDtypeStruct(q.shape, BF) for q in qs]
    return pl.pallas_call(
        functools.partial(attn_kernel, table, mes, nkv, group, nb, na, bks),
        in_specs=[pl.BlockSpec(memory_space=pltpu.SMEM)] + [hbm()] * (len(qs) + len(flat)),
        out_specs=[hbm()] * len(qs),
        scratch_shapes=[pltpu.VMEM(q.shape, BF) for q in qs] * 2 + [
            pltpu.VMEM((16, nb, kvw), BF),
            pltpu.VMEM((16, na, kvw), BF),
            pltpu.VMEM((nkv, gr, HEAD), F32),
            pltpu.VMEM((nkv, gr, HEAD), F32),
            pltpu.VMEM((nkv, gr, HEAD), F32),
            pltpu.SemaphoreType.DMA,
            pltpu.SemaphoreType.DMA,
            pltpu.SemaphoreType.DMA,
        ],
        out_shape=shapes,
        compiler_params=cparams(),
        cost_estimate=pl.CostEstimate(flops=flops, bytes_accessed=32 * (nb + na) * kvw, transcendentals=0),
        name="attention",
    )(sc, *qs, *flat)


def oproj_kernel(layer, bn, n_in, *refs):
    o_hbm, w_ref, outs = refs[:n_in], refs[n_in], refs[n_in + 1:2 * n_in + 1]
    o_ref, w_buf, w_sem, o_sem, *scratch = refs[2 * n_in + 1:]
    chip = ChipSum(outs, scratch)
    loads = [pltpu.make_async_copy(w_ref.at[layer, :, pl.ds(i * bn, bn)], w_buf.at[:, pl.ds(i * bn, bn)], w_sem.at[i]) for i in range(chip.n)]
    load_o, row = [], 0
    for i, src in enumerate(o_hbm):
        half = src.shape[0] // 2
        for part in range(2):
            load_o.append(pltpu.make_async_copy(src.at[pl.ds(part * half, half), :], o_ref.at[pl.ds(part * chip.half + row, half), :], o_sem.at[i, part]))
        row += half
    for copy in load_o + loads:
        copy.start()
    meet()
    for copy in load_o:
        copy.wait()
    for i in range(chip.n):
        loads[i].wait()
        if i >= 1:
            chip.send(i - 1).start()
        if i >= 3:
            chip.store(i - 3)
        acc = jnp.dot(o_ref[...], w_buf[:, i * bn:(i + 1) * bn], preferred_element_type=F32)
        if i >= 2:
            chip.combine(i - 2)
        chip.keep(i, acc)
    chip.tail()


def oproj(os, wo, layer):
    k = os[0].shape[1]
    rows = sum(o.shape[0] for o in os)
    d = wo.shape[2]
    bn = min(1024, d // 2)
    half = rows // 2
    return pl.pallas_call(
        functools.partial(oproj_kernel, layer, bn, len(os)),
        in_specs=[hbm()] * (len(os) + 1),
        out_specs=[hbm()] * len(os),
        out_shape=[jax.ShapeDtypeStruct((o.shape[0] // 2, d), BF) for o in os],
        scratch_shapes=[pltpu.VMEM((rows, k), BF), pltpu.VMEM((k, d), BF), pltpu.SemaphoreType.DMA((d // bn,)), pltpu.SemaphoreType.DMA((len(os), 2))] + sum_scratch(half, d, bn),
        compiler_params=pltpu.CompilerParams(vmem_limit_bytes=VMEM_LIMIT, collective_id=1, has_side_effects=True),
        cost_estimate=pl.CostEstimate(flops=2 * rows * k * d, bytes_accessed=2 * (rows * k + k * d + rows * d), transcendentals=0),
        name="oproj",
    )(*os, wo)


def mlp_kernel(layer, bf, bn, rb, n_out, across, *refs):
    srcs = refs[:3]
    gain_ref, wg_ref, wu_ref, wd_ref, ho_ref = refs[3:8]
    outs = refs[8:8 + n_out]
    x_ref, w_ref, both_ref, act_ref, w_sem, f_sem = refs[8 + n_out:14 + n_out]
    scratch = refs[14 + n_out:]
    d = x_ref.shape[1]
    norm = NormExchange(False, rb, srcs, gain_ref, ho_ref, x_ref, scratch[:8])
    chip = ChipSum(outs, scratch[8:], across)
    ff = wg_ref.shape[2]
    n_up = ff // bf
    n_down = chip.n
    half = x_ref.shape[0] // 2

    def up_copies(step):
        slot = step % 3
        cols = pl.ds(pl.multiple_of(step * bf, 128), bf)
        return (
            pltpu.make_async_copy(wg_ref.at[layer, :, cols], w_ref.at[slot, pl.ds(0, wg_ref.shape[1]), pl.ds(0, bf)], w_sem.at[slot, 0]),
            pltpu.make_async_copy(wu_ref.at[layer, :, cols], w_ref.at[slot, pl.ds(0, wg_ref.shape[1]), pl.ds(bf, bf)], w_sem.at[slot, 1]),
        )

    def down_copy(step):
        slot = (step + n_up) % 3
        return pltpu.make_async_copy(wd_ref.at[layer, :, chip.cols(step)], w_ref.at[slot, pl.ds(0, ff), pl.ds(0, bn)], w_sem.at[slot, 0])

    def gated(step):
        slot = step % 2
        gate = both_ref[slot, :, :bf]
        act = gate * jax.nn.sigmoid(gate) * both_ref[slot, :, bf:]
        act_ref[:, pl.ds(pl.multiple_of(step * bf, 128), bf)] = act.astype(BF)

    def first_copies(i):
        cols, dest = pl.ds(i * HEAD, HEAD), 2 * i * HEAD
        return (
            pltpu.make_async_copy(wg_ref.at[layer, :, cols], w_ref.at[0, pl.ds(0, d), pl.ds(dest, HEAD)], f_sem.at[i, 0]),
            pltpu.make_async_copy(wu_ref.at[layer, :, cols], w_ref.at[0, pl.ds(0, d), pl.ds(dest + HEAD, HEAD)], f_sem.at[i, 1]),
        )

    def first(i, r0, r1):
        both = jnp.dot(x_ref[r0:r1, :], w_ref[0, :d, 2 * i * HEAD:2 * (i + 1) * HEAD], preferred_element_type=F32)
        both_ref[0, r0:r1, i * HEAD:(i + 1) * HEAD] = both[:, :HEAD]
        both_ref[0, r0:r1, bf + i * HEAD:bf + (i + 1) * HEAD] = both[:, HEAD:]

    def start_first(parts):
        for i in parts:
            for copy in first_copies(i):
                copy.start()

    def start_up(step):
        for copy in up_copies(step):
            copy.start()

    def wait_up(step):
        for copy in up_copies(step):
            copy.wait()

    n_first = bf // HEAD
    norm.start(0)
    start_first([0])
    norm.start(1)
    meet(across)
    norm.run(lambda: start_first(range(1, n_first)))
    start_up(1)
    start_up(2) if n_up > 2 else down_copy(0).start()
    for i in range(n_first):
        for copy in first_copies(i):
            copy.wait()
        first(i, 0, half)
    norm.arrive()
    for i in range(n_first):
        first(i, half, 2 * half)

    def up(j, carry):
        wait_up(j)

        @pl.when(j + 2 < n_up)
        def _():
            start_up(j + 2)

        @pl.when(j + 2 >= n_up)
        def _():
            down_copy(j + 2 - n_up).start()

        gated(j - 1)
        both_ref[j % 2] = jnp.dot(x_ref[...], w_ref[j % 3, :x_ref.shape[1], :], preferred_element_type=F32)
        return carry

    lax.fori_loop(1, n_up, up, 0)
    gated(n_up - 1)

    def down(i, carry):
        down_copy(i).wait()

        @pl.when(i + 2 < n_down)
        def _():
            down_copy(i + 2).start()

        @pl.when(i >= 1)
        def _():
            chip.send(i - 1).start()

        @pl.when(i >= 3)
        def _():
            chip.store(i - 3)

        acc = jnp.dot(act_ref[...], w_ref[(i + n_up) % 3, :ff, :bn], preferred_element_type=F32)

        @pl.when(i >= 2)
        def _():
            chip.combine(i - 2)

        chip.keep(i, acc)
        return carry

    lax.fori_loop(0, n_down, down, 0)
    chip.tail()
    norm.finish()


def mlp(h, s, t, gain, wg, wu, wd, layer, rb, n_out, across):
    half, d = h.shape
    rows = 2 * half
    ff = wg.shape[2]
    bf = 384
    bn = min(512, d // 2)
    out = jax.ShapeDtypeStruct((half, d), BF)
    part = jax.ShapeDtypeStruct((half // n_out, d), BF)
    return pl.pallas_call(
        functools.partial(mlp_kernel, layer, bf, bn, rb, n_out, across),
        in_specs=[hbm()] * 7,
        out_specs=[hbm()] * (1 + n_out),
        out_shape=[out] + [part] * n_out,
        scratch_shapes=[
            pltpu.VMEM((rows, d), BF),
            pltpu.VMEM((3, max(d, ff), 2 * bf), BF),
            pltpu.VMEM((2, rows, 2 * bf), F32),
            pltpu.VMEM((rows, ff), BF),
            pltpu.SemaphoreType.DMA((3, 2)),
            pltpu.SemaphoreType.DMA((bf // HEAD, 2)),
        ] + norm_scratch(half, d, rb, False) + sum_scratch(half, d, bn, across),
        compiler_params=pltpu.CompilerParams(vmem_limit_bytes=VMEM_LIMIT, collective_id=4 if across else 2, has_side_effects=True),
        cost_estimate=pl.CostEstimate(flops=6 * rows * d * ff, bytes_accessed=2 * (2 * rows * d + 3 * d * ff), transcendentals=rows * ff),
        name="mlp",
    )(h, s, t, gain, wg, wu, wd)


def final_kernel(b, a, off, n_in, *refs):
    srcs, outs = refs[:3], refs[n_in:n_in + 1 + bool(a)]
    bufs, in_sem, out_sem = refs[n_in + 1 + bool(a):n_in + 4 + bool(a)], refs[-2], refs[-1]
    loads = [pltpu.make_async_copy(src.at[pl.ds(0, a + b), :], buf, in_sem.at[i]) for i, (src, buf) in enumerate(zip(srcs, bufs))]
    for copy in loads:
        copy.start()
    for copy in loads:
        copy.wait()

    def block(i, carry):
        rows = pl.ds(pl.multiple_of(i * 16, 16), 16)
        h, s, t = (buf[rows, :].astype(F32) for buf in bufs)
        bufs[0][rows, :] = (h + (s + t)).astype(BF)
        return carry

    lax.fori_loop(0, (a + b) // 16, block, 0)
    stores = [pltpu.make_async_copy(bufs[0].at[pl.ds(0, b), :], outs[0].at[pl.ds(off, b), :], out_sem.at[0])]
    if a:
        stores.append(pltpu.make_async_copy(bufs[0].at[pl.ds(b, a), :], outs[1], out_sem.at[1]))
    for copy in stores:
        copy.start()
    for copy in stores:
        copy.wait()


def final(h, s, t, b, a, off, n_b, out_b):
    d = h.shape[1]
    args = (h, s, t) if out_b is None else (h, s, t, out_b)
    shapes = [jax.ShapeDtypeStruct((n_b, d), BF)] + ([jax.ShapeDtypeStruct((a, d), BF)] if a else [])
    return pl.pallas_call(
        functools.partial(final_kernel, b, a, off, len(args)),
        in_specs=[hbm()] * len(args),
        out_specs=[hbm()] * len(shapes),
        out_shape=shapes,
        input_output_aliases={} if out_b is None else {3: 0},
        scratch_shapes=[pltpu.VMEM((a + b, d), BF)] * 3 + [pltpu.SemaphoreType.DMA((3,)), pltpu.SemaphoreType.DMA((2,))],
        compiler_params=cparams(),
        cost_estimate=pl.CostEstimate(flops=20 * (a + b) * d, bytes_accessed=8 * (a + b) * d, transcendentals=0),
        name="final",
    )(*args)


def solution(mesh):
    row_spec = P(('dp', 'pp', 'tp'), None)
    id_spec = P(('dp', 'pp', 'tp'))
    col_spec = P(None, None, 'tp')
    in_row_spec = P(None, 'tp', None)
    full_spec = P()
    n_pp = mesh.shape['pp']
    across_core = [(i, i ^ 1) for i in range(4)]
    across_y = [(i, i ^ 2) for i in range(4)]

    def per_device(tok_a, seg_a, pos_a, tok_b, seg_b, pos_b, g_attn, wq, wk, wv, wo, g_mlp, wg, wu, wd):
        n_layers, _ = g_attn.shape
        nb, na = tok_b.shape[0], tok_a.shape[0]
        n_kv_all = wk.shape[2] // HEAD
        nkv = n_kv_all // 4
        group = wq.shape[2] // HEAD // nkv
        table = chunk_table(nb, na)
        n_chunks = len(table)
        rb = 16

        off_b, off_a, b0, a0 = [], [], 0, 0
        for b, a in table:
            off_b.append(b0)
            off_a.append(a0)
            b0, a0 = b0 + b, a0 + a
        gain_attn = [g_attn[l:l + 1] for l in range(n_layers)]
        gain_mlp = [g_mlp[l:l + 1] for l in range(n_layers)]

        own_rows = []
        for (b, a), ob, oa in zip(table, off_b, off_a):
            parts = [tok_b[ob:ob + b]] if b else []
            parts += [tok_a[oa:oa + a]] if a else []
            own_rows.append(parts[0] if len(parts) == 1 else jnp.concatenate(parts, axis=0))

        def permute(x, axis, pairs):
            return lax.ppermute(x, axis, pairs)

        def over_core(mine, got):
            pair = jnp.stack([mine, got])
            return jnp.concatenate([pair, permute(pair, 'tp', across_core)], axis=0)

        below = jnp.stack([jnp.sum((seg < v).astype(jnp.int32)) for seg in (seg_b, seg_a) for v in range(4)])
        pos_b_rows = over_core(pos_b, permute(pos_b, 'tp', across_y))
        got_rows = [permute(own_rows[k], 'tp', across_y) for k in range(n_chunks)]
        got_pos_a, got_below = permute(pos_a, 'tp', across_y), permute(below, 'tp', across_y)

        inv_freq = jnp.power(ROPE_BASE, -2.0 * jnp.arange(HEAD // 2, dtype=F32) / HEAD)

        def trig(pos):
            angles = pos.astype(F32)[..., None] * inv_freq
            cos, sin = jnp.cos(angles), jnp.sin(angles)
            return jnp.concatenate([cos, cos], axis=-1), jnp.concatenate([-sin, sin], axis=-1)

        def chunk_trig(k, after):
            (b, a), ob, oa = table[k], off_b[k], off_a[k]
            parts = ([pos_b_rows[:, ob:ob + b]] if b else []) + ([pos_a_rows[:, oa:oa + a]] if a else [])
            pos = (parts[0] if len(parts) == 1 else jnp.concatenate(parts, axis=1)).reshape(4 * (a + b))
            if after is not None:
                pos, _ = lax.optimization_barrier((pos, after))
            return trig(pos)

        cos, sin = [None] * n_chunks, [None] * n_chunks
        bk_b, bk_a = min(512, 16 * nb), min(512, 16 * na)
        out_b, out_a = None, None
        srcs = list(zip(own_rows, got_rows))
        h = [None] * n_chunks
        for l in range(n_layers):
            q, kvs, n = [None] * n_chunks, [None] * n_chunks, [None] * n_chunks
            last = l + 1 == n_layers
            for k in range(n_chunks):
                if l == 0:
                    cos[k], sin[k] = chunk_trig(k, kvs[k - 1][0] if k else None)
                h[k], n[k], kv = kv_proj(srcs[k], gain_attn[l], wk, wv, cos[k], sin[k], l, nkv, rb)
                if l == 0 and k == 0:
                    got_pos_a, got_below, _ = lax.optimization_barrier((got_pos_a, got_below, kv))
                    pos_a_rows = over_core(pos_a, got_pos_a)
                    below = jnp.sum(over_core(below, got_below), axis=0)
                    others = [permute(below, 'pp', [(i, (i + s) % n_pp) for i in range(n_pp)]) for s in range(1, n_pp)]
                    starts = below + others[0] + others[1] + others[2]
                kvs[k] = [kv]
                for s in range(1, n_pp):
                    if k == 2 or (k == 0 and l):
                        kvs[k].append(permute(kv, 'pp', [(i, i + s) for i in range(n_pp - s)]))
                    else:
                        kvs[k].append(permute(kvs[k][-1], 'pp', [(i, i + 1) for i in range(s - 1, n_pp - 1)]))
            sums = []
            groups = ([0], [k for k in range(1, n_chunks)])
            for members in groups:
                qs = q_proj([n[k] for k in members], wq, [x for k in members for x in (cos[k], sin[k])], l)
                for k, x in zip(members, qs):
                    q[k] = x
            for members in groups:
                os = attention(table, members, starts, [q[k] for k in members], kvs, nkv, group, nb, na, (bk_b, bk_a))
                parts = oproj(os, wo, l)
                for k, x in zip(members, parts):
                    sums.append((x, permute(x, 'tp', across_y)))
            for k in range(n_chunks):
                across = last and k + 1 == n_chunks
                h[k], *parts = mlp(h[k], *sums[k], gain_mlp[l], wg, wu, wd, l, rb, 2 if last else 1, across)
                got = parts[-1] if across else permute(parts[-1], 'tp', across_y)
                srcs[k] = (h[k], parts[0], got)
        for k, ((b, a), parts) in enumerate(zip(table, srcs)):
            out_b, *rest = final(*parts, b, a, off_b[k], nb, out_b)
            out_a = rest[0] if rest else out_a
        return out_a, out_b

    def prefill(tokens_a, segment_a, position_a, tokens_b, segment_b, position_b, norm_attn, w_query, w_key, w_value, w_out, norm_mlp, w_gate, w_up, w_down):
        mapped = jax.shard_map(per_device, mesh=mesh, in_specs=(row_spec, id_spec, id_spec, row_spec, id_spec, id_spec, full_spec, col_spec, full_spec, full_spec, in_row_spec, full_spec, col_spec, col_spec, in_row_spec), out_specs=(row_spec, row_spec), check_vma=False)
        return mapped(tokens_a, segment_a, position_a, tokens_b, segment_b, position_b, norm_attn, w_query, w_key, w_value, w_out, norm_mlp, w_gate, w_up, w_down)

    return prefill
```

```python
import functools
import math
import jax
import jax.numpy as jnp
from jax import lax
from jax.experimental import pallas as pl
from jax.experimental.pallas import tpu as pltpu
from jax.sharding import PartitionSpec as P

HEAD = 128
ROPE_BASE = 500000.0
EPS = 1e-5
NEG = -1e30
BF = jnp.bfloat16
F32 = jnp.float32
VMEM_LIMIT = 63 * 1024 * 1024
OWNER_XOR = (0, 2, 1, 3)


def chunk_table(nb, na):
    if nb == 256:
        return [(112, 0), (80, 32), (64, 0)]
    return [(nb // 2, na), (nb // 2, 0)]


def cparams(semantics=None, limit=VMEM_LIMIT):
    return pltpu.CompilerParams(dimension_semantics=semantics, vmem_limit_bytes=limit)


def hbm():
    return pl.BlockSpec(memory_space=pltpu.HBM)


MESH = pl.DeviceIdType.MESH


def other_core():
    t = lax.axis_index('tp')
    return {'tp': t + 1 - 2 * (t % 2)}


def other_side():
    return {'tp': (lax.axis_index('tp') + 2) % 4}


def meet(across=False):
    barrier = pltpu.get_barrier_semaphore()
    peers = [other_core()] + ([other_side()] if across else [])
    for peer in peers:
        pl.semaphore_signal(barrier, inc=1, device_id=peer, device_id_type=MESH)
    pl.semaphore_wait(barrier, len(peers))


def norm_rows(wide, gain):
    inv = lax.rsqrt(jnp.mean(wide * wide, axis=-1, keepdims=True) + EPS)
    return (wide * inv * gain).astype(BF)


def norm_scratch(half, d, rb, init):
    n = half // rb
    bufs = [pltpu.VMEM((half, d), BF)] * (1 if init else 3)
    return bufs + [pltpu.VMEM((1, d), BF), pltpu.SemaphoreType.DMA((2, 4)), pltpu.SemaphoreType.DMA((n,)), pltpu.SemaphoreType.DMA((n,)), pltpu.SemaphoreType.DMA]


class NormExchange:
    def __init__(self, init, rb, srcs, gain_ref, ho_ref, x_ref, scratch):
        self.init, self.rb, self.srcs, self.gain_ref, self.ho_ref, self.x_ref = init, rb, srcs, gain_ref, ho_ref, x_ref
        self.bufs = scratch[:1 if init else 3]
        self.gain_buf, self.in_sem, self.send_sem, self.recv_sem, self.out_sem = scratch[1 if init else 3:]
        self.half = x_ref.shape[0] // 2
        self.own = self.half // 2
        self.n = self.half // rb

    def gain(self, piece):
        return [] if piece else [pltpu.make_async_copy(self.gain_ref, self.gain_buf, self.in_sem.at[0, 3])]

    def loads(self, piece):
        q = self.own
        dst = pl.ds(piece * q, q)
        if self.init:
            return self.gain(piece) + [pltpu.make_async_copy(self.srcs[piece], self.bufs[0].at[dst, :], self.in_sem.at[piece, 0])]
        src = (dst, dst, pl.ds((1 - piece) * q, q))
        return self.gain(piece) + [pltpu.make_async_copy(ref.at[rows, :], buf.at[dst, :], self.in_sem.at[piece, i]) for i, (ref, rows, buf) in enumerate(zip(self.srcs, src, self.bufs))]

    def send(self, i):
        rows = pl.ds(pl.multiple_of(i * self.rb, self.rb), self.rb)
        there = pl.ds(pl.multiple_of(self.half + i * self.rb, self.rb), self.rb)
        return pltpu.make_async_remote_copy(src_ref=self.x_ref.at[rows, :], dst_ref=self.x_ref.at[there, :], send_sem=self.send_sem.at[i], recv_sem=self.recv_sem.at[i], device_id=other_core(), device_id_type=MESH)

    def store(self):
        return pltpu.make_async_copy(self.bufs[0], self.ho_ref, self.out_sem)

    def start(self, piece):
        for copy in self.loads(piece):
            copy.start()

    def run(self, after_first):
        per = self.n // 2

        def block(i, carry):
            rows = pl.ds(pl.multiple_of(i * self.rb, self.rb), self.rb)
            if self.init:
                h = self.bufs[0][rows, :]
            else:
                hb, sb, tb = self.bufs
                h = (hb[rows, :].astype(F32) + (sb[rows, :].astype(F32) + tb[rows, :].astype(F32))).astype(BF)
                hb[rows, :] = h
            self.x_ref[rows, :] = norm_rows(h.astype(F32), self.gain_buf[...].astype(F32))

            @pl.when(i >= 1)
            def _():
                self.send(i - 1).start()

            return carry

        for piece in range(2):
            for copy in self.loads(piece):
                copy.wait()
            if piece == 0:
                after_first()
            lax.fori_loop(piece * per, (piece + 1) * per, block, 0)
        self.store().start()
        self.send(self.n - 1).start()

    def arrive(self):
        for i in range(self.n):
            self.send(i).wait_recv()

    def finish(self):
        for i in range(self.n):
            self.send(i).wait_send()
        self.store().wait()


def sum_scratch(half, d, bn, across=False):
    n = d // bn
    extra = [pltpu.VMEM((half // 2, d), BF), pltpu.SemaphoreType.DMA((n,)), pltpu.SemaphoreType.DMA((n,)), pltpu.SemaphoreType.DMA]
    return [
        pltpu.VMEM((3, half, bn), F32),
        pltpu.VMEM((n, half, bn), BF),
        pltpu.VMEM((n, half, bn), BF),
        pltpu.VMEM((half, d), BF),
        pltpu.SemaphoreType.DMA((n,)),
        pltpu.SemaphoreType.DMA((n,)),
        pltpu.SemaphoreType.DMA((n,)),
    ] + (extra if across else [])


class ChipSum:
    def __init__(self, outs, scratch, across=False):
        self.across = across
        self.outs = outs
        self.mine, self.give, self.got, self.total, self.send_sem, self.recv_sem, self.out_sem, *extra = scratch
        if across:
            self.far, self.y_send, self.y_recv, self.far_sem = extra
        self.n, self.half, self.bn = self.give.shape

    def send(self, i):
        return pltpu.make_async_remote_copy(src_ref=self.give.at[i], dst_ref=self.got.at[i], send_sem=self.send_sem.at[i], recv_sem=self.recv_sem.at[i], device_id=other_core(), device_id_type=MESH)

    def send_far(self, i):
        q = self.half // 2
        return pltpu.make_async_remote_copy(src_ref=self.total.at[pl.ds(q, q), self.cols(i)], dst_ref=self.far.at[:, self.cols(i)], send_sem=self.y_send.at[i], recv_sem=self.y_recv.at[i], device_id=other_side(), device_id_type=MESH)

    def cols(self, i):
        return pl.ds(pl.multiple_of(i * self.bn, 128), self.bn)

    def stores(self, i):
        copies, row = [], 0
        for out in self.outs[:1] if self.across else self.outs:
            copies.append(pltpu.make_async_copy(self.total.at[pl.ds(row, out.shape[0]), self.cols(i)], out.at[:, self.cols(i)], self.out_sem.at[i]))
            row += out.shape[0]
        return copies

    def keep(self, i, acc):
        self.mine[i % 3] = acc[:self.half]
        self.give[i] = acc[self.half:].astype(BF)

    def combine(self, i):
        self.send(i).wait_recv()
        self.total[:, self.cols(i)] = (self.mine[i % 3] + self.got[i].astype(F32)).astype(BF)

    def store(self, i):
        if self.across:
            self.send_far(i).start()
        for copy in self.stores(i):
            copy.start()

    def tail(self):
        last = self.n - 1
        self.send(last).start()
        if self.n >= 3:
            self.store(last - 2)
        self.combine(last - 1)
        self.store(last - 1)
        self.combine(last)
        self.store(last)
        for i in range(self.n):
            self.send(i).wait_send()
            for copy in self.stores(i):
                copy.wait()
        if self.across:
            for i in range(self.n):
                self.send_far(i).wait()
            copy = pltpu.make_async_copy(self.far, self.outs[1], self.far_sem)
            copy.start()
            copy.wait()


def rope(vals, cos, sin):
    return (vals * cos + pltpu.roll(vals, HEAD // 2, 1) * sin).astype(BF)


def kv_kernel(init, layer, nkv, rb, *refs):
    n_src = 2 if init else 3
    srcs = refs[:n_src]
    gain_ref, wk_ref, wv_ref, cos_hbm, sin_hbm, ho_ref, n_ref, kv_ref, x_ref, w_ref, kv_buf, cos_ref, sin_ref, w_sem, o_sem = refs[n_src:n_src + 15]
    norm = NormExchange(init, rb, srcs, gain_ref, ho_ref, x_ref, refs[n_src + 15:])
    half = x_ref.shape[0] // 2
    own = half // 2
    width = nkv * HEAD
    t = lax.axis_index('tp')
    cols = pl.ds(pl.multiple_of(t * width, 128), width)
    weights = [
        pltpu.make_async_copy(wk_ref.at[layer, :, cols], w_ref.at[:, pl.ds(0, width)], w_sem.at[0]),
        pltpu.make_async_copy(wv_ref.at[layer, :, cols], w_ref.at[:, pl.ds(width, width)], w_sem.at[1]),
        pltpu.make_async_copy(cos_hbm, cos_ref, w_sem.at[2]),
        pltpu.make_async_copy(sin_hbm, sin_ref, w_sem.at[3]),
    ]
    owners = (t, (t + 2) % 4, t + 1 - 2 * (t % 2), 3 - t)

    def start_weights():
        for copy in weights:
            copy.start()

    def rows_out(r0):
        rows = pl.ds(r0, half)
        return pltpu.make_async_copy(x_ref.at[rows, :], n_ref.at[rows, :], o_sem.at[4 + r0 // half])

    def kv_out(place):
        return pltpu.make_async_copy(kv_buf.at[pl.ds(place * own, own), :], kv_ref.at[owners[place]], o_sem.at[place])

    def kv_rows(r0, r1):
        both = jnp.dot(x_ref[r0:r1, :], w_ref[...], preferred_element_type=F32)
        for i in range(nkv):
            kv_buf[r0:r1, i * HEAD:(i + 1) * HEAD] = rope(both[:, i * HEAD:(i + 1) * HEAD], cos_ref[r0:r1, :], sin_ref[r0:r1, :])
        kv_buf[r0:r1, width:] = both[:, width:].astype(BF)

    norm.start(0)
    norm.start(1)
    meet()
    norm.run(start_weights)
    rows_out(0).start()
    for copy in weights:
        copy.wait()
    kv_rows(0, half)
    norm.arrive()
    rows_out(half).start()
    kv_out(0).start()
    kv_out(1).start()
    kv_rows(half, 2 * half)
    kv_out(2).start()
    kv_out(3).start()
    norm.finish()
    rows_out(0).wait()
    rows_out(half).wait()
    for place in range(4):
        kv_out(place).wait()


def kv_proj(srcs, gain, wk, wv, cos, sin, layer, nkv, rb):
    init = len(srcs) == 2
    d = wk.shape[1]
    half = 2 * srcs[0].shape[0] if init else srcs[0].shape[0]
    rows = 2 * half
    width = nkv * HEAD
    return pl.pallas_call(
        functools.partial(kv_kernel, init, layer, nkv, rb),
        in_specs=[hbm()] * (len(srcs) + 5),
        out_specs=[hbm()] * 3,
        out_shape=[jax.ShapeDtypeStruct((half, d), BF), jax.ShapeDtypeStruct((rows, d), BF), jax.ShapeDtypeStruct((4, rows // 4, 2 * width), BF)],
        scratch_shapes=[
            pltpu.VMEM((rows, d), BF),
            pltpu.VMEM((d, 2 * width), BF),
            pltpu.VMEM((rows, 2 * width), BF),
            pltpu.VMEM((rows, HEAD), F32),
            pltpu.VMEM((rows, HEAD), F32),
            pltpu.SemaphoreType.DMA((4,)),
            pltpu.SemaphoreType.DMA((6,)),
        ] + norm_scratch(half, d, rb, init),
        compiler_params=pltpu.CompilerParams(vmem_limit_bytes=VMEM_LIMIT, collective_id=3 if init else 0, has_side_effects=True),
        cost_estimate=pl.CostEstimate(flops=2 * rows * d * 2 * width, bytes_accessed=2 * d * (3 * rows + 2 * width), transcendentals=0),
        name="kv_init" if init else "kv_proj",
    )(*srcs, gain, wk, wv, cos, sin)


def q_kernel(n_in, layer_ref, *refs):
    ns, trigs, outs = refs[:n_in], refs[n_in:3 * n_in], refs[3 * n_in + 1:4 * n_in + 1]
    wq_ref = refs[3 * n_in]
    x_ref, w_ref, q_buf, cos_ref, sin_ref, w_sem, o_sem, x_sem = refs[4 * n_in + 1:]
    layer = layer_ref[0]
    bq = w_ref.shape[2]
    loads, trig, offs, row = [], [], [], 0
    for i, n_hbm in enumerate(ns):
        rows = pl.ds(row, n_hbm.shape[0])
        loads.append(pltpu.make_async_copy(n_hbm, x_ref.at[rows, :], x_sem.at[i, 0]))
        trig.append(pltpu.make_async_copy(trigs[2 * i], cos_ref.at[rows, :], x_sem.at[i, 1]))
        trig.append(pltpu.make_async_copy(trigs[2 * i + 1], sin_ref.at[rows, :], x_sem.at[i, 2]))
        offs.append(rows)
        row += n_hbm.shape[0]

    def weight(j):
        return pltpu.make_async_copy(wq_ref.at[layer, :, pl.ds(pl.multiple_of(j * bq, 128), bq)], w_ref.at[j], w_sem.at[j])

    def stores(j):
        cols = pl.ds(pl.multiple_of(j * bq, 128), bq)
        return [pltpu.make_async_copy(q_buf.at[j, rows, :], q_ref.at[:, cols], o_sem.at[i]) for i, (rows, q_ref) in enumerate(zip(offs, outs))]

    n_blocks = w_ref.shape[0]
    for copy in loads + [weight(0)] + trig + [weight(j) for j in range(1, n_blocks)]:
        copy.start()
    for copy in loads + trig:
        copy.wait()

    def block(j, carry):
        weight(j).wait()
        acc = jnp.dot(x_ref[...], w_ref[j], preferred_element_type=F32)
        for i in range(bq // HEAD):
            q_buf[j, :, i * HEAD:(i + 1) * HEAD] = rope(acc[:, i * HEAD:(i + 1) * HEAD], cos_ref[...], sin_ref[...])
        for copy in stores(j):
            copy.start()
        return carry

    lax.fori_loop(0, n_blocks, block, 0)
    for j in range(n_blocks):
        for copy in stores(j):
            copy.wait()


def q_proj(ns, wq, trigs, layer):
    d = ns[0].shape[1]
    rows = sum(n.shape[0] for n in ns)
    qcols = wq.shape[2]
    bq = 256
    nb = qcols // bq
    return pl.pallas_call(
        functools.partial(q_kernel, len(ns)),
        in_specs=[pl.BlockSpec(memory_space=pltpu.SMEM)] + [hbm()] * (3 * len(ns) + 1),
        out_specs=[hbm()] * len(ns),
        out_shape=[jax.ShapeDtypeStruct((n.shape[0], qcols), BF) for n in ns],
        scratch_shapes=[
            pltpu.VMEM((rows, d), BF),
            pltpu.VMEM((nb, d, bq), BF),
            pltpu.VMEM((nb, rows, bq), BF),
            pltpu.VMEM((rows, HEAD), F32),
            pltpu.VMEM((rows, HEAD), F32),
            pltpu.SemaphoreType.DMA((nb,)),
            pltpu.SemaphoreType.DMA((len(ns),)),
            pltpu.SemaphoreType.DMA((len(ns), 3)),
        ],
        compiler_params=cparams(),
        cost_estimate=pl.CostEstimate(flops=2 * rows * d * qcols, bytes_accessed=2 * d * (rows + qcols), transcendentals=0),
        name="q_proj",
    )(jnp.full((1,), layer, jnp.int32), *ns, *trigs, wq)


SM_C = HEAD ** -0.5 * math.log2(math.e)


def lanes(x, width):
    return jnp.concatenate([x] * (width // HEAD), axis=1) if width > HEAD else x


def flash_step(qs, k, v, ok, m, l, acc):
    s = lax.dot_general(qs, k, (((1,), (1,)), ((), ())), preferred_element_type=F32) * SM_C
    if ok is not None:
        s = jnp.where(ok, s, NEG)
    _, width = s.shape
    m_new = jnp.maximum(m, jnp.max(s, axis=1, keepdims=True))
    alpha = jnp.exp2(m - m_new)
    p = jnp.exp2(s - lanes(m_new, width))
    part = p[:, :HEAD]
    for i in range(1, width // HEAD):
        part = part + p[:, i * HEAD:(i + 1) * HEAD]
    return m_new, l * alpha + part, acc * alpha + jnp.dot(p.astype(BF), v, preferred_element_type=F32)


def flash(q_rows, qi, ql, qi_min, ql_max, kv_ref, bk, nkv, group, lo, hi, m_ref, l_ref, acc_ref):
    rows = qi.shape[0]
    gr = group * rows
    qs = [jnp.concatenate([q_rows(kh * group + i) for i in range(group)], axis=0) for kh in range(nkv)]
    m_ref[:, :gr, :] = jnp.full((nkv, gr, HEAD), NEG, F32)
    l_ref[:, :gr, :] = jnp.zeros((nkv, gr, HEAD), F32)
    acc_ref[:, :gr, :] = jnp.zeros((nkv, gr, HEAD), F32)

    per = kv_ref.shape[1]

    def keys(j, col):
        block = kv_ref[pl.ds(j * (bk // per), bk // per), :, col * HEAD:(col + 1) * HEAD]
        return block.reshape(bk, HEAD)

    def step(j, masked):
        base = j * bk
        ok = None
        if masked:
            kid = base + lax.broadcasted_iota(jnp.int32, (rows, bk), 1)
            ok = (kid <= qi) & (kid >= ql)
            ok = jnp.concatenate([ok] * group, axis=0)
        new = []
        for kh in range(nkv):
            k = keys(j, kh)
            v = keys(j, nkv + kh)
            new.append(flash_step(qs[kh], k, v, ok, m_ref[kh, :gr, :], l_ref[kh, :gr, :], acc_ref[kh, :gr, :]))
        for kh in range(nkv):
            m_ref[kh, :gr, :], l_ref[kh, :gr, :], acc_ref[kh, :gr, :] = new[kh]

    def body(j, carry):
        base = j * bk
        full = (ql_max <= base) & (qi_min >= base + bk - 1)

        @pl.when(full)
        def _():
            step(j, False)

        @pl.when(jnp.logical_not(full))
        def _():
            step(j, True)

        return carry

    lax.fori_loop(lo, hi, body, 0)
    outs = []
    for kh in range(nkv):
        total = jnp.sum(l_ref[kh, :gr, :], axis=1, keepdims=True)
        out = (acc_ref[kh, :gr, :] / total).astype(BF)
        outs += [out[i * rows:(i + 1) * rows, :] for i in range(group)]
    return outs


def attn_kernel(table, mes, nkv, group, nb, na, bks, sc_ref, *refs):
    n_me, n_kv = len(mes), 4 * len(table)
    q_hbm, kv_hbm, o_hbm = refs[:n_me], refs[n_me:n_me + n_kv], refs[n_me + n_kv:2 * n_me + n_kv]
    refs = refs[2 * n_me + n_kv:]
    q_refs, o_refs = refs[:n_me], refs[n_me:2 * n_me]
    kvb_ref, kva_ref, m_ref, l_ref, acc_ref, sem, q_sem, o_sem = refs[2 * n_me:]
    with_a = any(table[me][1] for me in mes)
    t = lax.axis_index('tp')
    p = lax.axis_index('pp')
    load_q = [pltpu.make_async_copy(src, dst, q_sem) for src, dst in zip(q_hbm, q_refs)]
    copies, off_b, off_a = [], 0, 0
    for k, (bk_, ak_) in enumerate(table):
        for s in range(4):
            src = kv_hbm[4 * k + s]
            slot = pl.ds((3 - s) * 4, 4)
            if bk_:
                copies.append(pltpu.make_async_copy(src.at[:, pl.ds(0, bk_), :], kvb_ref.at[slot, pl.ds(off_b, bk_), :], sem))
            if with_a and ak_:
                copies.append(pltpu.make_async_copy(src.at[:, pl.ds(bk_, ak_), :], kva_ref.at[slot, pl.ds(off_a, ak_), :], sem))
        off_b += bk_
        off_a += ak_
    for copy in copies + load_q:
        copy.start()
    for copy in copies + load_q:
        copy.wait()

    def first_key(which, n_own):
        return [sc_ref[4 * which + v] + (3 - p) * 4 * n_own for v in range(4)]

    def lowest(starts, idx):
        low = jnp.zeros_like(idx) + starts[0]
        for v in range(1, 4):
            low = jnp.where(idx >= starts[v], starts[v], low)
        return low

    def one_chunk(me, q_ref, o_ref, out_hbm):
        b, a = table[me]
        own = a + b
        off_b, off_a = sum(x[0] for x in table[:me]), sum(x[1] for x in table[:me])

        def store(o):
            rows = pl.ds(pl.multiple_of(o * own, 16), own)
            return pltpu.make_async_copy(o_ref.at[rows, :], out_hbm.at[rows, :], o_sem)

        if b:
            starts_b = first_key(0, nb)

            def one_owner(o, carry):
                r0 = pl.multiple_of(o * own, 16)
                owner = t ^ (2 * (o % 2) + o // 2)
                i0 = 12 * nb + owner * nb + off_b
                low0 = lowest(starts_b, i0)
                last_low = lowest(starts_b, i0 + b - 1)
                idx = i0 + lax.broadcasted_iota(jnp.int32, (b, 1), 0)
                q_rows = lambda h: q_ref[pl.ds(r0, b), h * HEAD:(h + 1) * HEAD]
                outs = flash(q_rows, idx, lowest(starts_b, idx), i0, last_low, kvb_ref, bks[0], nkv, group, low0 // bks[0], (i0 + b - 1) // bks[0] + 1, m_ref, l_ref, acc_ref)
                for h, out in enumerate(outs):
                    o_ref[pl.ds(r0, b), h * HEAD:(h + 1) * HEAD] = out
                if not a:
                    store(o).start()
                return carry

            lax.fori_loop(0, 4, one_owner, 0)
        if a:
            starts_a = first_key(1, na)
            idx = jnp.concatenate([12 * na + (t ^ OWNER_XOR[o]) * na + off_a + lax.broadcasted_iota(jnp.int32, (a, 1), 0) for o in range(4)], axis=0)
            spans = [(o * own + b, o * own + b + a) for o in range(4)]
            gather = lambda c0, c1: jnp.concatenate([q_ref[r0:r1, c0:c1] for r0, r1 in spans], axis=0)
            n_blocks = 16 * na // bks[1]
            outs = flash(lambda h: gather(h * HEAD, (h + 1) * HEAD), idx, lowest(starts_a, idx), 0, 16 * na, kva_ref, bks[1], nkv, group, starts_a[0] // bks[1], n_blocks, m_ref, l_ref, acc_ref)
            for h, out in enumerate(outs):
                for o, (r0, r1) in enumerate(spans):
                    o_ref[r0:r1, h * HEAD:(h + 1) * HEAD] = out[o * a:(o + 1) * a, :]
            for o in range(4):
                store(o).start()
        return [store(o) for o in range(4)]

    stores = []
    for i, me in enumerate(mes):
        stores += one_chunk(me, q_refs[i], o_refs[i], o_hbm[i])
    for copy in stores:
        copy.wait()


def attention(table, mes, sc, qs, kvs, nkv, group, nb, na, bks):
    qcols = qs[0].shape[1]
    gr = group * max(max(4 * table[me][1], table[me][0]) for me in mes)
    kvw = 2 * nkv * HEAD
    flat = [x for per_chunk in kvs for x in per_chunk]
    flops = sum(4 * (4 * table[me][0] * 16 * nb + 4 * table[me][1] * 16 * na) * qcols for me in mes)
    shapes = [jax.ShapeDtypeStruct(q.shape, BF) for q in qs]
    return pl.pallas_call(
        functools.partial(attn_kernel, table, mes, nkv, group, nb, na, bks),
        in_specs=[pl.BlockSpec(memory_space=pltpu.SMEM)] + [hbm()] * (len(qs) + len(flat)),
        out_specs=[hbm()] * len(qs),
        scratch_shapes=[pltpu.VMEM(q.shape, BF) for q in qs] * 2 + [
            pltpu.VMEM((16, nb, kvw), BF),
            pltpu.VMEM((16, na, kvw), BF),
            pltpu.VMEM((nkv, gr, HEAD), F32),
            pltpu.VMEM((nkv, gr, HEAD), F32),
            pltpu.VMEM((nkv, gr, HEAD), F32),
            pltpu.SemaphoreType.DMA,
            pltpu.SemaphoreType.DMA,
            pltpu.SemaphoreType.DMA,
        ],
        out_shape=shapes,
        compiler_params=cparams(),
        cost_estimate=pl.CostEstimate(flops=flops, bytes_accessed=32 * (nb + na) * kvw, transcendentals=0),
        name="attention",
    )(sc, *qs, *flat)


def oproj_kernel(layer, n_in, *refs):
    o_hbm, w_ref, outs = refs[:n_in], refs[n_in], refs[n_in + 1:2 * n_in + 1]
    o_ref, w_buf, w_sem, o_sem, *scratch = refs[2 * n_in + 1:]
    chip = ChipSum(outs, scratch)

    def load(i):
        return pltpu.make_async_copy(w_ref.at[layer, :, chip.cols(i)], w_buf.at[i], w_sem.at[i])

    load_o, row = [], 0
    for i, src in enumerate(o_hbm):
        half = src.shape[0] // 2
        for part in range(2):
            load_o.append(pltpu.make_async_copy(src.at[pl.ds(part * half, half), :], o_ref.at[pl.ds(part * chip.half + row, half), :], o_sem.at[i, part]))
        row += half
    for copy in load_o + [load(i) for i in range(chip.n)]:
        copy.start()
    meet()
    for copy in load_o:
        copy.wait()

    def block(i, carry):
        load(i).wait()

        @pl.when(i >= 1)
        def _():
            chip.send(i - 1).start()

        @pl.when(i >= 3)
        def _():
            chip.store(i - 3)

        acc = jnp.dot(o_ref[...], w_buf[i], preferred_element_type=F32)

        @pl.when(i >= 2)
        def _():
            chip.combine(i - 2)

        chip.keep(i, acc)
        return carry

    lax.fori_loop(0, chip.n, block, 0)
    chip.tail()


def oproj(os, wo, layer):
    k = os[0].shape[1]
    rows = sum(o.shape[0] for o in os)
    d = wo.shape[2]
    bn = min(512, d // 2)
    half = rows // 2
    return pl.pallas_call(
        functools.partial(oproj_kernel, layer, len(os)),
        in_specs=[hbm()] * (len(os) + 1),
        out_specs=[hbm()] * len(os),
        out_shape=[jax.ShapeDtypeStruct((o.shape[0] // 2, d), BF) for o in os],
        scratch_shapes=[pltpu.VMEM((rows, k), BF), pltpu.VMEM((d // bn, k, bn), BF), pltpu.SemaphoreType.DMA((d // bn,)), pltpu.SemaphoreType.DMA((len(os), 2))] + sum_scratch(half, d, bn),
        compiler_params=pltpu.CompilerParams(vmem_limit_bytes=VMEM_LIMIT, collective_id=1, has_side_effects=True),
        cost_estimate=pl.CostEstimate(flops=2 * rows * k * d, bytes_accessed=2 * (rows * k + k * d + rows * d), transcendentals=0),
        name="oproj",
    )(*os, wo)


def mlp_kernel(layer, bf, bn, rb, n_out, across, *refs):
    srcs = refs[:3]
    gain_ref, wg_ref, wu_ref, wd_ref, ho_ref = refs[3:8]
    outs = refs[8:8 + n_out]
    x_ref, w_ref, both_ref, act_ref, w_sem = refs[8 + n_out:13 + n_out]
    scratch = refs[13 + n_out:]
    norm = NormExchange(False, rb, srcs, gain_ref, ho_ref, x_ref, scratch[:8])
    chip = ChipSum(outs, scratch[8:], across)
    ff = wg_ref.shape[2]
    n_up = ff // bf
    n_down = chip.n

    def up_copies(step):
        slot = step % 3
        cols = pl.ds(pl.multiple_of(step * bf, 128), bf)
        return (
            pltpu.make_async_copy(wg_ref.at[layer, :, cols], w_ref.at[slot, pl.ds(0, wg_ref.shape[1]), pl.ds(0, bf)], w_sem.at[slot, 0]),
            pltpu.make_async_copy(wu_ref.at[layer, :, cols], w_ref.at[slot, pl.ds(0, wg_ref.shape[1]), pl.ds(bf, bf)], w_sem.at[slot, 1]),
        )

    def down_copy(step):
        slot = (step + n_up) % 3
        return pltpu.make_async_copy(wd_ref.at[layer, :, chip.cols(step)], w_ref.at[slot, pl.ds(0, ff), pl.ds(0, bn)], w_sem.at[slot, 0])

    def gated(step):
        slot = step % 2
        gate = both_ref[slot, :, :bf]
        act = gate * jax.nn.sigmoid(gate) * both_ref[slot, :, bf:]
        act_ref[:, pl.ds(pl.multiple_of(step * bf, 128), bf)] = act.astype(BF)

    def start_up(step):
        for copy in up_copies(step):
            copy.start()

    def wait_up(step):
        for copy in up_copies(step):
            copy.wait()

    norm.start(0)
    norm.start(1)
    start_up(0)
    meet(across)
    norm.run(lambda: start_up(1))
    norm.arrive()

    def up(j, carry):
        wait_up(j)

        @pl.when(j + 2 < n_up)
        def _():
            start_up(j + 2)

        @pl.when(j + 2 >= n_up)
        def _():
            down_copy(j + 2 - n_up).start()

        gated(jnp.maximum(j - 1, 0))
        both_ref[j % 2] = jnp.dot(x_ref[...], w_ref[j % 3, :x_ref.shape[1], :], preferred_element_type=F32)
        return carry

    lax.fori_loop(0, n_up, up, 0)
    gated(n_up - 1)

    def down(i, carry):
        down_copy(i).wait()

        @pl.when(i + 2 < n_down)
        def _():
            down_copy(i + 2).start()

        @pl.when(i >= 1)
        def _():
            chip.send(i - 1).start()

        @pl.when(i >= 3)
        def _():
            chip.store(i - 3)

        acc = jnp.dot(act_ref[...], w_ref[(i + n_up) % 3, :ff, :bn], preferred_element_type=F32)

        @pl.when(i >= 2)
        def _():
            chip.combine(i - 2)

        chip.keep(i, acc)
        return carry

    lax.fori_loop(0, n_down, down, 0)
    chip.tail()
    norm.finish()


def mlp(h, s, t, gain, wg, wu, wd, layer, rb, n_out, across):
    half, d = h.shape
    rows = 2 * half
    ff = wg.shape[2]
    bf = 384
    bn = min(512, d // 2)
    out = jax.ShapeDtypeStruct((half, d), BF)
    part = jax.ShapeDtypeStruct((half // n_out, d), BF)
    return pl.pallas_call(
        functools.partial(mlp_kernel, layer, bf, bn, rb, n_out, across),
        in_specs=[hbm()] * 7,
        out_specs=[hbm()] * (1 + n_out),
        out_shape=[out] + [part] * n_out,
        scratch_shapes=[
            pltpu.VMEM((rows, d), BF),
            pltpu.VMEM((3, max(d, ff), 2 * bf), BF),
            pltpu.VMEM((2, rows, 2 * bf), F32),
            pltpu.VMEM((rows, ff), BF),
            pltpu.SemaphoreType.DMA((3, 2)),
        ] + norm_scratch(half, d, rb, False) + sum_scratch(half, d, bn, across),
        compiler_params=pltpu.CompilerParams(vmem_limit_bytes=VMEM_LIMIT, collective_id=4 if across else 2, has_side_effects=True),
        cost_estimate=pl.CostEstimate(flops=6 * rows * d * ff, bytes_accessed=2 * (2 * rows * d + 3 * d * ff), transcendentals=rows * ff),
        name="mlp",
    )(h, s, t, gain, wg, wu, wd)


def final_kernel(spans, n_in, n_out, *refs):
    outs = refs[n_in:n_in + n_out]
    bufs, in_sem, out_sem = refs[n_in + n_out:-2], refs[-2], refs[-1]
    loads, stores = [], []
    for c, (b, a, off) in enumerate(spans):
        mine = bufs[3 * c:3 * c + 3]
        loads.append([pltpu.make_async_copy(src.at[pl.ds(0, a + b), :], buf, in_sem.at[c, i]) for i, (src, buf) in enumerate(zip(refs[3 * c:3 * c + 3], mine))])
        stores.append(pltpu.make_async_copy(mine[0].at[pl.ds(0, b), :], outs[0].at[pl.ds(off, b), :], out_sem.at[c, 0]))
        if a:
            stores.append(pltpu.make_async_copy(mine[0].at[pl.ds(b, a), :], outs[1], out_sem.at[c, 1]))
    for copies in loads:
        for copy in copies:
            copy.start()
    for c, (b, a, off) in enumerate(spans):
        mine = bufs[3 * c:3 * c + 3]
        for copy in loads[c]:
            copy.wait()

        def block(i, carry, mine=mine):
            rows = pl.ds(pl.multiple_of(i * 16, 16), 16)
            h, s, t = (buf[rows, :].astype(F32) for buf in mine)
            mine[0][rows, :] = (h + (s + t)).astype(BF)
            return carry

        lax.fori_loop(0, (a + b) // 16, block, 0)
    for copy in stores:
        copy.start()
    for copy in stores:
        copy.wait()


def final(srcs, spans, n_b, out_b):
    d = srcs[0].shape[1]
    args = tuple(srcs) if out_b is None else (*srcs, out_b)
    with_a = [a for _, a, _ in spans if a]
    shapes = [jax.ShapeDtypeStruct((n_b, d), BF)] + [jax.ShapeDtypeStruct((a, d), BF) for a in with_a]
    rows = sum(a + b for b, a, _ in spans)
    return pl.pallas_call(
        functools.partial(final_kernel, spans, len(args), len(shapes)),
        in_specs=[hbm()] * len(args),
        out_specs=[hbm()] * len(shapes),
        out_shape=shapes,
        input_output_aliases={} if out_b is None else {len(srcs): 0},
        scratch_shapes=[pltpu.VMEM((a + b, d), BF) for b, a, _ in spans for _ in range(3)] + [pltpu.SemaphoreType.DMA((len(spans), 3)), pltpu.SemaphoreType.DMA((len(spans), 2))],
        compiler_params=cparams(),
        cost_estimate=pl.CostEstimate(flops=20 * rows * d, bytes_accessed=8 * rows * d, transcendentals=0),
        name="final",
    )(*args)


def solution(mesh):
    row_spec = P(('dp', 'pp', 'tp'), None)
    id_spec = P(('dp', 'pp', 'tp'))
    col_spec = P(None, None, 'tp')
    in_row_spec = P(None, 'tp', None)
    full_spec = P()
    n_pp = mesh.shape['pp']
    across_core = [(i, i ^ 1) for i in range(4)]
    across_y = [(i, i ^ 2) for i in range(4)]

    def per_device(tok_a, seg_a, pos_a, tok_b, seg_b, pos_b, g_attn, wq, wk, wv, wo, g_mlp, wg, wu, wd):
        n_layers, _ = g_attn.shape
        nb, na = tok_b.shape[0], tok_a.shape[0]
        n_kv_all = wk.shape[2] // HEAD
        nkv = n_kv_all // 4
        group = wq.shape[2] // HEAD // nkv
        table = chunk_table(nb, na)
        n_chunks = len(table)
        rb = 16

        off_b, off_a, b0, a0 = [], [], 0, 0
        for b, a in table:
            off_b.append(b0)
            off_a.append(a0)
            b0, a0 = b0 + b, a0 + a
        gain_attn = [g_attn[l:l + 1] for l in range(n_layers)]
        gain_mlp = [g_mlp[l:l + 1] for l in range(n_layers)]

        own_rows = []
        for (b, a), ob, oa in zip(table, off_b, off_a):
            parts = [tok_b[ob:ob + b]] if b else []
            parts += [tok_a[oa:oa + a]] if a else []
            own_rows.append(parts[0] if len(parts) == 1 else jnp.concatenate(parts, axis=0))

        def permute(x, axis, pairs):
            return lax.ppermute(x, axis, pairs)

        def over_core(mine, got):
            pair = jnp.stack([mine, got])
            return jnp.concatenate([pair, permute(pair, 'tp', across_core)], axis=0)

        below = jnp.stack([jnp.sum((seg < v).astype(jnp.int32)) for seg in (seg_b, seg_a) for v in range(4)])
        pos_b_rows = over_core(pos_b, permute(pos_b, 'tp', across_y))
        got_rows = [permute(own_rows[k], 'tp', across_y) for k in range(n_chunks)]
        got_pos_a, got_below = permute(pos_a, 'tp', across_y), permute(below, 'tp', across_y)

        inv_freq = jnp.power(ROPE_BASE, -2.0 * jnp.arange(HEAD // 2, dtype=F32) / HEAD)

        def trig(pos):
            angles = pos.astype(F32)[..., None] * inv_freq
            cos, sin = jnp.cos(angles), jnp.sin(angles)
            return jnp.concatenate([cos, cos], axis=-1), jnp.concatenate([-sin, sin], axis=-1)

        def chunk_trig(k, after):
            (b, a), ob, oa = table[k], off_b[k], off_a[k]
            parts = ([pos_b_rows[:, ob:ob + b]] if b else []) + ([pos_a_rows[:, oa:oa + a]] if a else [])
            pos = (parts[0] if len(parts) == 1 else jnp.concatenate(parts, axis=1)).reshape(4 * (a + b))
            if after is not None:
                pos, _ = lax.optimization_barrier((pos, after))
            return trig(pos)

        cos, sin = [None] * n_chunks, [None] * n_chunks
        bk_b, bk_a = min(512, 16 * nb), min(512, 16 * na)
        out_b, out_a = None, None
        srcs = list(zip(own_rows, got_rows))
        h = [None] * n_chunks
        for l in range(n_layers):
            q, kvs, n = [None] * n_chunks, [None] * n_chunks, [None] * n_chunks
            last = l + 1 == n_layers
            for k in range(n_chunks):
                if l == 0:
                    cos[k], sin[k] = chunk_trig(k, kvs[k - 1][0] if k else None)
                h[k], n[k], kv = kv_proj(srcs[k], gain_attn[l], wk, wv, cos[k], sin[k], l, nkv, rb)
                if l == 0 and k == 0:
                    got_pos_a, got_below, _ = lax.optimization_barrier((got_pos_a, got_below, kv))
                    pos_a_rows = over_core(pos_a, got_pos_a)
                    below = jnp.sum(over_core(below, got_below), axis=0)
                    others = [permute(below, 'pp', [(i, (i + s) % n_pp) for i in range(n_pp)]) for s in range(1, n_pp)]
                    starts = below + others[0] + others[1] + others[2]
                kvs[k] = [kv]
                for s in range(1, n_pp):
                    if k == 2 or (k == 0 and l):
                        kvs[k].append(permute(kv, 'pp', [(i, i + s) for i in range(n_pp - s)]))
                    else:
                        kvs[k].append(permute(kvs[k][-1], 'pp', [(i, i + 1) for i in range(s - 1, n_pp - 1)]))
            sums = []
            groups = ([0], [k for k in range(1, n_chunks)])
            for members in groups:
                qs = q_proj([n[k] for k in members], wq, [x for k in members for x in (cos[k], sin[k])], l)
                for k, x in zip(members, qs):
                    q[k] = x
            for members in groups:
                os = attention(table, members, starts, [q[k] for k in members], kvs, nkv, group, nb, na, (bk_b, bk_a))
                parts = oproj(os, wo, l)
                for k, x in zip(members, parts):
                    sums.append((x, permute(x, 'tp', across_y)))
            for k in range(n_chunks):
                across = last and k + 1 == n_chunks
                h[k], *parts = mlp(h[k], *sums[k], gain_mlp[l], wg, wu, wd, l, rb, 2 if last else 1, across)
                got = parts[-1] if across else permute(parts[-1], 'tp', across_y)
                srcs[k] = (h[k], parts[0], got)
        for members in groups:
            out_b, *rest = final([x for k in members for x in srcs[k]], tuple((*table[k], off_b[k]) for k in members), nb, out_b)
            out_a = rest[0] if rest else out_a
        return out_a, out_b

    def prefill(tokens_a, segment_a, position_a, tokens_b, segment_b, position_b, norm_attn, w_query, w_key, w_value, w_out, norm_mlp, w_gate, w_up, w_down):
        mapped = jax.shard_map(per_device, mesh=mesh, in_specs=(row_spec, id_spec, id_spec, row_spec, id_spec, id_spec, full_spec, col_spec, full_spec, full_spec, in_row_spec, full_spec, col_spec, col_spec, in_row_spec), out_specs=(row_spec, row_spec), check_vma=False)
        return mapped(tokens_a, segment_a, position_a, tokens_b, segment_b, position_b, norm_attn, w_query, w_key, w_value, w_out, norm_mlp, w_gate, w_up, w_down)

    return prefill
```

```python
import functools
import math
import jax
import jax.numpy as jnp
from jax import lax
from jax.experimental import pallas as pl
from jax.experimental.pallas import tpu as pltpu
from jax.sharding import PartitionSpec as P

HEAD = 128
ROPE_BASE = 500000.0
EPS = 1e-5
NEG = -1e30
BF = jnp.bfloat16
F32 = jnp.float32
VMEM_LIMIT = 63 * 1024 * 1024
OWNER_XOR = (0, 2, 1, 3)


def chunk_table(nb, na):
    if nb == 256:
        return [(112, 0), (80, 32), (64, 0)]
    return [(nb // 2, na), (nb // 2, 0)]


def cparams(semantics=None, limit=VMEM_LIMIT):
    return pltpu.CompilerParams(dimension_semantics=semantics, vmem_limit_bytes=limit)


def hbm():
    return pl.BlockSpec(memory_space=pltpu.HBM)


MESH = pl.DeviceIdType.MESH


def other_core():
    t = lax.axis_index('tp')
    return {'tp': t + 1 - 2 * (t % 2)}


def other_side():
    return {'tp': (lax.axis_index('tp') + 2) % 4}


def meet(across=False):
    barrier = pltpu.get_barrier_semaphore()
    peers = [other_core()] + ([other_side()] if across else [])
    for peer in peers:
        pl.semaphore_signal(barrier, inc=1, device_id=peer, device_id_type=MESH)
    pl.semaphore_wait(barrier, len(peers))


def norm_rows(wide, gain):
    inv = lax.rsqrt(jnp.mean(wide * wide, axis=-1, keepdims=True) + EPS)
    return (wide * inv * gain).astype(BF)


def norm_scratch(half, d, rb, init):
    n = half // rb
    bufs = [pltpu.VMEM((half, d), BF)] * (1 if init else 3)
    return bufs + [pltpu.VMEM((1, d), BF), pltpu.SemaphoreType.DMA((2, 4)), pltpu.SemaphoreType.DMA((n,)), pltpu.SemaphoreType.DMA((n,)), pltpu.SemaphoreType.DMA]


class NormExchange:
    def __init__(self, init, rb, srcs, gain_ref, ho_ref, x_ref, scratch):
        self.init, self.rb, self.srcs, self.gain_ref, self.ho_ref, self.x_ref = init, rb, srcs, gain_ref, ho_ref, x_ref
        self.bufs = scratch[:1 if init else 3]
        self.gain_buf, self.in_sem, self.send_sem, self.recv_sem, self.out_sem = scratch[1 if init else 3:]
        self.half = x_ref.shape[0] // 2
        self.own = self.half // 2
        self.n = self.half // rb

    def gain(self, piece):
        return [] if piece else [pltpu.make_async_copy(self.gain_ref, self.gain_buf, self.in_sem.at[0, 3])]

    def loads(self, piece):
        q = self.own
        dst = pl.ds(piece * q, q)
        if self.init:
            return self.gain(piece) + [pltpu.make_async_copy(self.srcs[piece], self.bufs[0].at[dst, :], self.in_sem.at[piece, 0])]
        src = (dst, dst, pl.ds((1 - piece) * q, q))
        return self.gain(piece) + [pltpu.make_async_copy(ref.at[rows, :], buf.at[dst, :], self.in_sem.at[piece, i]) for i, (ref, rows, buf) in enumerate(zip(self.srcs, src, self.bufs))]

    def send(self, i):
        rows = pl.ds(pl.multiple_of(i * self.rb, self.rb), self.rb)
        there = pl.ds(pl.multiple_of(self.half + i * self.rb, self.rb), self.rb)
        return pltpu.make_async_remote_copy(src_ref=self.x_ref.at[rows, :], dst_ref=self.x_ref.at[there, :], send_sem=self.send_sem.at[i], recv_sem=self.recv_sem.at[i], device_id=other_core(), device_id_type=MESH)

    def store(self):
        return pltpu.make_async_copy(self.bufs[0], self.ho_ref, self.out_sem)

    def start(self, piece):
        for copy in self.loads(piece):
            copy.start()

    def run(self, after_first):
        per = self.n // 2

        def block(i, carry):
            rows = pl.ds(pl.multiple_of(i * self.rb, self.rb), self.rb)
            if self.init:
                h = self.bufs[0][rows, :]
            else:
                hb, sb, tb = self.bufs
                h = (hb[rows, :].astype(F32) + (sb[rows, :].astype(F32) + tb[rows, :].astype(F32))).astype(BF)
                hb[rows, :] = h
            self.x_ref[rows, :] = norm_rows(h.astype(F32), self.gain_buf[...].astype(F32))

            @pl.when(i >= 1)
            def _():
                self.send(i - 1).start()

            return carry

        for piece in range(2):
            for copy in self.loads(piece):
                copy.wait()
            if piece == 0:
                after_first()
            lax.fori_loop(piece * per, (piece + 1) * per, block, 0)
        self.store().start()
        self.send(self.n - 1).start()

    def arrive(self):
        for i in range(self.n):
            self.send(i).wait_recv()

    def finish(self):
        for i in range(self.n):
            self.send(i).wait_send()
        self.store().wait()


def sum_scratch(half, d, bn, across=False):
    n = d // bn
    extra = [pltpu.VMEM((half // 2, d), BF), pltpu.SemaphoreType.DMA((n,)), pltpu.SemaphoreType.DMA((n,)), pltpu.SemaphoreType.DMA]
    return [
        pltpu.VMEM((3, half, bn), F32),
        pltpu.VMEM((n, half, bn), BF),
        pltpu.VMEM((n, half, bn), BF),
        pltpu.VMEM((half, d), BF),
        pltpu.SemaphoreType.DMA((n,)),
        pltpu.SemaphoreType.DMA((n,)),
        pltpu.SemaphoreType.DMA((n,)),
    ] + (extra if across else [])


class ChipSum:
    def __init__(self, outs, scratch, across=False):
        self.across = across
        self.outs = outs
        self.mine, self.give, self.got, self.total, self.send_sem, self.recv_sem, self.out_sem, *extra = scratch
        if across:
            self.far, self.y_send, self.y_recv, self.far_sem = extra
        self.n, self.half, self.bn = self.give.shape

    def send(self, i):
        return pltpu.make_async_remote_copy(src_ref=self.give.at[i], dst_ref=self.got.at[i], send_sem=self.send_sem.at[i], recv_sem=self.recv_sem.at[i], device_id=other_core(), device_id_type=MESH)

    def send_far(self, i):
        q = self.half // 2
        return pltpu.make_async_remote_copy(src_ref=self.total.at[pl.ds(q, q), self.cols(i)], dst_ref=self.far.at[:, self.cols(i)], send_sem=self.y_send.at[i], recv_sem=self.y_recv.at[i], device_id=other_side(), device_id_type=MESH)

    def cols(self, i):
        return pl.ds(pl.multiple_of(i * self.bn, 128), self.bn)

    def stores(self, i):
        copies, row = [], 0
        for out in self.outs[:1] if self.across else self.outs:
            copies.append(pltpu.make_async_copy(self.total.at[pl.ds(row, out.shape[0]), self.cols(i)], out.at[:, self.cols(i)], self.out_sem.at[i]))
            row += out.shape[0]
        return copies

    def keep(self, i, acc):
        self.mine[i % 3] = acc[:self.half]
        self.give[i] = acc[self.half:].astype(BF)

    def combine(self, i):
        self.send(i).wait_recv()
        self.total[:, self.cols(i)] = (self.mine[i % 3] + self.got[i].astype(F32)).astype(BF)

    def store(self, i):
        if self.across:
            self.send_far(i).start()
        for copy in self.stores(i):
            copy.start()

    def tail(self):
        last = self.n - 1
        self.send(last).start()
        if self.n >= 3:
            self.store(last - 2)
        self.combine(last - 1)
        self.store(last - 1)
        self.combine(last)
        self.store(last)
        for i in range(self.n):
            self.send(i).wait_send()
            for copy in self.stores(i):
                copy.wait()
        if self.across:
            for i in range(self.n):
                self.send_far(i).wait()
            copy = pltpu.make_async_copy(self.far, self.outs[1], self.far_sem)
            copy.start()
            copy.wait()


def rope(vals, cos, sin):
    return (vals * cos + pltpu.roll(vals, HEAD // 2, 1) * sin).astype(BF)


def kv_kernel(init, layer, nkv, rb, *refs):
    n_src = 2 if init else 3
    srcs = refs[:n_src]
    gain_ref, wk_ref, wv_ref, cos_hbm, sin_hbm, ho_ref, n_ref, kv_ref, x_ref, w_ref, kv_buf, cos_ref, sin_ref, w_sem, o_sem = refs[n_src:n_src + 15]
    norm = NormExchange(init, rb, srcs, gain_ref, ho_ref, x_ref, refs[n_src + 15:])
    half = x_ref.shape[0] // 2
    own = half // 2
    width = nkv * HEAD
    t = lax.axis_index('tp')
    cols = pl.ds(pl.multiple_of(t * width, 128), width)
    weights = [
        pltpu.make_async_copy(wk_ref.at[layer, :, cols], w_ref.at[:, pl.ds(0, width)], w_sem.at[0]),
        pltpu.make_async_copy(wv_ref.at[layer, :, cols], w_ref.at[:, pl.ds(width, width)], w_sem.at[1]),
        pltpu.make_async_copy(cos_hbm, cos_ref, w_sem.at[2]),
        pltpu.make_async_copy(sin_hbm, sin_ref, w_sem.at[3]),
    ]
    owners = (t, (t + 2) % 4, t + 1 - 2 * (t % 2), 3 - t)

    def start_weights():
        for copy in weights:
            copy.start()

    def rows_out(r0):
        rows = pl.ds(r0, half)
        return pltpu.make_async_copy(x_ref.at[rows, :], n_ref.at[rows, :], o_sem.at[4 + r0 // half])

    def kv_out(place):
        return pltpu.make_async_copy(kv_buf.at[pl.ds(place * own, own), :], kv_ref.at[owners[place]], o_sem.at[place])

    def kv_rows(r0, r1):
        both = jnp.dot(x_ref[r0:r1, :], w_ref[...], preferred_element_type=F32)
        for i in range(nkv):
            kv_buf[r0:r1, i * HEAD:(i + 1) * HEAD] = rope(both[:, i * HEAD:(i + 1) * HEAD], cos_ref[r0:r1, :], sin_ref[r0:r1, :])
        kv_buf[r0:r1, width:] = both[:, width:].astype(BF)

    norm.start(0)
    norm.start(1)
    meet()
    norm.run(start_weights)
    rows_out(0).start()
    for copy in weights:
        copy.wait()
    kv_rows(0, half)
    norm.arrive()
    rows_out(half).start()
    kv_out(0).start()
    kv_out(1).start()
    kv_rows(half, 2 * half)
    kv_out(2).start()
    kv_out(3).start()
    norm.finish()
    rows_out(0).wait()
    rows_out(half).wait()
    for place in range(4):
        kv_out(place).wait()


def kv_proj(srcs, gain, wk, wv, cos, sin, layer, nkv, rb):
    init = len(srcs) == 2
    d = wk.shape[1]
    half = 2 * srcs[0].shape[0] if init else srcs[0].shape[0]
    rows = 2 * half
    width = nkv * HEAD
    return pl.pallas_call(
        functools.partial(kv_kernel, init, layer, nkv, rb),
        in_specs=[hbm()] * (len(srcs) + 5),
        out_specs=[hbm()] * 3,
        out_shape=[jax.ShapeDtypeStruct((half, d), BF), jax.ShapeDtypeStruct((rows, d), BF), jax.ShapeDtypeStruct((4, rows // 4, 2 * width), BF)],
        scratch_shapes=[
            pltpu.VMEM((rows, d), BF),
            pltpu.VMEM((d, 2 * width), BF),
            pltpu.VMEM((rows, 2 * width), BF),
            pltpu.VMEM((rows, HEAD), F32),
            pltpu.VMEM((rows, HEAD), F32),
            pltpu.SemaphoreType.DMA((4,)),
            pltpu.SemaphoreType.DMA((6,)),
        ] + norm_scratch(half, d, rb, init),
        compiler_params=pltpu.CompilerParams(vmem_limit_bytes=VMEM_LIMIT, collective_id=3 if init else 0, has_side_effects=True),
        cost_estimate=pl.CostEstimate(flops=2 * rows * d * 2 * width, bytes_accessed=2 * d * (3 * rows + 2 * width), transcendentals=0),
        name="kv_init" if init else "kv_proj",
    )(*srcs, gain, wk, wv, cos, sin)


def q_blocks(qcols):
    blocks, c = [], 0
    while c < qcols:
        width = min(512 if c else 256, qcols - c)
        blocks.append((c, width))
        c += width
    return blocks


def q_kernel(layer, n_in, *refs):
    ns, trigs, outs = refs[:n_in], refs[n_in:3 * n_in], refs[3 * n_in + 1:4 * n_in + 1]
    wq_ref = refs[3 * n_in]
    x_ref, w_ref, q_buf, cos_ref, sin_ref, w_sem, o_sem, x_sem = refs[4 * n_in + 1:]
    blocks = q_blocks(q_buf.shape[1])
    loads, trig, offs, row = [], [], [], 0
    for i, n_hbm in enumerate(ns):
        rows = pl.ds(row, n_hbm.shape[0])
        x_dst, cos_dst, sin_dst = (ref if n_in == 1 else ref.at[rows, :] for ref in (x_ref, cos_ref, sin_ref))
        loads.append(pltpu.make_async_copy(n_hbm, x_dst, x_sem.at[i, 0]))
        trig.append(pltpu.make_async_copy(trigs[2 * i], cos_dst, x_sem.at[i, 1]))
        trig.append(pltpu.make_async_copy(trigs[2 * i + 1], sin_dst, x_sem.at[i, 2]))
        offs.append(rows)
        row += n_hbm.shape[0]
    weights = [pltpu.make_async_copy(wq_ref.at[layer, :, pl.ds(c, bw)], w_ref.at[:, pl.ds(c, bw)], w_sem.at[i]) for i, (c, bw) in enumerate(blocks)]
    for copy in loads + weights[:1] + trig + weights[1:]:
        copy.start()
    for copy in loads + trig:
        copy.wait()
    stores = []
    for j, (c, bw) in enumerate(blocks):
        weights[j].wait()
        acc = jnp.dot(x_ref[...], w_ref[:, c:c + bw], preferred_element_type=F32)
        for i in range(bw // HEAD):
            q_buf[:, c + i * HEAD:c + (i + 1) * HEAD] = rope(acc[:, i * HEAD:(i + 1) * HEAD], cos_ref[...], sin_ref[...])
        for i, q_ref in enumerate(outs):
            rows = slice(None) if n_in == 1 else offs[i]
            stores.append(pltpu.make_async_copy(q_buf.at[rows, pl.ds(c, bw)], q_ref.at[:, pl.ds(c, bw)], o_sem.at[i, j]))
            stores[-1].start()
    for copy in stores:
        copy.wait()


def q_proj(ns, wq, trigs, layer):
    d = ns[0].shape[1]
    rows = sum(n.shape[0] for n in ns)
    qcols = wq.shape[2]
    nb = len(q_blocks(qcols))
    return pl.pallas_call(
        functools.partial(q_kernel, layer, len(ns)),
        in_specs=[hbm()] * (3 * len(ns) + 1),
        out_specs=[hbm()] * len(ns),
        out_shape=[jax.ShapeDtypeStruct((n.shape[0], qcols), BF) for n in ns],
        scratch_shapes=[
            pltpu.VMEM((rows, d), BF),
            pltpu.VMEM((d, qcols), BF),
            pltpu.VMEM((rows, qcols), BF),
            pltpu.VMEM((rows, HEAD), F32),
            pltpu.VMEM((rows, HEAD), F32),
            pltpu.SemaphoreType.DMA((nb,)),
            pltpu.SemaphoreType.DMA((len(ns), nb)),
            pltpu.SemaphoreType.DMA((len(ns), 3)),
        ],
        compiler_params=cparams(),
        cost_estimate=pl.CostEstimate(flops=2 * rows * d * qcols, bytes_accessed=2 * d * (rows + qcols), transcendentals=0),
        name="q_proj",
    )(*ns, *trigs, wq)


SM_C = HEAD ** -0.5 * math.log2(math.e)


def lanes(x, width):
    return jnp.concatenate([x] * (width // HEAD), axis=1) if width > HEAD else x


def flash_step(qs, k, v, ok, m, l, acc):
    s = lax.dot_general(qs, k, (((1,), (1,)), ((), ())), preferred_element_type=F32) * SM_C
    if ok is not None:
        s = jnp.where(ok, s, NEG)
    _, width = s.shape
    m_new = jnp.maximum(m, jnp.max(s, axis=1, keepdims=True))
    alpha = jnp.exp2(m - m_new)
    p = jnp.exp2(s - lanes(m_new, width))
    part = p[:, :HEAD]
    for i in range(1, width // HEAD):
        part = part + p[:, i * HEAD:(i + 1) * HEAD]
    return m_new, l * alpha + part, acc * alpha + jnp.dot(p.astype(BF), v, preferred_element_type=F32)


def flash(q_rows, qi, ql, qi_min, ql_max, kv_ref, bk, nkv, group, lo, hi, m_ref, l_ref, acc_ref):
    rows = qi.shape[0]
    gr = group * rows
    qs = [jnp.concatenate([q_rows(kh * group + i) for i in range(group)], axis=0) for kh in range(nkv)]
    m_ref[:, :gr, :] = jnp.full((nkv, gr, HEAD), NEG, F32)
    l_ref[:, :gr, :] = jnp.zeros((nkv, gr, HEAD), F32)
    acc_ref[:, :gr, :] = jnp.zeros((nkv, gr, HEAD), F32)

    per = kv_ref.shape[1]

    def keys(j, col):
        block = kv_ref[pl.ds(j * (bk // per), bk // per), :, col * HEAD:(col + 1) * HEAD]
        return block.reshape(bk, HEAD)

    def step(j, masked):
        base = j * bk
        ok = None
        if masked:
            kid = base + lax.broadcasted_iota(jnp.int32, (rows, bk), 1)
            ok = (kid <= qi) & (kid >= ql)
            ok = jnp.concatenate([ok] * group, axis=0)
        new = []
        for kh in range(nkv):
            k = keys(j, kh)
            v = keys(j, nkv + kh)
            new.append(flash_step(qs[kh], k, v, ok, m_ref[kh, :gr, :], l_ref[kh, :gr, :], acc_ref[kh, :gr, :]))
        for kh in range(nkv):
            m_ref[kh, :gr, :], l_ref[kh, :gr, :], acc_ref[kh, :gr, :] = new[kh]

    def body(j, carry):
        base = j * bk
        full = (ql_max <= base) & (qi_min >= base + bk - 1)

        @pl.when(full)
        def _():
            step(j, False)

        @pl.when(jnp.logical_not(full))
        def _():
            step(j, True)

        return carry

    lax.fori_loop(lo, hi, body, 0)
    outs = []
    for kh in range(nkv):
        total = jnp.sum(l_ref[kh, :gr, :], axis=1, keepdims=True)
        out = (acc_ref[kh, :gr, :] / total).astype(BF)
        outs += [out[i * rows:(i + 1) * rows, :] for i in range(group)]
    return outs


def attn_kernel(table, mes, nkv, group, nb, na, bks, sc_ref, *refs):
    n_me, n_kv = len(mes), 4 * len(table)
    q_hbm, kv_hbm, o_hbm = refs[:n_me], refs[n_me:n_me + n_kv], refs[n_me + n_kv:2 * n_me + n_kv]
    refs = refs[2 * n_me + n_kv:]
    q_refs, o_refs = refs[:n_me], refs[n_me:2 * n_me]
    kvb_ref, kva_ref, m_ref, l_ref, acc_ref, sem, q_sem, o_sem = refs[2 * n_me:]
    with_a = any(table[me][1] for me in mes)
    t = lax.axis_index('tp')
    p = lax.axis_index('pp')
    load_q = [pltpu.make_async_copy(src, dst, q_sem) for src, dst in zip(q_hbm, q_refs)]
    copies, off_b, off_a = [], 0, 0
    for k, (bk_, ak_) in enumerate(table):
        for s in range(4):
            src = kv_hbm[4 * k + s]
            slot = pl.ds((3 - s) * 4, 4)
            if bk_:
                copies.append(pltpu.make_async_copy(src.at[:, pl.ds(0, bk_), :], kvb_ref.at[slot, pl.ds(off_b, bk_), :], sem))
            if with_a and ak_:
                copies.append(pltpu.make_async_copy(src.at[:, pl.ds(bk_, ak_), :], kva_ref.at[slot, pl.ds(off_a, ak_), :], sem))
        off_b += bk_
        off_a += ak_
    for copy in copies + load_q:
        copy.start()
    for copy in copies + load_q:
        copy.wait()

    def first_key(which, n_own):
        return [sc_ref[4 * which + v] + (3 - p) * 4 * n_own for v in range(4)]

    def lowest(starts, idx):
        low = jnp.zeros_like(idx) + starts[0]
        for v in range(1, 4):
            low = jnp.where(idx >= starts[v], starts[v], low)
        return low

    def one_chunk(me, q_ref, o_ref, out_hbm):
        b, a = table[me]
        own = a + b
        off_b, off_a = sum(x[0] for x in table[:me]), sum(x[1] for x in table[:me])

        def store(o):
            rows = pl.ds(pl.multiple_of(o * own, 16), own)
            return pltpu.make_async_copy(o_ref.at[rows, :], out_hbm.at[rows, :], o_sem)

        if b:
            starts_b = first_key(0, nb)

            def one_owner(o, carry):
                r0 = pl.multiple_of(o * own, 16)
                owner = t ^ (2 * (o % 2) + o // 2)
                i0 = 12 * nb + owner * nb + off_b
                low0 = lowest(starts_b, i0)
                last_low = lowest(starts_b, i0 + b - 1)
                idx = i0 + lax.broadcasted_iota(jnp.int32, (b, 1), 0)
                q_rows = lambda h: q_ref[pl.ds(r0, b), h * HEAD:(h + 1) * HEAD]
                outs = flash(q_rows, idx, lowest(starts_b, idx), i0, last_low, kvb_ref, bks[0], nkv, group, low0 // bks[0], (i0 + b - 1) // bks[0] + 1, m_ref, l_ref, acc_ref)
                for h, out in enumerate(outs):
                    o_ref[pl.ds(r0, b), h * HEAD:(h + 1) * HEAD] = out
                if not a:
                    store(o).start()
                return carry

            lax.fori_loop(0, 4, one_owner, 0)
        if a:
            starts_a = first_key(1, na)
            idx = jnp.concatenate([12 * na + (t ^ OWNER_XOR[o]) * na + off_a + lax.broadcasted_iota(jnp.int32, (a, 1), 0) for o in range(4)], axis=0)
            spans = [(o * own + b, o * own + b + a) for o in range(4)]
            gather = lambda c0, c1: jnp.concatenate([q_ref[r0:r1, c0:c1] for r0, r1 in spans], axis=0)
            n_blocks = 16 * na // bks[1]
            outs = flash(lambda h: gather(h * HEAD, (h + 1) * HEAD), idx, lowest(starts_a, idx), 0, 16 * na, kva_ref, bks[1], nkv, group, starts_a[0] // bks[1], n_blocks, m_ref, l_ref, acc_ref)
            for h, out in enumerate(outs):
                for o, (r0, r1) in enumerate(spans):
                    o_ref[r0:r1, h * HEAD:(h + 1) * HEAD] = out[o * a:(o + 1) * a, :]
            for o in range(4):
                store(o).start()
        return [store(o) for o in range(4)]

    stores = []
    for i, me in enumerate(mes):
        stores += one_chunk(me, q_refs[i], o_refs[i], o_hbm[i])
    for copy in stores:
        copy.wait()


def attention(table, mes, sc, qs, kvs, nkv, group, nb, na, bks):
    qcols = qs[0].shape[1]
    gr = group * max(max(4 * table[me][1], table[me][0]) for me in mes)
    kvw = 2 * nkv * HEAD
    flat = [x for per_chunk in kvs for x in per_chunk]
    flops = sum(4 * (4 * table[me][0] * 16 * nb + 4 * table[me][1] * 16 * na) * qcols for me in mes)
    shapes = [jax.ShapeDtypeStruct(q.shape, BF) for q in qs]
    return pl.pallas_call(
        functools.partial(attn_kernel, table, mes, nkv, group, nb, na, bks),
        in_specs=[pl.BlockSpec(memory_space=pltpu.SMEM)] + [hbm()] * (len(qs) + len(flat)),
        out_specs=[hbm()] * len(qs),
        scratch_shapes=[pltpu.VMEM(q.shape, BF) for q in qs] * 2 + [
            pltpu.VMEM((16, nb, kvw), BF),
            pltpu.VMEM((16, na, kvw), BF),
            pltpu.VMEM((nkv, gr, HEAD), F32),
            pltpu.VMEM((nkv, gr, HEAD), F32),
            pltpu.VMEM((nkv, gr, HEAD), F32),
            pltpu.SemaphoreType.DMA,
            pltpu.SemaphoreType.DMA,
            pltpu.SemaphoreType.DMA,
        ],
        out_shape=shapes,
        compiler_params=cparams(),
        cost_estimate=pl.CostEstimate(flops=flops, bytes_accessed=32 * (nb + na) * kvw, transcendentals=0),
        name="attention",
    )(sc, *qs, *flat)


def oproj_kernel(layer, bn, n_in, *refs):
    o_hbm, w_ref, outs = refs[:n_in], refs[n_in], refs[n_in + 1:2 * n_in + 1]
    o_ref, w_buf, w_sem, o_sem, *scratch = refs[2 * n_in + 1:]
    chip = ChipSum(outs, scratch)
    loads = [pltpu.make_async_copy(w_ref.at[layer, :, pl.ds(i * bn, bn)], w_buf.at[:, pl.ds(i * bn, bn)], w_sem.at[i]) for i in range(chip.n)]
    load_o, row = ([pltpu.make_async_copy(o_hbm[0], o_ref, o_sem.at[0, 0])] if n_in == 1 else []), 0
    for i, src in enumerate(o_hbm if n_in > 1 else ()):
        half = src.shape[0] // 2
        for part in range(2):
            load_o.append(pltpu.make_async_copy(src.at[pl.ds(part * half, half), :], o_ref.at[pl.ds(part * chip.half + row, half), :], o_sem.at[i, part]))
        row += half
    for copy in load_o + loads:
        copy.start()
    meet()
    for copy in load_o:
        copy.wait()
    for i in range(chip.n):
        loads[i].wait()
        if i >= 1:
            chip.send(i - 1).start()
        if i >= 3:
            chip.store(i - 3)
        acc = jnp.dot(o_ref[...], w_buf[:, i * bn:(i + 1) * bn], preferred_element_type=F32)
        if i >= 2:
            chip.combine(i - 2)
        chip.keep(i, acc)
    chip.tail()


def oproj(os, wo, layer):
    k = os[0].shape[1]
    rows = sum(o.shape[0] for o in os)
    d = wo.shape[2]
    bn = min(1024, d // 2)
    half = rows // 2
    return pl.pallas_call(
        functools.partial(oproj_kernel, layer, bn, len(os)),
        in_specs=[hbm()] * (len(os) + 1),
        out_specs=[hbm()] * len(os),
        out_shape=[jax.ShapeDtypeStruct((o.shape[0] // 2, d), BF) for o in os],
        scratch_shapes=[pltpu.VMEM((rows, k), BF), pltpu.VMEM((k, d), BF), pltpu.SemaphoreType.DMA((d // bn,)), pltpu.SemaphoreType.DMA((len(os), 2))] + sum_scratch(half, d, bn),
        compiler_params=pltpu.CompilerParams(vmem_limit_bytes=VMEM_LIMIT, collective_id=1, has_side_effects=True),
        cost_estimate=pl.CostEstimate(flops=2 * rows * k * d, bytes_accessed=2 * (rows * k + k * d + rows * d), transcendentals=0),
        name="oproj",
    )(*os, wo)


def mlp_kernel(layer, bf, bn, rb, n_out, across, *refs):
    srcs = refs[:3]
    gain_ref, wg_ref, wu_ref, wd_ref, ho_ref = refs[3:8]
    outs = refs[8:8 + n_out]
    x_ref, w_ref, both_ref, act_ref, w_sem = refs[8 + n_out:13 + n_out]
    scratch = refs[13 + n_out:]
    norm = NormExchange(False, rb, srcs, gain_ref, ho_ref, x_ref, scratch[:8])
    chip = ChipSum(outs, scratch[8:], across)
    ff = wg_ref.shape[2]
    n_up = ff // bf
    n_down = chip.n

    def up_copies(step):
        slot = step % 3
        cols = pl.ds(pl.multiple_of(step * bf, 128), bf)
        return (
            pltpu.make_async_copy(wg_ref.at[layer, :, cols], w_ref.at[slot, pl.ds(0, wg_ref.shape[1]), pl.ds(0, bf)], w_sem.at[slot, 0]),
            pltpu.make_async_copy(wu_ref.at[layer, :, cols], w_ref.at[slot, pl.ds(0, wg_ref.shape[1]), pl.ds(bf, bf)], w_sem.at[slot, 1]),
        )

    def down_copy(step):
        slot = (step + n_up) % 3
        return pltpu.make_async_copy(wd_ref.at[layer, :, chip.cols(step)], w_ref.at[slot, pl.ds(0, ff), pl.ds(0, bn)], w_sem.at[slot, 0])

    def gated(step):
        slot = step % 2
        gate = both_ref[slot, :, :bf]
        act = gate * jax.nn.sigmoid(gate) * both_ref[slot, :, bf:]
        act_ref[:, pl.ds(pl.multiple_of(step * bf, 128), bf)] = act.astype(BF)

    def start_up(step):
        for copy in up_copies(step):
            copy.start()

    def wait_up(step):
        for copy in up_copies(step):
            copy.wait()

    norm.start(0)
    norm.start(1)
    start_up(0)
    meet(across)
    norm.run(lambda: start_up(1))
    norm.arrive()

    def up(j, carry):
        wait_up(j)

        @pl.when(j + 2 < n_up)
        def _():
            start_up(j + 2)

        @pl.when(j + 2 >= n_up)
        def _():
            down_copy(j + 2 - n_up).start()

        gated(jnp.maximum(j - 1, 0))
        both_ref[j % 2] = jnp.dot(x_ref[...], w_ref[j % 3, :x_ref.shape[1], :], preferred_element_type=F32)
        return carry

    lax.fori_loop(0, n_up, up, 0)
    gated(n_up - 1)

    def down(i, carry):
        down_copy(i).wait()

        @pl.when(i + 2 < n_down)
        def _():
            down_copy(i + 2).start()

        @pl.when(i >= 1)
        def _():
            chip.send(i - 1).start()

        @pl.when(i >= 3)
        def _():
            chip.store(i - 3)

        acc = jnp.dot(act_ref[...], w_ref[(i + n_up) % 3, :ff, :bn], preferred_element_type=F32)

        @pl.when(i >= 2)
        def _():
            chip.combine(i - 2)

        chip.keep(i, acc)
        return carry

    lax.fori_loop(0, n_down, down, 0)
    chip.tail()
    norm.finish()


def mlp(h, s, t, gain, wg, wu, wd, layer, rb, n_out, across):
    half, d = h.shape
    rows = 2 * half
    ff = wg.shape[2]
    bf = 384
    bn = min(512, d // 2)
    out = jax.ShapeDtypeStruct((half, d), BF)
    part = jax.ShapeDtypeStruct((half // n_out, d), BF)
    return pl.pallas_call(
        functools.partial(mlp_kernel, layer, bf, bn, rb, n_out, across),
        in_specs=[hbm()] * 7,
        out_specs=[hbm()] * (1 + n_out),
        out_shape=[out] + [part] * n_out,
        scratch_shapes=[
            pltpu.VMEM((rows, d), BF),
            pltpu.VMEM((3, max(d, ff), 2 * bf), BF),
            pltpu.VMEM((2, rows, 2 * bf), F32),
            pltpu.VMEM((rows, ff), BF),
            pltpu.SemaphoreType.DMA((3, 2)),
        ] + norm_scratch(half, d, rb, False) + sum_scratch(half, d, bn, across),
        compiler_params=pltpu.CompilerParams(vmem_limit_bytes=VMEM_LIMIT, collective_id=4 if across else 2, has_side_effects=True),
        cost_estimate=pl.CostEstimate(flops=6 * rows * d * ff, bytes_accessed=2 * (2 * rows * d + 3 * d * ff), transcendentals=rows * ff),
        name="mlp",
    )(h, s, t, gain, wg, wu, wd)


def final_kernel(spans, n_in, n_out, *refs):
    outs = refs[n_in:n_in + n_out]
    bufs, in_sem, out_sem = refs[n_in + n_out:-2], refs[-2], refs[-1]
    loads, stores = [], []
    for c, (b, a, off) in enumerate(spans):
        mine = bufs[3 * c:3 * c + 3]
        loads.append([pltpu.make_async_copy(src.at[pl.ds(0, a + b), :], buf, in_sem.at[c, i]) for i, (src, buf) in enumerate(zip(refs[3 * c:3 * c + 3], mine))])
        stores.append(pltpu.make_async_copy(mine[0].at[pl.ds(0, b), :], outs[0].at[pl.ds(off, b), :], out_sem.at[c, 0]))
        if a:
            stores.append(pltpu.make_async_copy(mine[0].at[pl.ds(b, a), :], outs[1], out_sem.at[c, 1]))
    for copies in loads:
        for copy in copies:
            copy.start()
    for c, (b, a, off) in enumerate(spans):
        mine = bufs[3 * c:3 * c + 3]
        for copy in loads[c]:
            copy.wait()

        def block(i, carry, mine=mine):
            rows = pl.ds(pl.multiple_of(i * 16, 16), 16)
            h, s, t = (buf[rows, :].astype(F32) for buf in mine)
            mine[0][rows, :] = (h + (s + t)).astype(BF)
            return carry

        lax.fori_loop(0, (a + b) // 16, block, 0)
    for copy in stores:
        copy.start()
    for copy in stores:
        copy.wait()


def final(srcs, spans, n_b, out_b):
    d = srcs[0].shape[1]
    args = tuple(srcs) if out_b is None else (*srcs, out_b)
    with_a = [a for _, a, _ in spans if a]
    shapes = [jax.ShapeDtypeStruct((n_b, d), BF)] + [jax.ShapeDtypeStruct((a, d), BF) for a in with_a]
    rows = sum(a + b for b, a, _ in spans)
    return pl.pallas_call(
        functools.partial(final_kernel, spans, len(args), len(shapes)),
        in_specs=[hbm()] * len(args),
        out_specs=[hbm()] * len(shapes),
        out_shape=shapes,
        input_output_aliases={} if out_b is None else {len(srcs): 0},
        scratch_shapes=[pltpu.VMEM((a + b, d), BF) for b, a, _ in spans for _ in range(3)] + [pltpu.SemaphoreType.DMA((len(spans), 3)), pltpu.SemaphoreType.DMA((len(spans), 2))],
        compiler_params=cparams(),
        cost_estimate=pl.CostEstimate(flops=20 * rows * d, bytes_accessed=8 * rows * d, transcendentals=0),
        name="final",
    )(*args)


def solution(mesh):
    row_spec = P(('dp', 'pp', 'tp'), None)
    id_spec = P(('dp', 'pp', 'tp'))
    col_spec = P(None, None, 'tp')
    in_row_spec = P(None, 'tp', None)
    full_spec = P()
    n_pp = mesh.shape['pp']
    across_core = [(i, i ^ 1) for i in range(4)]
    across_y = [(i, i ^ 2) for i in range(4)]

    def per_device(tok_a, seg_a, pos_a, tok_b, seg_b, pos_b, g_attn, wq, wk, wv, wo, g_mlp, wg, wu, wd):
        n_layers, _ = g_attn.shape
        nb, na = tok_b.shape[0], tok_a.shape[0]
        n_kv_all = wk.shape[2] // HEAD
        nkv = n_kv_all // 4
        group = wq.shape[2] // HEAD // nkv
        table = chunk_table(nb, na)
        n_chunks = len(table)
        rb = 16

        off_b, off_a, b0, a0 = [], [], 0, 0
        for b, a in table:
            off_b.append(b0)
            off_a.append(a0)
            b0, a0 = b0 + b, a0 + a
        gain_attn = [g_attn[l:l + 1] for l in range(n_layers)]
        gain_mlp = [g_mlp[l:l + 1] for l in range(n_layers)]

        own_rows = []
        for (b, a), ob, oa in zip(table, off_b, off_a):
            parts = [tok_b[ob:ob + b]] if b else []
            parts += [tok_a[oa:oa + a]] if a else []
            own_rows.append(parts[0] if len(parts) == 1 else jnp.concatenate(parts, axis=0))

        def permute(x, axis, pairs):
            return lax.ppermute(x, axis, pairs)

        def over_core(mine, got):
            pair = jnp.stack([mine, got])
            return jnp.concatenate([pair, permute(pair, 'tp', across_core)], axis=0)

        below = jnp.stack([jnp.sum((seg < v).astype(jnp.int32)) for seg in (seg_b, seg_a) for v in range(4)])
        pos_b_rows = over_core(pos_b, permute(pos_b, 'tp', across_y))
        got_rows = [permute(own_rows[k], 'tp', across_y) for k in range(n_chunks)]
        got_pos_a, got_below = permute(pos_a, 'tp', across_y), permute(below, 'tp', across_y)

        inv_freq = jnp.power(ROPE_BASE, -2.0 * jnp.arange(HEAD // 2, dtype=F32) / HEAD)

        def trig(pos):
            angles = pos.astype(F32)[..., None] * inv_freq
            cos, sin = jnp.cos(angles), jnp.sin(angles)
            return jnp.concatenate([cos, cos], axis=-1), jnp.concatenate([-sin, sin], axis=-1)

        def chunk_trig(k, after):
            (b, a), ob, oa = table[k], off_b[k], off_a[k]
            parts = ([pos_b_rows[:, ob:ob + b]] if b else []) + ([pos_a_rows[:, oa:oa + a]] if a else [])
            pos = (parts[0] if len(parts) == 1 else jnp.concatenate(parts, axis=1)).reshape(4 * (a + b))
            if after is not None:
                pos, _ = lax.optimization_barrier((pos, after))
            return trig(pos)

        cos, sin = [None] * n_chunks, [None] * n_chunks
        bk_b, bk_a = min(512, 16 * nb), min(512, 16 * na)
        out_b, out_a = None, None
        srcs = list(zip(own_rows, got_rows))
        h = [None] * n_chunks
        for l in range(n_layers):
            q, kvs, n = [None] * n_chunks, [None] * n_chunks, [None] * n_chunks
            last = l + 1 == n_layers
            for k in range(n_chunks):
                if l == 0:
                    cos[k], sin[k] = chunk_trig(k, kvs[k - 1][0] if k else None)
                h[k], n[k], kv = kv_proj(srcs[k], gain_attn[l], wk, wv, cos[k], sin[k], l, nkv, rb)
                if l == 0 and k == 0:
                    got_pos_a, got_below, _ = lax.optimization_barrier((got_pos_a, got_below, kv))
                    pos_a_rows = over_core(pos_a, got_pos_a)
                    below = jnp.sum(over_core(below, got_below), axis=0)
                    others = [permute(below, 'pp', [(i, (i + s) % n_pp) for i in range(n_pp)]) for s in range(1, n_pp)]
                    starts = below + others[0] + others[1] + others[2]
                kvs[k] = [kv]
                for s in range(1, n_pp):
                    if k == 2 or (k == 0 and l):
                        kvs[k].append(permute(kv, 'pp', [(i, i + s) for i in range(n_pp - s)]))
                    else:
                        kvs[k].append(permute(kvs[k][-1], 'pp', [(i, i + 1) for i in range(s - 1, n_pp - 1)]))
            sums = []
            groups = ([0], [k for k in range(1, n_chunks)])
            for members in groups:
                qs = q_proj([n[k] for k in members], wq, [x for k in members for x in (cos[k], sin[k])], l)
                for k, x in zip(members, qs):
                    q[k] = x
            for members in groups:
                os = attention(table, members, starts, [q[k] for k in members], kvs, nkv, group, nb, na, (bk_b, bk_a))
                parts = oproj(os, wo, l)
                for k, x in zip(members, parts):
                    sums.append((x, permute(x, 'tp', across_y)))
            for k in range(n_chunks):
                across = last and k + 1 == n_chunks
                h[k], *parts = mlp(h[k], *sums[k], gain_mlp[l], wg, wu, wd, l, rb, 2 if last else 1, across)
                got = parts[-1] if across else permute(parts[-1], 'tp', across_y)
                srcs[k] = (h[k], parts[0], got)
        for members in groups:
            out_b, *rest = final([x for k in members for x in srcs[k]], tuple((*table[k], off_b[k]) for k in members), nb, out_b)
            out_a = rest[0] if rest else out_a
        return out_a, out_b

    def prefill(tokens_a, segment_a, position_a, tokens_b, segment_b, position_b, norm_attn, w_query, w_key, w_value, w_out, norm_mlp, w_gate, w_up, w_down):
        mapped = jax.shard_map(per_device, mesh=mesh, in_specs=(row_spec, id_spec, id_spec, row_spec, id_spec, id_spec, full_spec, col_spec, full_spec, full_spec, in_row_spec, full_spec, col_spec, col_spec, in_row_spec), out_specs=(row_spec, row_spec), check_vma=False)
        return mapped(tokens_a, segment_a, position_a, tokens_b, segment_b, position_b, norm_attn, w_query, w_key, w_value, w_out, norm_mlp, w_gate, w_up, w_down)

    return prefill
```
